128 devices in a mesh: seq: 32 (over y_lo, z, x), head: 4 (over y_hi, core).
Axes of the slice: x: 4, y: 4 (y_hi: 2, y_lo: 2; y = y_hi * 2 + y_lo), z: 4, core: 2. Of those that a mesh axis runs over, the one named last changes fastest.
Arguments:
- queries: bfloat16 [4096, 3072], P('seq', 'head'), may hold values from -8 to 8
- latents: bfloat16 [4096, 576], P('seq'), may hold values from -8 to 8
- key_up: bfloat16 [512, 2048], P(None, 'head'), may hold values from -0.25 to 0.25
- value_up: bfloat16 [512, 2048], P(None, 'head'), may hold values from -0.25 to 0.25
- out_grad: bfloat16 [4096, 2048], P('seq', 'head'), may hold values from -48 to 48
- positions: int32 [4096], P('seq'), may hold values from 0 to 4095, as said below
Outputs:
- query_grad: bfloat16 [4096, 3072], P('seq', 'head')
- latent_grad: float32 [4096, 576], P('seq')
- key_up_grad: float32 [512, 2048], P(None, 'head')
- value_up_grad: float32 [512, 2048], P(None, 'head')
The draws below stay inside these ranges and needn't reach their ends.
Inputs may be any that keep to these rules, and one draw needn't show every extreme that they name: Every position from 0 to 4095 occurs once; positions come in stripes of 128 consecutive positions in ascending order, each stripe whole within the rows of one device.
All inputs are finite; a program needn't handle non-finite values.
Results may differ from the reference program's by a relative error of at most 0.0084.
Values may be sent and summed in bfloat16 or wider, within the bound.
A program may use at most 64 MiB of HBM per device.

```python
import math
import jax
import jax.numpy as jnp
from jax import lax

D_LAT = 512
D_ROPE = 64
D_NOPE = 128
D_V = 128
STRIPE = 128
HEADS = 16
SEQ = 4096


def stripe_positions(key):
    order = jax.random.permutation(jax.random.fold_in(key, 11), SEQ // STRIPE).astype(jnp.int32)
    within = jnp.arange(STRIPE, dtype=jnp.int32)
    return (order[:, None] * STRIPE + within[None, :]).reshape(SEQ)


def draw_positions(key, part):
    return stripe_positions(key)


def draw_queries(key, part):
    width = HEADS * (D_NOPE + D_ROPE)
    own = jax.random.fold_in(key, 21)
    base = jax.random.normal(own, (SEQ, width), jnp.float32)
    return jnp.clip(base, -8.0, 8.0).astype(jnp.bfloat16)


def draw_latents(key, part):
    width = D_LAT + D_ROPE
    own = jax.random.fold_in(key, 31)
    base = jax.random.normal(own, (SEQ, width), jnp.float32)
    return jnp.clip(base, -8.0, 8.0).astype(jnp.bfloat16)


def block_levels(stream_key, extent, pieces, least, top_value):
    factor_of = 1.0
    for position, shards_of in pieces:
        steps = jax.random.uniform(jax.random.fold_in(jax.random.fold_in(stream_key, 6), position), (shards_of,), jnp.float32, least / len(pieces), top_value / len(pieces))
        factor_of = factor_of * jnp.repeat(jnp.exp(steps), extent[position] // shards_of).reshape((-1,) + (1,) * (len(extent) - 1 - position))
    return factor_of


def normal_values(own_key, dims, deviation, limit, pieces=(), held_as=jnp.bfloat16):
    factor_of = block_levels(own_key, dims, pieces, -0.22, 0.18) if pieces else 1.0
    entries = jax.random.normal(own_key, dims, jnp.float32) * deviation * factor_of
    return jnp.minimum(jnp.maximum(entries, -limit), limit).astype(held_as)


def setup_inputs(seed: int = 0) -> dict:
    key_of = jax.random.split(jax.random.key(seed), 7)
    return {
        "queries": draw_queries(jax.random.fold_in(key_of[6], 71), 0),
        "latents": draw_latents(jax.random.fold_in(key_of[6], 71), 0),
        "key_up": normal_values(key_of[2], (D_LAT, HEADS * D_NOPE), D_LAT ** -0.5, 0.25, ((1, 4),)),
        "value_up": normal_values(key_of[3], (D_LAT, HEADS * D_V), D_LAT ** -0.5, 0.25, ((1, 4),)),
        "out_grad": normal_values(key_of[4], (SEQ, HEADS * D_V), 8.0, 48.0, ((0, 32), (1, 4))),
        "positions": draw_positions(jax.random.fold_in(key_of[6], 71), 0),
    }


NEG = -1e+30

def reference(queries, latents, key_up, value_up, out_grad, positions):
    seq = latents.shape[0]
    heads = key_up.shape[1] // D_NOPE
    qk = D_NOPE + D_ROPE
    scale = 1.0 / math.sqrt(qk)
    compressed = latents[:, :D_LAT]
    rope_keys = latents[:, D_LAT:].astype(jnp.float32)
    key_nope = jnp.dot(compressed, key_up, preferred_element_type=jnp.float32).astype(jnp.bfloat16)
    values = jnp.dot(compressed, value_up, preferred_element_type=jnp.float32).astype(jnp.bfloat16)
    key_heads = lax.optimization_barrier(key_nope).astype(jnp.float32).reshape(seq, heads, D_NOPE)
    value_heads = lax.optimization_barrier(values).astype(jnp.float32).reshape(seq, heads, D_V)
    block = math.gcd(seq, 512)
    nblocks = seq // block
    q_blocks = queries.reshape(nblocks, block, heads, qk)
    g_blocks = out_grad.reshape(nblocks, block, heads, D_V)
    p_blocks = positions.reshape(nblocks, block)

    def one_block(carry, inputs):
        key_acc, rope_acc, value_acc = carry
        q_block, g_block, pos_block = inputs
        q_nope = q_block[:, :, :D_NOPE].astype(jnp.float32)
        q_rope = q_block[:, :, D_NOPE:].astype(jnp.float32)
        grads = g_block.astype(jnp.float32)
        scores = jnp.einsum('bhd,khd->hbk', q_nope, key_heads)
        scores = (scores + jnp.einsum('bhd,kd->hbk', q_rope, rope_keys)) * scale
        visible = (positions[None, :] <= pos_block[:, None])[None]
        masked = jnp.where(visible, scores, NEG)
        top = lax.optimization_barrier(jnp.max(masked, axis=2, keepdims=True))
        total = lax.optimization_barrier(jnp.sum(jnp.exp(jnp.where(visible, scores - top, NEG)), axis=2, keepdims=True))
        lse = top + jnp.log(total)
        probs = jnp.exp(jnp.where(visible, scores - lse, NEG))
        dprobs = jnp.einsum('bhd,khd->hbk', grads, value_heads)
        delta = lax.optimization_barrier(jnp.sum(probs * dprobs, axis=2, keepdims=True))
        dscore16 = (probs * (dprobs - delta) * scale).astype(jnp.bfloat16)
        dscore = lax.optimization_barrier(dscore16).astype(jnp.float32)
        probs16 = lax.optimization_barrier(probs.astype(jnp.bfloat16)).astype(jnp.float32)
        grad_nope = jnp.einsum('hbk,khd->bhd', dscore, key_heads)
        grad_rope = jnp.einsum('hbk,kd->bhd', dscore, rope_keys)
        q_grad = jnp.concatenate([grad_nope, grad_rope], axis=2).reshape(block, heads * qk)
        key_acc = key_acc + jnp.einsum('hbk,bhd->khd', dscore, q_nope)
        rope_acc = rope_acc + jnp.einsum('hbk,bhd->kd', dscore, q_rope)
        value_acc = value_acc + jnp.einsum('hbk,bhd->khd', probs16, grads)
        return ((key_acc, rope_acc, value_acc), q_grad.astype(jnp.bfloat16))
    start = (jnp.zeros((seq, heads, D_NOPE), jnp.float32), jnp.zeros((seq, D_ROPE), jnp.float32), jnp.zeros((seq, heads, D_V), jnp.float32))
    sums, q_grads = lax.scan(one_block, start, (q_blocks, g_blocks, p_blocks))
    key_acc, rope_acc, value_acc = sums
    key_grad = key_acc.reshape(seq, heads * D_NOPE)
    value_grad = value_acc.reshape(seq, heads * D_V)
    high = lax.Precision.HIGHEST
    key_up32 = key_up.astype(jnp.float32)
    value_up32 = value_up.astype(jnp.float32)
    folded = jnp.dot(key_grad, key_up32.T, precision=high)
    folded = folded + jnp.dot(value_grad, value_up32.T, precision=high)
    latent_grad = jnp.concatenate([folded, rope_acc], axis=1)
    compressed32 = compressed.astype(jnp.float32)
    key_up_grad = jnp.dot(compressed32.T, key_grad, precision=high)
    value_up_grad = jnp.dot(compressed32.T, value_grad, precision=high)
    query_grad = q_grads.reshape(seq, heads * qk)
    return (query_grad, latent_grad, key_up_grad, value_up_grad)
```

```python
import math

import jax
import jax.numpy as jnp
from jax import lax
from jax.experimental import pallas as pl
from jax.experimental.pallas import tpu as pltpu
from jax.sharding import PartitionSpec as P


D_LAT = 512
D_ROPE = 64
D_NOPE = 128
D_V = 128
ROWS = 128
NA = 4
NB = 4
NY = 2
QW = 384
KW = 384
LW = 640
QTOK = NB * NA * ROWS
KTOK = NY * NA * ROWS
TILE = 256
NEG = -1e30
FLOOR = -1e29
SCALE = 1.0 / math.sqrt(D_NOPE + D_ROPE)
LOG2E = math.log2(math.e)
MESH = pl.DeviceIdType.MESH
F32 = jnp.float32
BF16 = jnp.bfloat16
VMEM = pl.BlockSpec(memory_space=pltpu.VMEM)
SMEM = pl.BlockSpec(memory_space=pltpu.SMEM)
NT = (((1,), (1,)), ((), ()))
TN = (((0,), (0,)), ((), ()))


def coords():
    seq = lax.axis_index("seq")
    head = lax.axis_index("head")
    core = head % 2
    y = seq // 16
    z = (seq // 4) % 4
    x = seq % 4
    a = x + core * (z - x)
    b = z + core * (x - z)
    sa = 1 + 3 * core
    sb = 4 - 3 * core

    def dev(a2, b2, y2):
        return (y2 * 16 + a2 * sa + b2 * sb, head)

    return seq, head, y, a, b, dev


def meet(partners):
    barrier = pltpu.get_barrier_semaphore()
    for p in partners:
        pl.semaphore_signal(barrier, inc=1, device_id=p, device_id_type=MESH)
    pl.semaphore_wait(barrier, len(partners))


def rcopy(src, dst, send, recv, device):
    return pltpu.make_async_remote_copy(
        src_ref=src, dst_ref=dst, send_sem=send, recv_sem=recv, device_id=device, device_id_type=MESH
    )


def dot(u, v, dims=(((1,), (0,)), ((), ()))):
    return lax.dot_general(u, v, dims, preferred_element_type=F32)


def shape(dims, dtype=BF16):
    return jax.ShapeDtypeStruct(dims, dtype)


def compute_params():
    return pltpu.CompilerParams(vmem_limit_bytes=56 * 1024 * 1024)


def comm_params(which):
    return pltpu.CompilerParams(
        collective_id=which, has_side_effects=True, vmem_limit_bytes=40 * 1024 * 1024
    )


def prologue_kernel(pos_ref, q_ref, lat_ref, ku_ref, vu_ref, g_ref, pq_ref, pk_ref):
    stripe = lax.shift_right_logical(pos_ref[0], 7).astype(F32)
    lane = lax.broadcasted_iota(jnp.int32, (ROWS, 64), 1)
    q_tail = jnp.where(lane == 0, stripe, 0.0).astype(BF16)
    k_tail = jnp.where(lane == 1, stripe, 0.0).astype(BF16)
    comp = lat_ref[:, :D_LAT]
    kn = dot(comp, ku_ref[...]).astype(BF16)
    vv = dot(comp, vu_ref[...]).astype(BF16)
    k_rest = jnp.concatenate([lat_ref[:, D_LAT:], k_tail], axis=1)
    for h in range(NA):
        q = q_ref[:, h * 192 : (h + 1) * 192]
        pq_ref[h, :, 0:128] = q[:, :128]
        pq_ref[h, :, 128:256] = jnp.concatenate([q[:, 128:], q_tail], axis=1)
        pq_ref[h, :, 256:384] = g_ref[:, h * 128 : (h + 1) * 128]
        pk_ref[h, :, 0:128] = kn[:, h * 128 : (h + 1) * 128]
        pk_ref[h, :, 128:256] = k_rest
        pk_ref[h, :, 256:384] = vv[:, h * 128 : (h + 1) * 128]


def key_positions(kb_ref):
    pick = (lax.broadcasted_iota(jnp.int32, (256, TILE), 0) == 193).astype(F32).astype(BF16)
    stripe = dot(kb_ref[:, :256], pick)
    row = lax.broadcasted_iota(jnp.int32, (KTOK, TILE), 0) % ROWS
    return stripe * 128.0 + row.astype(F32)


def query_positions(qp):
    pick = (lax.broadcasted_iota(jnp.int32, (8, 256), 1) == 192).astype(F32).astype(BF16)
    stripe = dot(pick, qp, NT)[0:1, :]
    col = lax.broadcasted_iota(jnp.int32, (1, TILE), 1) % ROWS
    return stripe * 128.0 + col.astype(F32)


def forward_kernel(qb_ref, kb_ref, st_ref, kpos):
    kpos[...] = key_positions(kb_ref)
    st_ref[...] = jnp.zeros_like(st_ref)

    def tile(i, _):
        at = pl.ds(pl.multiple_of(i * TILE, TILE), TILE)
        qp = qb_ref[at, :256]
        raw = dot(kb_ref[:, :256], qp, NT)
        s = jnp.where(kpos[...] <= query_positions(qp), raw * (SCALE * LOG2E), NEG)
        top = jnp.max(s, axis=0, keepdims=True)
        w = jnp.exp2(s - jnp.maximum(top, FLOOR))
        dp = dot(kb_ref[:, 256:], qb_ref[at, 256:], NT)
        st_ref[0:1, at] = top
        st_ref[1:2, at] = jnp.sum(w, axis=0, keepdims=True)
        st_ref[2:3, at] = jnp.sum(w * dp, axis=0, keepdims=True)
        return 0

    lax.fori_loop(0, QTOK // TILE, tile, 0)


def backward_kernel(qb_ref, kb_ref, sb_ref, dq_ref, dkv_ref, kpos, dk, dv):
    kpos[...] = key_positions(kb_ref)
    dk[...] = jnp.zeros_like(dk)
    dv[...] = jnp.zeros_like(dv)

    def tile(i, _):
        at = pl.ds(pl.multiple_of(i * TILE, TILE), TILE)
        tops = [sb_ref[j, 0:1, at] for j in range(NB)]
        top = jnp.maximum(jnp.maximum(tops[0], tops[1]), jnp.maximum(tops[2], tops[3]))
        fades = [jnp.exp2(t - top) for t in tops]
        total = sum(f * sb_ref[j, 1:2, at] for j, f in enumerate(fades))
        delta = sum(f * sb_ref[j, 2:3, at] for j, f in enumerate(fades)) / total
        lse = top + jnp.log(total) * LOG2E
        qp = qb_ref[at, :256]
        raw = dot(kb_ref[:, :256], qp, NT)
        s = jnp.where(kpos[...] <= query_positions(qp), raw * (SCALE * LOG2E), NEG)
        p = jnp.exp2(s - lse)
        grad = qb_ref[at, 256:]
        dp = dot(kb_ref[:, 256:], grad, NT)
        ds = (p * (dp - delta) * SCALE).astype(BF16)
        dv[...] += dot(p.astype(BF16), grad)
        dk[...] += dot(ds, qp)
        dq_ref[at, :] = dot(ds, kb_ref[:, :256], TN).astype(BF16)
        return 0

    lax.fori_loop(0, QTOK // TILE, tile, 0)
    dkv_ref[:, :256] = dk[...].astype(BF16)
    dkv_ref[:, 256:] = dv[...].astype(BF16)


def fold_kernel(rq_ref, rk_ref, cl_ref, ku_ref, vu_ref, dq_ref, lp_ref, up_ref):
    _, _, _, a, _, _ = coords()
    dq_ref[...] = sum(rq_ref[j].astype(F32) for j in range(NB)).astype(BF16)
    both = rk_ref[0].astype(F32) + rk_ref[1].astype(F32)
    g = jnp.concatenate([both[:, :128], both[:, 256:]], axis=1).astype(BF16)
    at = pl.ds(pl.multiple_of(a * 128, 128), 128)
    w = jnp.concatenate([ku_ref[:, at], vu_ref[:, at]], axis=1)
    lp_ref[:, :D_LAT] = dot(g, w, NT).astype(BF16)
    lp_ref[:, D_LAT:] = both[:, 128:256].astype(BF16)
    up_ref[...] = dot(cl_ref[...], g, TN).astype(BF16)


def own_kernel(rdq_ref, rlp_ref, rup_ref, qg_ref, ls_ref, us_ref):
    for h in range(NA):
        qg_ref[:, h * 192 : (h + 1) * 192] = rdq_ref[h, :, :192]
    ls_ref[...] = sum(rlp_ref[j].astype(F32) for j in range(NA)).astype(BF16)
    us_ref[...] = sum(rup_ref[j].astype(F32) for j in range(NB * NY)).astype(BF16)


def final_kernel(lh_ref, ug_ref, lat_ref, kug_ref, vug_ref):
    total = sum(lh_ref[j].astype(F32) for j in range(4))
    lat_ref[...] = total[:, : D_LAT + D_ROPE]
    for h in range(NA):
        for p in range(NB * NY):
            piece = ug_ref[h, p].astype(F32)
            kug_ref[p * 64 : (p + 1) * 64, h * 128 : (h + 1) * 128] = piece[:, :128]
            vug_ref[p * 64 : (p + 1) * 64, h * 128 : (h + 1) * 128] = piece[:, 128:]


def scatter_kernel(pq, pk, lat, qb, kb, cl, saq, raq, sak, rak, sal, ral, sbq, rbq, syk, ryk):
    _, _, y, a, b, dev = coords()
    meet(
        [dev((a + d) % NA, b, y) for d in (1, 2, 3)]
        + [dev(a, (b + d) % NB, y) for d in (1, 2, 3)]
        + [dev(a, b, 1 - y)]
    )
    done = []
    for d in (1, 3, 2):
        to = (a + d) % NA
        c = rcopy(pq.at[to], qb.at[b, a], saq.at[d - 1], raq.at[d - 1], dev(to, b, y))
        c.start()
        done.append(c)
    for d in (1, 3, 2):
        to = (a + d) % NA
        c = rcopy(pk.at[to], kb.at[y, a], sak.at[d - 1], rak.at[d - 1], dev(to, b, y))
        c.start()
        done.append(c)
    for d in (1, 3, 2):
        to = (a + d) % NB
        c = rcopy(pq.at[a], qb.at[b, a], sbq.at[d - 1, 0], rbq.at[d - 1, 0], dev(a, (b + d) % NB, y))
        c.start()
        done.append(c)
    c = rcopy(pk.at[a], kb.at[y, a], syk.at[0], ryk.at[0], dev(a, b, 1 - y))
    c.start()
    done.append(c)
    for d in (1, 3, 2):
        to = (a + d) % NA
        c = rcopy(lat, cl.at[a], sal.at[d - 1], ral.at[d - 1], dev(to, b, y))
        c.start()
        done.append(c)
    qb[b, a] = pq[a]
    kb[y, a] = pk[a]
    cl[a] = lat[...]
    for d in (1, 3, 2):
        src = (a + NA - d) % NA
        rcopy(qb.at[b, src], qb.at[b, src], saq.at[d - 1], raq.at[d - 1], dev(src, b, y)).wait_recv()
        for e in (1, 3, 2):
            c = rcopy(
                qb.at[b, src], qb.at[b, src], sbq.at[e - 1, d], rbq.at[e - 1, d], dev(a, (b + e) % NB, y)
            )
            c.start()
            done.append(c)
    for d in (1, 3, 2):
        src = (a + NA - d) % NA
        rcopy(kb.at[y, src], kb.at[y, src], sak.at[d - 1], rak.at[d - 1], dev(src, b, y)).wait_recv()
        c = rcopy(kb.at[y, src], kb.at[y, src], syk.at[d], ryk.at[d], dev(a, b, 1 - y))
        c.start()
        done.append(c)
    for d in range(NA):
        src = (a + NA - d) % NA
        for e in (1, 2, 3):
            sb = (b + NB - e) % NB
            rcopy(qb.at[sb, src], qb.at[sb, src], sbq.at[e - 1, d], rbq.at[e - 1, d], dev(a, sb, y)).wait_recv()
        other = kb.at[1 - y, src]
        rcopy(other, other, syk.at[d], ryk.at[d], dev(a, b, 1 - y)).wait_recv()
    for d in (1, 2, 3):
        src = (a + NA - d) % NA
        rcopy(cl.at[src], cl.at[src], sal.at[d - 1], ral.at[d - 1], dev(src, b, y)).wait_recv()
    for c in done:
        c.wait_send()


def stats_kernel(st, sb, send, recv):
    _, _, y, a, b, dev = coords()
    meet([dev(a, (b + d) % NB, y) for d in (1, 2, 3)])
    done = []
    for d in (2, 1, 3):
        c = rcopy(st, sb.at[b], send.at[d - 1], recv.at[d - 1], dev(a, (b + d) % NB, y))
        c.start()
        done.append(c)
    sb[b] = st[...]
    for d in (1, 3, 2):
        src = (b + NB - d) % NB
        rcopy(sb.at[src], sb.at[src], send.at[d - 1], recv.at[d - 1], dev(a, src, y)).wait_recv()
    for c in done:
        c.wait_send()


def partial_kernel(dq, dkv, rq, rk, sq, rcq, sk, rck):
    _, _, y, a, b, dev = coords()
    meet([dev(a, (b + d) % NB, y) for d in (1, 2, 3)] + [dev(a, b, 1 - y)])
    done = []
    c = rcopy(dkv.at[1 - y], rk.at[y], sk, rck, dev(a, b, 1 - y))
    c.start()
    done.append(c)
    for d in (2, 1, 3):
        to = (b + d) % NB
        c = rcopy(dq.at[to], rq.at[b], sq.at[d - 1], rcq.at[d - 1], dev(a, to, y))
        c.start()
        done.append(c)
    rq[b] = dq[b]
    rk[y] = dkv[y]
    for d in (1, 3, 2):
        src = (b + NB - d) % NB
        rcopy(rq.at[src], rq.at[src], sq.at[d - 1], rcq.at[d - 1], dev(a, src, y)).wait_recv()
    rcopy(rk.at[1 - y], rk.at[1 - y], sk, rck, dev(a, b, 1 - y)).wait_recv()
    for c in done:
        c.wait_send()


def return_kernel(dq, lp, up, rdq, rlp, rup, sq, rq, sl, rl, su, ru):
    _, _, y, a, b, dev = coords()
    others = [(e, f) for e in range(NB) for f in range(NY) if (e, f) != (0, 0)]
    meet(
        [dev((a + d) % NA, b, y) for d in (1, 2, 3)]
        + [dev(a, (b + e) % NB, (y + f) % NY) for e, f in others]
    )
    done = []
    mine = b * NY + y
    for d in (2, 1, 3):
        to = (a + d) % NA
        c = rcopy(lp.at[to], rlp.at[a], sl.at[d - 1], rl.at[d - 1], dev(to, b, y))
        c.start()
        done.append(c)
        c = rcopy(dq.at[to], rdq.at[a], sq.at[d - 1], rq.at[d - 1], dev(to, b, y))
        c.start()
        done.append(c)
    for i, (e, f) in enumerate(others):
        tb, ty = (b + e) % NB, (y + f) % NY
        c = rcopy(up.at[tb * NY + ty], rup.at[mine], su.at[i], ru.at[i], dev(a, tb, ty))
        c.start()
        done.append(c)
    rdq[a] = dq[a]
    rlp[a] = lp[a]
    rup[mine] = up[mine]
    for d in (1, 3, 2):
        src = (a + NA - d) % NA
        rcopy(rlp.at[src], rlp.at[src], sl.at[d - 1], rl.at[d - 1], dev(src, b, y)).wait_recv()
        rcopy(rdq.at[src], rdq.at[src], sq.at[d - 1], rq.at[d - 1], dev(src, b, y)).wait_recv()
    for i, (e, f) in enumerate(others):
        fb, fy = (b + NB - e) % NB, (y + f) % NY
        slot = rup.at[fb * NY + fy]
        rcopy(slot, slot, su.at[i], ru.at[i], dev(a, fb, fy)).wait_recv()
    for c in done:
        c.wait_send()


def share_kernel(ls, us, lh, ug, sl, rl, sy, ry, sb_, rb, sa_, ra):
    seq, head, y, a, b, dev = coords()
    meet(
        [(seq, (head + d) % 4) for d in (1, 2, 3)]
        + [dev((a + d) % NA, b, y) for d in (1, 2, 3)]
        + [dev(a, (b + d) % NB, y) for d in (1, 2, 3)]
        + [dev(a, b, 1 - y)]
    )
    done = []

    def go(src, dst, s, r, device):
        c = rcopy(src, dst, s, r, device)
        c.start()
        done.append(c)

    def landed(ref, s, r, device):
        rcopy(ref, ref, s, r, device).wait_recv()

    mine = b * NY + y
    go(us, ug.at[a, mine], sy, ry, dev(a, b, 1 - y))
    for e in (2, 1, 3):
        go(us, ug.at[a, mine], sb_.at[e - 1, 0], rb.at[e - 1, 0], dev(a, (b + e) % NB, y))
    for d in (2, 1, 3):
        go(us, ug.at[a, mine], sa_.at[d - 1, 0, 0], ra.at[d - 1, 0, 0], dev((a + d) % NA, b, y))
    for d in (1, 2, 3):
        go(ls, lh.at[head], sl.at[d - 1], rl.at[d - 1], (seq, (head + d) % 4))
    ug[a, mine] = us[...]
    lh[head] = ls[...]

    def pass_on(slot, e, f):
        for d in (2, 1, 3):
            go(slot, slot, sa_.at[d - 1, e, f], ra.at[d - 1, e, f], dev((a + d) % NA, b, y))

    across = ug.at[a, b * NY + 1 - y]
    landed(across, sy, ry, dev(a, b, 1 - y))
    for e in (2, 1, 3):
        go(across, across, sb_.at[e - 1, 1], rb.at[e - 1, 1], dev(a, (b + e) % NB, y))
    pass_on(across, 0, 1)
    for f in range(NY):
        for e in (1, 3, 2):
            fb = (b + NB - e) % NB
            slot = ug.at[a, fb * NY + (y + f) % NY]
            landed(slot, sb_.at[e - 1, f], rb.at[e - 1, f], dev(a, fb, y))
            pass_on(slot, e, f)
    for d in (1, 2, 3):
        fa = (a + NA - d) % NA
        for e in range(NB):
            for f in range(NY):
                slot = ug.at[fa, (b + NB - e) % NB * NY + (y + f) % NY]
                landed(slot, sa_.at[d - 1, e, f], ra.at[d - 1, e, f], dev(fa, b, y))
    for d in (1, 2, 3):
        fh = (head + 4 - d) % 4
        landed(lh.at[fh], sl.at[d - 1], rl.at[d - 1], (seq, fh))
    for c in done:
        c.wait_send()


def local(kernel, outs, scratch=(), specs=None):
    def call(*args):
        return pl.pallas_call(
            kernel,
            out_shape=outs,
            in_specs=specs or [VMEM] * len(args),
            out_specs=jax.tree.map(lambda _: VMEM, outs),
            scratch_shapes=list(scratch),
            compiler_params=compute_params(),
        )(*args)

    return call


def remote(kernel, which, outs, sems):
    def call(*args):
        return pl.pallas_call(
            kernel,
            out_shape=outs,
            in_specs=[VMEM] * len(args),
            out_specs=jax.tree.map(lambda _: VMEM, outs),
            scratch_shapes=[pltpu.SemaphoreType.DMA(s) if s else pltpu.SemaphoreType.DMA for s in sems],
            compiler_params=comm_params(which),
        )(*args)

    return call


def shards(queries, latents, key_up, value_up, out_grad, positions):
    pq, pk = local(
        prologue_kernel,
        (shape((NA, ROWS, QW)), shape((NA, ROWS, KW))),
        specs=[SMEM] + [VMEM] * 5,
    )(positions, queries, latents, key_up, value_up, out_grad)
    qb, kb, cl = remote(
        scatter_kernel,
        1,
        (shape((NB, NA, ROWS, QW)), shape((NY, NA, ROWS, KW)), shape((NA, ROWS, D_LAT))),
        [(3,), (3,), (3,), (3,), (3,), (3,), (3, 4), (3, 4), (4,), (4,)],
    )(pq, pk, latents[:, :D_LAT])
    qb = qb.reshape(QTOK, QW)
    kb = kb.reshape(KTOK, KW)
    st = local(forward_kernel, shape((8, QTOK), F32), [pltpu.VMEM((KTOK, TILE), F32)])(qb, kb)
    sb = remote(stats_kernel, 2, shape((NB, 8, QTOK), F32), [(3,), (3,)])(st)
    dq, dkv = local(
        backward_kernel,
        (shape((QTOK, 256)), shape((KTOK, KW))),
        [pltpu.VMEM((KTOK, TILE), F32), pltpu.VMEM((KTOK, 256), F32), pltpu.VMEM((KTOK, 128), F32)],
    )(qb, kb, sb)
    half = NA * ROWS
    rq, rk = remote(
        partial_kernel,
        3,
        (shape((NB, half, 256)), shape((NY, half, KW))),
        [(3,), (3,), (), ()],
    )(dq.reshape(NB, half, 256), dkv.reshape(NY, half, KW))
    dq, lp, up = local(
        fold_kernel, (shape((half, 256)), shape((half, LW)), shape((D_LAT, 256)))
    )(rq, rk, cl.reshape(half, D_LAT), key_up, value_up)
    rdq, rlp, rup = remote(
        return_kernel,
        4,
        (shape((NA, ROWS, 256)), shape((NA, ROWS, LW)), shape((NB * NY, 64, 256))),
        [(3,), (3,), (3,), (3,), (7,), (7,)],
    )(dq.reshape(NA, ROWS, 256), lp.reshape(NA, ROWS, LW), up.reshape(NB * NY, 64, 256))
    query_grad, ls, us = local(
        own_kernel, (shape((ROWS, 768)), shape((ROWS, LW)), shape((64, 256)))
    )(rdq, rlp, rup)
    lh, ug = remote(
        share_kernel,
        5,
        (shape((4, ROWS, LW)), shape((NA, NB * NY, 64, 256))),
        [(3,), (3,), (), (), (3, 2), (3, 2), (3, 4, 2), (3, 4, 2)],
    )(ls, us)
    latent_grad, key_up_grad, value_up_grad = local(
        final_kernel,
        (shape((ROWS, D_LAT + D_ROPE), F32), shape((D_LAT, 512), F32), shape((D_LAT, 512), F32)),
    )(lh, ug)
    return (query_grad, latent_grad, key_up_grad, value_up_grad)


def solution(mesh):
    in_specs = (
        P("seq", "head"),
        P("seq", None),
        P(None, "head"),
        P(None, "head"),
        P("seq", "head"),
        P("seq"),
    )
    out_specs = (P("seq", "head"), P("seq", None), P(None, "head"), P(None, "head"))
    return jax.shard_map(shards, mesh=mesh, in_specs=in_specs, out_specs=out_specs, check_vma=False)
```

```python
import math

import jax
import jax.numpy as jnp
from jax import lax
from jax.experimental import pallas as pl
from jax.experimental.pallas import tpu as pltpu
from jax.sharding import PartitionSpec as P


D_LAT = 512
D_ROPE = 64
D_NOPE = 128
D_V = 128
ROWS = 128
NA = 4
NB = 4
NY = 2
QW = 384
KW = 384
LW = 640
QTOK = NB * NA * ROWS
KTOK = NY * NA * ROWS
TILE = 256
NEG = -1e30
FLOOR = -1e29
SCALE = 1.0 / math.sqrt(D_NOPE + D_ROPE)
LOG2E = math.log2(math.e)
MESH = pl.DeviceIdType.MESH
F32 = jnp.float32
BF16 = jnp.bfloat16
VMEM = pl.BlockSpec(memory_space=pltpu.VMEM)
SMEM = pl.BlockSpec(memory_space=pltpu.SMEM)
NT = (((1,), (1,)), ((), ()))
TN = (((0,), (0,)), ((), ()))


def coords():
    seq = lax.axis_index("seq")
    head = lax.axis_index("head")
    core = head % 2
    y = seq // 16
    z = (seq // 4) % 4
    x = seq % 4
    a = x + core * (z - x)
    b = z + core * (x - z)
    sa = 1 + 3 * core
    sb = 4 - 3 * core

    def dev(a2, b2, y2):
        return (y2 * 16 + a2 * sa + b2 * sb, head)

    return seq, head, y, a, b, dev


def rcopy(src, dst, send, recv, device):
    return pltpu.make_async_remote_copy(
        src_ref=src, dst_ref=dst, send_sem=send, recv_sem=recv, device_id=device, device_id_type=MESH
    )


def dot(u, v, dims=(((1,), (0,)), ((), ()))):
    return lax.dot_general(u, v, dims, preferred_element_type=F32)


def shape(dims, dtype=BF16):
    return jax.ShapeDtypeStruct(dims, dtype)


def whole_kernel(
    pos_ref, q_ref, latt_ref, ku_ref, vu_ref, g_ref,
    qg_ref, lg_ref, kug_ref, vug_ref,
    pq, pk, qb, kb, cl, kpos, s_all, dp_all, stl, sb, rows, dqa, dqs, rq, dka, dva, dks, rk,
    lps, rlp, dqf, rdq, ups, rup, usk, usv, ugk, ugv, lsum, lhalf, rhalf, ly, ry_, lfin, rfin,
    s_aq, r_aq, s_ak, r_ak, s_al, r_al, s_bq, r_bq, s_yk, r_yk, s_st, r_st, s_dq, r_dq, s_dk, r_dk,
    s_lp, r_lp, s_qf, r_qf, s_up, r_up, s_ky, r_ky, s_kb, r_kb, s_ka, r_ka, s_vy, r_vy, s_va, r_va, s_vb, r_vb,
    s_h, r_h,
):
    seq, head, y, a, b, dev = coords()
    core = head % 2
    twin = (seq, head + 1 - 2 * core)
    far = (seq, (head + 2) % 4)
    across = dev(a, b, 1 - y)
    near = (1, 3, 2)
    others = [(e, f) for e in range(NB) for f in range(NY) if (e, f) != (0, 0)]

    barrier = pltpu.get_barrier_semaphore()
    for p in (
        [dev((a + d) % NA, b, y) for d in near]
        + [dev(a, (b + e) % NB, (y + f) % NY) for e, f in others]
        + [twin, far]
    ):
        pl.semaphore_signal(barrier, inc=1, device_id=p, device_id_type=MESH)

    done = []

    def go(src, dst, send, recv, device):
        c = rcopy(src, dst, send, recv, device)
        c.start()
        done.append(c)

    def landed(ref, send, recv):
        rcopy(ref, ref, send, recv, across).wait_recv()

    stripe = lax.shift_right_logical(pos_ref[0], 7).astype(F32)
    lane = lax.broadcasted_iota(jnp.int32, (ROWS, 128), 1)
    q_tail = jnp.where(lane == 64, stripe, 0.0)[:, 64:].astype(BF16)
    k_tail = jnp.where(lane == 65, stripe, 0.0)
    comp = latt_ref[:D_LAT, :]
    kn = dot(comp, ku_ref[...], TN).astype(BF16)
    vv = dot(comp, vu_ref[...], TN).astype(BF16)
    eye = (
        lax.broadcasted_iota(jnp.int32, (64, 128), 0) == lax.broadcasted_iota(jnp.int32, (64, 128), 1)
    ).astype(F32).astype(BF16)
    k_rest = (dot(latt_ref[D_LAT:, :], eye, TN) + k_tail).astype(BF16)
    for h in range(NA):
        pk[h, :, 0:128] = kn[:, h * 128 : (h + 1) * 128]
        pk[h, :, 128:256] = k_rest
        pk[h, :, 256:384] = vv[:, h * 128 : (h + 1) * 128]
        q = q_ref[:, h * 192 : (h + 1) * 192]
        pq[h, :, 0:128] = q[:, :128]
        pq[h, :, 128:256] = jnp.concatenate([q[:, 128:], q_tail], axis=1)
        pq[h, :, 256:384] = g_ref[:, h * 128 : (h + 1) * 128]

    pl.semaphore_wait(barrier, 3 + len(others) + 2)

    for d in near:
        to = (a + d) % NA
        go(pk.at[to], kb.at[0, a], s_ak.at[d - 1], r_ak.at[d - 1], dev(to, b, y))
        go(pq.at[to], qb.at[b, a], s_aq.at[d - 1], r_aq.at[d - 1], dev(to, b, y))
    go(pk.at[a], kb.at[1, a], s_yk.at[0], r_yk.at[0], across)
    for e in near:
        go(pq.at[a], qb.at[b, a], s_bq.at[e - 1, 0], r_bq.at[b, 0], dev(a, (b + e) % NB, y))
    for d in near:
        go(latt_ref.at[pl.ds(0, D_LAT)], cl.at[a], s_al.at[d - 1], r_al.at[d - 1], dev((a + d) % NA, b, y))
    qb[b, a] = pq[a]
    kb[0, a] = pk[a]
    cl[a] = comp
    for d in near:
        frm = (a + NA - d) % NA
        slot = kb.at[0, frm]
        landed(slot, s_ak.at[d - 1], r_ak.at[d - 1])
        go(slot, kb.at[1, frm], s_yk.at[d], r_yk.at[d], across)
        slot = qb.at[b, frm]
        landed(slot, s_aq.at[d - 1], r_aq.at[d - 1])
        for e in near:
            go(slot, slot, s_bq.at[e - 1, d], r_bq.at[b, d], dev(a, (b + e) % NB, y))
    for d in (0, 1, 3, 2):
        landed(kb.at[1, (a + NA - d) % NA], s_yk.at[d], r_yk.at[d])

    kp = kb[...].reshape(KTOK, KW)[:, :256]
    pick = (lax.broadcasted_iota(jnp.int32, (256, TILE), 0) == 193).astype(F32).astype(BF16)
    row = lax.broadcasted_iota(jnp.int32, (KTOK, TILE), 0) % ROWS
    kpos[...] = dot(kp, pick) * 128.0 + row.astype(F32)
    stl[...] = jnp.zeros_like(stl)
    pickq = (lax.broadcasted_iota(jnp.int32, (8, 256), 1) == 192).astype(F32).astype(BF16)
    col = lax.broadcasted_iota(jnp.int32, (1, TILE), 1) % ROWS
    for j in range(NB):

        @pl.when(b != j)
        def _():
            for d in range(NA):
                landed(qb.at[j, (a + NA - d) % NA], s_bq.at[0, d], r_bq.at[j, d])

        for t in range(2):
            at = slice(t * TILE, (t + 1) * TILE)
            two = qb[j, 2 * t : 2 * t + 2].reshape(TILE, QW)
            qp = two[:, :256]
            keys = kb[...].reshape(KTOK, KW)
            qpos = dot(pickq, qp, NT)[0:1, :] * 128.0 + col.astype(F32)
            raw = dot(keys[:, :256], qp, NT)
            s = jnp.where(kpos[...] <= qpos, raw * (SCALE * LOG2E), NEG)
            s_all[j, :, at] = s
            top = jnp.max(s, axis=0, keepdims=True)
            w = jnp.exp2(s - jnp.maximum(top, FLOOR))
            dp = dot(keys[:, 256:], two[:, 256:], NT)
            dp_all[j, :, at] = dp
            stl[j, 0:1, at] = top
            stl[j, 1:2, at] = jnp.sum(w, axis=0, keepdims=True)
            stl[j, 2:3, at] = jnp.sum(w * dp, axis=0, keepdims=True)
        for e in near:
            go(stl.at[j], sb.at[j, b], s_st.at[e - 1, j], r_st.at[j, b], dev(a, (b + e) % NB, y))

    half = NA * ROWS
    for j in range(NB):
        sb[j, b] = stl[j]
        for i in range(NB):

            @pl.when(b != i)
            def _():
                landed(sb.at[j, i], s_st.at[0, j], r_st.at[j, i])

        tops = [sb[j, i, 0:1, :] for i in range(NB)]
        top = jnp.maximum(jnp.maximum(tops[0], tops[1]), jnp.maximum(tops[2], tops[3]))
        fades = [jnp.exp2(t - top) for t in tops]
        total = sum(f * sb[j, i, 1:2, :] for i, f in enumerate(fades))
        rows[j, 1:2, :] = sum(f * sb[j, i, 2:3, :] for i, f in enumerate(fades)) / total
        rows[j, 0:1, :] = top + jnp.log(total) * LOG2E

    for k in (1, 0):
        ks = slice(k * half, (k + 1) * half)
        for j in range(NB):
            qall = qb[j].reshape(half, QW)
            keys = kb[k].reshape(half, KW)
            p = jnp.exp2(s_all[j, ks, :] - rows[j, 0:1, :])
            ds = (p * (dp_all[j, ks, :] - rows[j, 1:2, :]) * SCALE).astype(BF16)
            dv = dot(p.astype(BF16), qall[:, 256:])
            dk = dot(ds, qall[:, :256])
            dq = dot(ds, keys[:, :256], TN)
            if j == 0:
                dva[ks, :] = dv
                dka[ks, :] = dk
            else:
                dva[ks, :] += dv
                dka[ks, :] += dk
            if k == 1:
                dqa[j] = dq
            else:
                dqs[j] = (dqa[j] + dq).astype(BF16)

                @pl.when(b != j)
                def _():
                    rcopy(dqs.at[j], rq.at[b], s_dq.at[j], r_dq.at[b], dev(a, j, y)).start()

        if k == 1:
            dks[:, :256] = dka[half:, :].astype(BF16)
            dks[:, 256:] = dva[half:, :].astype(BF16)
            go(dks, rk, s_dk, r_dk, across)

    for d in near:
        landed(cl.at[(a + NA - d) % NA], s_al.at[d - 1], r_al.at[d - 1])
    landed(rk, s_dk, r_dk)
    dk = dka[:half, :] + rk[:, :256].astype(F32)
    dv = dva[:half, :] + rk[:, 256:].astype(F32)
    g = jnp.concatenate([dk[:, :128], dv], axis=1).astype(BF16)
    mine_cols = pl.ds(pl.multiple_of(a * 128, 128), 128)
    w = jnp.concatenate([ku_ref[:, mine_cols], vu_ref[:, mine_cols]], axis=1)
    comps = jnp.concatenate([cl[i] for i in range(NA)], axis=1)
    up = dot(comps, g)
    for i in range(NB * NY):
        ups[i] = up[i * 64 : (i + 1) * 64, :].astype(BF16)
    lp = dot(w, g, NT)
    rope = dot(eye, dk[:, 128:].astype(BF16), NT)
    for i in range(NA):
        lps[i, :D_LAT, :] = lp[:, i * 128 : (i + 1) * 128].astype(BF16)
        lps[i, D_LAT:, :] = rope[:, i * 128 : (i + 1) * 128].astype(BF16)
    mine = b * NY + y
    for i, (e, f) in enumerate(others):
        tb, ty = (b + e) % NB, (y + f) % NY
        go(ups.at[tb * NY + ty], rup.at[mine], s_up.at[i], r_up.at[i], dev(a, tb, ty))
    for d in near:
        go(lps.at[(a + d) % NA], rlp.at[a], s_lp.at[d - 1], r_lp.at[d - 1], dev((a + d) % NA, b, y))
    rup[mine] = ups[mine]
    rlp[a] = lps[a]

    rq[b] = dqs[b]
    for j in range(NB):

        @pl.when(b != j)
        def _():
            landed(rq.at[j], s_dq.at[j], r_dq.at[j])

    dqf[...] = sum(rq[j].astype(F32) for j in range(NB)).astype(BF16).reshape(NA, ROWS, 256)
    for d in near:
        go(dqf.at[(a + d) % NA], rdq.at[a], s_qf.at[d - 1], r_qf.at[d - 1], dev((a + d) % NA, b, y))
    rdq[a] = dqf[a]

    for i, (e, f) in enumerate(others):
        fb, fy = (b + NB - e) % NB, (y + f) % NY
        landed(rup.at[fb * NY + fy], s_up.at[i], r_up.at[i])
    us = sum(rup[i].astype(F32) for i in range(NB * NY)).astype(BF16)
    usk[...] = us[:, :128]
    usv[...] = us[:, 128:]
    ugk[a, mine] = us[:, :128]
    ugv[a, mine] = us[:, 128:]
    go(usk, ugk.at[a, mine], s_ky, r_ky, across)
    go(usv, ugv.at[a, mine], s_vy, r_vy, across)
    for e in near:
        go(usk, ugk.at[a, mine], s_kb.at[e - 1, 0], r_kb.at[e - 1, 0], dev(a, (b + e) % NB, y))
    for d in near:
        go(usv, ugv.at[a, mine], s_va.at[d - 1, 0], r_va.at[d - 1, 0], dev((a + d) % NA, b, y))
    for d in near:
        go(usk, ugk.at[a, mine], s_ka.at[d - 1, 0, 0], r_ka.at[d - 1, 0, 0], dev((a + d) % NA, b, y))
    for e in near:
        go(usv, ugv.at[a, mine], s_vb.at[e - 1, 0, 0], r_vb.at[e - 1, 0, 0], dev(a, (b + e) % NB, y))

    for d in near:
        landed(rlp.at[(a + NA - d) % NA], s_lp.at[d - 1], r_lp.at[d - 1])
    lsum[...] = sum(rlp[i].astype(F32) for i in range(NA)).reshape(2, 288, 128)
    lhalf[...] = lsum[1 - core].astype(BF16)
    go(lhalf, rhalf, s_h.at[0], r_h.at[0], twin)

    def k_over_a(slot, e, f):
        for d in near:
            go(slot, slot, s_ka.at[d - 1, e, f], r_ka.at[d - 1, e, f], dev((a + d) % NA, b, y))

    def v_over_b(slot, d, f):
        for e in near:
            go(slot, slot, s_vb.at[e - 1, d, f], r_vb.at[e - 1, d, f], dev(a, (b + e) % NB, y))

    other = b * NY + 1 - y
    landed(ugk.at[a, other], s_ky, r_ky)
    for e in near:
        go(ugk.at[a, other], ugk.at[a, other], s_kb.at[e - 1, 1], r_kb.at[e - 1, 1], dev(a, (b + e) % NB, y))
    landed(ugv.at[a, other], s_vy, r_vy)
    for d in near:
        go(ugv.at[a, other], ugv.at[a, other], s_va.at[d - 1, 1], r_va.at[d - 1, 1], dev((a + d) % NA, b, y))
    k_over_a(ugk.at[a, other], 0, 1)
    v_over_b(ugv.at[a, other], 0, 1)

    landed(rhalf, s_h.at[0], r_h.at[0])
    both = lsum[core] + rhalf[...].astype(F32)
    ly[...] = both.astype(BF16)
    go(ly, ry_, s_h.at[1], r_h.at[1], far)

    for f in range(NY):
        for e in near:
            slot = ugk.at[a, (b + NB - e) % NB * NY + (y + f) % NY]
            landed(slot, s_kb.at[e - 1, f], r_kb.at[e - 1, f])
            k_over_a(slot, e, f)
            slot = ugv.at[(a + NA - e) % NA, b * NY + (y + f) % NY]
            landed(slot, s_va.at[e - 1, f], r_va.at[e - 1, f])
            v_over_b(slot, e, f)

    landed(ry_, s_h.at[1], r_h.at[1])
    whole = ly[...].astype(F32) + ry_[...].astype(F32)
    lfin[...] = whole
    go(lfin, rfin, s_h.at[2], r_h.at[2], twin)

    for d in near:
        landed(rdq.at[(a + NA - d) % NA], s_qf.at[d - 1], r_qf.at[d - 1])
    for h in range(NA):
        qg_ref[:, h * 192 : (h + 1) * 192] = rdq[h, :, :192]

    landed(rfin, s_h.at[2], r_h.at[2])
    lg_ref[core] = lfin[...]
    lg_ref[1 - core] = rfin[...]

    for d in near:
        fa = (a + NA - d) % NA
        for e in range(NB):
            for f in range(NY):
                landed(
                    ugk.at[fa, (b + NB - e) % NB * NY + (y + f) % NY],
                    s_ka.at[d - 1, e, f], r_ka.at[d - 1, e, f],
                )
                landed(
                    ugv.at[(a + NA - e) % NA, (b + NB - d) % NB * NY + (y + f) % NY],
                    s_vb.at[d - 1, e, f], r_vb.at[d - 1, e, f],
                )
    for h in range(NA):
        kug_ref[:, h * 128 : (h + 1) * 128] = ugk[h].reshape(D_LAT, 128)
        vug_ref[:, h * 128 : (h + 1) * 128] = ugv[h].reshape(D_LAT, 128)
    for j in range(NB):

        @pl.when(b != j)
        def _():
            rcopy(dqs.at[j], dqs.at[j], s_dq.at[j], r_dq.at[j], across).wait_send()

    for c in done:
        c.wait_send()


def shards(queries, latents, key_up, value_up, out_grad, positions):
    half = NA * ROWS
    dma = pltpu.SemaphoreType.DMA
    scratch = [
        pltpu.VMEM((NA, ROWS, QW), BF16),
        pltpu.VMEM((NA, ROWS, KW), BF16),
        pltpu.VMEM((NB, NA, ROWS, QW), BF16),
        pltpu.VMEM((NY, NA, ROWS, KW), BF16),
        pltpu.VMEM((NA, D_LAT, ROWS), BF16),
        pltpu.VMEM((KTOK, TILE), F32),
        pltpu.VMEM((NB, KTOK, half), F32),
        pltpu.VMEM((NB, KTOK, half), F32),
        pltpu.VMEM((NB, 8, half), F32),
        pltpu.VMEM((NB, NB, 8, half), F32),
        pltpu.VMEM((NB, 8, half), F32),
        pltpu.VMEM((NB, half, 256), F32),
        pltpu.VMEM((NB, half, 256), BF16),
        pltpu.VMEM((NB, half, 256), BF16),
        pltpu.VMEM((KTOK, 256), F32),
        pltpu.VMEM((KTOK, 128), F32),
        pltpu.VMEM((half, KW), BF16),
        pltpu.VMEM((half, KW), BF16),
        pltpu.VMEM((NA, 576, ROWS), BF16),
        pltpu.VMEM((NA, 576, ROWS), BF16),
        pltpu.VMEM((NA, ROWS, 256), BF16),
        pltpu.VMEM((NA, ROWS, 256), BF16),
        pltpu.VMEM((NB * NY, 64, 256), BF16),
        pltpu.VMEM((NB * NY, 64, 256), BF16),
        pltpu.VMEM((64, 128), BF16),
        pltpu.VMEM((64, 128), BF16),
        pltpu.VMEM((NA, NB * NY, 64, 128), BF16),
        pltpu.VMEM((NA, NB * NY, 64, 128), BF16),
        pltpu.VMEM((2, 288, ROWS), F32),
        pltpu.VMEM((288, ROWS), BF16),
        pltpu.VMEM((288, ROWS), BF16),
        pltpu.VMEM((288, ROWS), BF16),
        pltpu.VMEM((288, ROWS), BF16),
        pltpu.VMEM((288, ROWS), F32),
        pltpu.VMEM((288, ROWS), F32),
    ]
    sems = [
        dma((3,)), dma((3,)), dma((3,)), dma((3,)), dma((3,)), dma((3,)),
        dma((3, 4)), dma((4, 4)), dma((4,)), dma((4,)),
        dma((3, 4)), dma((4, 4)), dma((4,)), dma((4,)), dma, dma,
        dma((3,)), dma((3,)), dma((3,)), dma((3,)), dma((7,)), dma((7,)),
        dma, dma, dma((3, 2)), dma((3, 2)), dma((3, 4, 2)), dma((3, 4, 2)),
        dma, dma, dma((3, 2)), dma((3, 2)), dma((3, 4, 2)), dma((3, 4, 2)),
        dma((3,)), dma((3,)),
    ]
    qg, lg, kug, vug = pl.pallas_call(
        whole_kernel,
        out_shape=(
            shape((ROWS, 768)),
            shape((2, 288, ROWS), F32),
            shape((D_LAT, 512)),
            shape((D_LAT, 512)),
        ),
        in_specs=[SMEM] + [VMEM] * 5,
        out_specs=(VMEM,) * 4,
        scratch_shapes=scratch + sems,
        compiler_params=pltpu.CompilerParams(
            collective_id=0, has_side_effects=True, vmem_limit_bytes=58 * 1024 * 1024
        ),
    )(positions, queries, latents.T, key_up, value_up, out_grad)
    return (qg, lg.reshape(576, ROWS).T, kug.astype(F32), vug.astype(F32))


def solution(mesh):
    in_specs = (
        P("seq", "head"),
        P("seq", None),
        P(None, "head"),
        P(None, "head"),
        P("seq", "head"),
        P("seq"),
    )
    out_specs = (P("seq", "head"), P("seq", None), P(None, "head"), P(None, "head"))
    return jax.shard_map(shards, mesh=mesh, in_specs=in_specs, out_specs=out_specs, check_vma=False)
```

```python
import math

import jax
import jax.numpy as jnp
from jax import lax
from jax.experimental import pallas as pl
from jax.experimental.pallas import tpu as pltpu
from jax.sharding import PartitionSpec as P


D_LAT = 512
D_ROPE = 64
D_NOPE = 128
D_V = 128
ROWS = 128
NA = 4
NB = 4
NY = 2
QW = 384
KW = 384
LW = 640
QTOK = NB * NA * ROWS
KTOK = NY * NA * ROWS
TILE = 256
NEG = -1e30
LIMIT = 52
FLOOR = -1e29
SCALE = 1.0 / math.sqrt(D_NOPE + D_ROPE)
LOG2E = math.log2(math.e)
MESH = pl.DeviceIdType.MESH
F32 = jnp.float32
BF16 = jnp.bfloat16
VMEM = pl.BlockSpec(memory_space=pltpu.VMEM)
SMEM = pl.BlockSpec(memory_space=pltpu.SMEM)
NT = (((1,), (1,)), ((), ()))
TN = (((0,), (0,)), ((), ()))


def coords():
    seq = lax.axis_index("seq")
    head = lax.axis_index("head")
    core = head % 2
    y = seq // 16
    z = (seq // 4) % 4
    x = seq % 4
    a = x + core * (z - x)
    b = z + core * (x - z)
    sa = 1 + 3 * core
    sb = 4 - 3 * core

    def dev(a2, b2, y2):
        return (y2 * 16 + a2 * sa + b2 * sb, head)

    return seq, head, y, a, b, dev


def rcopy(src, dst, send, recv, device):
    return pltpu.make_async_remote_copy(
        src_ref=src, dst_ref=dst, send_sem=send, recv_sem=recv, device_id=device, device_id_type=MESH
    )


def dot(u, v, dims=(((1,), (0,)), ((), ()))):
    return lax.dot_general(u, v, dims, preferred_element_type=F32)


def shape(dims, dtype=BF16):
    return jax.ShapeDtypeStruct(dims, dtype)


def whole_kernel(
    pos_ref, q_hbm, latt_hbm, ku_hbm, vu_hbm, g_hbm,
    qg_ref, lg_ref, ugk, ugv,
    q_ref, latt_ref, ku_ref, vu_ref, g_ref,
    pq, pk, qb, kb, cl, kpos, s_all, dp_all, stl, sb, rows, ds_all, dqs, rq, dka, dva, gs0, gs1, rg0, rg1,
    dqf, rdq, ups, rup, usk, usv, lsum, lhalf, rhalf, hs, rh, lfin, rfin,
    s_in, s_aq, r_aq, s_ak, r_ak, s_al, r_al, s_bq, r_bq, s_yk, r_yk, s_yl, r_yl, s_st, r_st, s_dq, r_dq,
    s_g0, r_g0, s_g1, r_g1, s_qf, r_qf, s_up, r_up,
    s_ky, r_ky, s_kb, r_kb, s_ka, r_ka, s_vy, r_vy, s_va, r_va, s_vb, r_vb, s_h, r_h,
):
    seq, head, y, a, b, dev = coords()
    core = head % 2
    twin = (seq, head + 1 - 2 * core)
    far = (seq, (head + 2) % 4)
    across = dev(a, b, 1 - y)
    corner = (across[0], (head + 2) % 4)
    near = (1, 3, 2)
    others = [(e, f) for e in range(NB) for f in range(NY) if (e, f) != (0, 0)]

    barrier = pltpu.get_barrier_semaphore()
    for p in (
        [dev((a + d) % NA, b, y) for d in near]
        + [dev(a, (b + e) % NB, (y + f) % NY) for e, f in others]
        + [twin, far, corner]
    ):
        pl.semaphore_signal(barrier, inc=1, device_id=p, device_id_type=MESH)

    done = []

    def go(src, dst, send, recv, device):
        c = rcopy(src, dst, send, recv, device)
        c.start()
        done.append(c)

    def landed(ref, send, recv):
        rcopy(ref, ref, send, recv, across).wait_recv()

    loads = [
        pltpu.make_async_copy(src, dst, s_in.at[i])
        for i, (src, dst) in enumerate(
            [(latt_hbm, latt_ref), (ku_hbm, ku_ref), (vu_hbm, vu_ref), (q_hbm, q_ref), (g_hbm, g_ref)]
        )
    ]
    for c in loads:
        c.start()
    for c in loads:
        c.wait()

    stripe = lax.shift_right_logical(pos_ref[0], 7).astype(F32)
    lane = lax.broadcasted_iota(jnp.int32, (ROWS, 128), 1)
    q_tail = jnp.where(lane == 64, stripe, 0.0)[:, 64:].astype(BF16)
    k_tail = jnp.where(lane == 65, stripe, 0.0)
    comp = latt_ref[:D_LAT, :]
    kn = dot(comp, ku_ref[...], TN).astype(BF16)
    vv = dot(comp, vu_ref[...], TN).astype(BF16)
    eye = (
        lax.broadcasted_iota(jnp.int32, (64, 128), 0) == lax.broadcasted_iota(jnp.int32, (64, 128), 1)
    ).astype(F32).astype(BF16)
    k_rest = (dot(latt_ref[D_LAT:, :], eye, TN) + k_tail).astype(BF16)
    for h in range(NA):
        pk[h, :, 0:128] = kn[:, h * 128 : (h + 1) * 128]
        pk[h, :, 128:256] = k_rest
        pk[h, :, 256:384] = vv[:, h * 128 : (h + 1) * 128]
        q = q_ref[:, h * 192 : (h + 1) * 192]
        pq[h, :, 0:128] = q[:, :128]
        pq[h, :, 128:256] = jnp.concatenate([q[:, 128:], q_tail], axis=1)
        pq[h, :, 256:384] = g_ref[:, h * 128 : (h + 1) * 128]

    pl.semaphore_wait(barrier, 3 + len(others) + 3)

    for d in near:
        to = (a + d) % NA
        go(pk.at[to], kb.at[0, a], s_ak.at[d - 1], r_ak.at[d - 1], dev(to, b, y))
        go(pq.at[to], qb.at[b, a], s_aq.at[d - 1], r_aq.at[d - 1], dev(to, b, y))
    go(pk.at[a], kb.at[1, a], s_yk.at[0], r_yk.at[0], across)
    for e in near:
        go(pq.at[a], qb.at[b, a], s_bq.at[e - 1, 0], r_bq.at[b, 0], dev(a, (b + e) % NB, y))
    for d in near:
        go(latt_ref.at[pl.ds(0, D_LAT)], cl.at[0, a], s_al.at[d - 1], r_al.at[d - 1], dev((a + d) % NA, b, y))
    qb[b, a] = pq[a]
    kb[0, a] = pk[a]
    cl[0, a] = comp
    for d in near:
        frm = (a + NA - d) % NA
        slot = kb.at[0, frm]
        landed(slot, s_ak.at[d - 1], r_ak.at[d - 1])
        go(slot, kb.at[1, frm], s_yk.at[d], r_yk.at[d], across)
        slot = qb.at[b, frm]
        landed(slot, s_aq.at[d - 1], r_aq.at[d - 1])
        for e in near:
            go(slot, slot, s_bq.at[e - 1, d], r_bq.at[b, d], dev(a, (b + e) % NB, y))
    for d in (0, 1, 3, 2):
        landed(kb.at[1, (a + NA - d) % NA], s_yk.at[d], r_yk.at[d])

    kp = kb[...].reshape(KTOK, KW)[:, :256]
    pick = (lax.broadcasted_iota(jnp.int32, (256, TILE), 0) == 193).astype(F32).astype(BF16)
    row = lax.broadcasted_iota(jnp.int32, (KTOK, TILE), 0) % ROWS
    kpos[...] = dot(kp, pick) * 128.0 + row.astype(F32)
    stl[...] = jnp.zeros_like(stl)
    pickq = (lax.broadcasted_iota(jnp.int32, (8, 256), 1) == 192).astype(F32).astype(BF16)
    col = lax.broadcasted_iota(jnp.int32, (1, TILE), 1) % ROWS
    for j in range(NB):

        @pl.when(b != j)
        def _():
            for d in range(NA):
                landed(qb.at[j, (a + NA - d) % NA], s_bq.at[0, d], r_bq.at[j, d])

        if j == 2:
            go(latt_ref.at[pl.ds(0, D_LAT)], cl.at[1, a], s_yl.at[0], r_yl.at[0], across)
            for d in near:
                slot = cl.at[0, (a + NA - d) % NA]
                landed(slot, s_al.at[d - 1], r_al.at[d - 1])
                go(slot, cl.at[1, (a + NA - d) % NA], s_yl.at[d], r_yl.at[d], across)
        for t in range(2):
            at = slice(t * TILE, (t + 1) * TILE)
            two = qb[j, 2 * t : 2 * t + 2].reshape(TILE, QW)
            qp = two[:, :256]
            keys = kb[...].reshape(KTOK, KW)
            qpos = dot(pickq, qp, NT)[0:1, :] * 128.0 + col.astype(F32)
            raw = dot(keys[:, :256], qp, NT)
            s = jnp.where(kpos[...] <= qpos, raw * (SCALE * LOG2E), NEG)
            s_all[j, :, at] = s
            top = jnp.max(s, axis=0, keepdims=True)
            w = jnp.exp2(s - jnp.maximum(top, FLOOR))
            dp = dot(keys[:, 256:], two[:, 256:], NT)
            dp_all[j, :, at] = dp
            stl[j, 0:1, at] = top
            stl[j, 1:2, at] = jnp.sum(w, axis=0, keepdims=True)
            stl[j, 2:3, at] = jnp.sum(w * dp, axis=0, keepdims=True)
        for e in near:
            go(stl.at[j], sb.at[j, b], s_st.at[e - 1, j], r_st.at[j, b], dev(a, (b + e) % NB, y))

    half = NA * ROWS
    for k in (1, 0):
        ks = slice(k * half, (k + 1) * half)
        for j in range(NB):
            if k == 1:
                sb[j, b] = stl[j]
                for i in range(NB):

                    @pl.when(b != i)
                    def _():
                        landed(sb.at[j, i], s_st.at[0, j], r_st.at[j, i])

                tops = [sb[j, i, 0:1, :] for i in range(NB)]
                top = jnp.maximum(jnp.maximum(tops[0], tops[1]), jnp.maximum(tops[2], tops[3]))
                fades = [jnp.exp2(t - top) for t in tops]
                total = sum(f * sb[j, i, 1:2, :] for i, f in enumerate(fades))
                rows[j, 1:2, :] = sum(f * sb[j, i, 2:3, :] for i, f in enumerate(fades)) / total
                rows[j, 0:1, :] = top + jnp.log(total) * LOG2E
            qall = qb[j].reshape(half, QW)
            p = jnp.exp2(s_all[j, ks, :] - rows[j, 0:1, :])
            ds = (p * (dp_all[j, ks, :] - rows[j, 1:2, :]) * SCALE).astype(BF16)
            ds_all[j, ks, :] = ds
            dv = dot(p.astype(BF16), qall[:, 256:])
            dk = dot(ds, qall[:, :256])
            if j == 0:
                dva[ks, :] = dv
                dka[ks, :] = dk
            else:
                dva[ks, :] += dv
                dka[ks, :] += dk
        if k == 1:
            for i in range(NA):
                at = slice(half + i * ROWS, half + (i + 1) * ROWS)
                gs1[i, :, :128] = dka[at, :128].astype(BF16)
                gs1[i, :, 128:] = dva[at, :].astype(BF16)
            for d in near:
                go(gs1.at[(a + d) % NA], rg1.at[a], s_g1.at[d - 1], r_g1.at[d - 1], dev((a + d) % NA, b, y))
        else:
            for i in range(NA):
                at = slice(i * ROWS, (i + 1) * ROWS)
                at1 = slice(half + i * ROWS, half + (i + 1) * ROWS)
                gs0[i, :, :128] = dka[at, :128].astype(BF16)
                gs0[i, :, 128:256] = dva[at, :].astype(BF16)
                gs0[i, :, 256:] = jnp.concatenate([dka[at, 128:192], dka[at1, 128:192]], axis=1).astype(BF16)
            for d in near:
                go(gs0.at[(a + d) % NA], rg0.at[a], s_g0.at[d - 1], r_g0.at[d - 1], dev((a + d) % NA, b, y))

    for d in (0, 1, 3, 2):
        landed(cl.at[1, (a + NA - d) % NA], s_yl.at[d], r_yl.at[d])
    g = jnp.concatenate([dka[:, :128], dva[...]], axis=1).astype(BF16)
    comps = jnp.concatenate([cl[k, i] for k in range(NY) for i in range(NA)], axis=1)
    up = dot(comps, g)
    for i in range(NB * NY):
        ups[i] = up[i * 64 : (i + 1) * 64, :].astype(BF16)
    mine = b * NY + y
    for i, (e, f) in enumerate(others):
        tb, ty = (b + e) % NB, (y + f) % NY
        go(ups.at[tb * NY + ty], rup.at[mine], s_up.at[i], r_up.at[i], dev(a, tb, ty))
    rup[mine] = ups[mine]

    keys = kb[...].reshape(KTOK, KW)
    for j in range(NB):
        dq = dot(ds_all[j], keys[:, :256], TN).astype(BF16)
        for i in range(NA):
            part = dq[i * ROWS : (i + 1) * ROWS, :]
            dqs[j, i, :ROWS, :] = part[:, :128]
            dqs[j, i, ROWS:, :] = jnp.concatenate([part[:64, 128:192], part[64:, 128:192]], axis=1)

        @pl.when(b != j)
        def _():
            rcopy(dqs.at[j], rq.at[b], s_dq.at[j], r_dq.at[b], dev(a, j, y)).start()

    rq[b] = dqs[b]
    rg0[a] = gs0[a]
    rg1[a] = gs1[a]

    for d in near:
        landed(rg1.at[(a + NA - d) % NA], s_g1.at[d - 1], r_g1.at[d - 1])
        landed(rg0.at[(a + NA - d) % NA], s_g0.at[d - 1], r_g0.at[d - 1])
    dk_all = jnp.concatenate(
        [jnp.concatenate([r[h, :, :128] for h in range(NA)], axis=1) for r in (rg0, rg1)], axis=0
    )
    dv_all = jnp.concatenate(
        [jnp.concatenate([r[h, :, 128:256] for h in range(NA)], axis=1) for r in (rg0, rg1)], axis=0
    )
    lp = dot(ku_ref[...], dk_all, NT) + dot(vu_ref[...], dv_all, NT)
    rope = sum(rg0[h, :, 256:].astype(F32) for h in range(NA)).T
    for k in range(NY):
        whole = jnp.concatenate([lp[:, k * 128 : (k + 1) * 128], rope[k * 64 : (k + 1) * 64, :]], axis=0)
        lsum[k] = whole.reshape(2, 288, ROWS)
    for k in range(NY):
        lhalf[k] = lsum[k, 1 - core].astype(BF16)
    go(lhalf, rhalf, s_h.at[0], r_h.at[0], twin)

    for i, (e, f) in enumerate(others):
        fb, fy = (b + NB - e) % NB, (y + f) % NY
        landed(rup.at[fb * NY + fy], s_up.at[i], r_up.at[i])
    us = sum(rup[i].astype(F32) for i in range(NB * NY)).astype(BF16)
    usk[...] = us[:, :128]
    usv[...] = us[:, 128:]
    ugk[a, mine] = us[:, :128]
    ugv[a, mine] = us[:, 128:]
    go(usk, ugk.at[a, mine], s_ky, r_ky, across)
    go(usv, ugv.at[a, mine], s_vy, r_vy, across)
    for e in near:
        go(usk, ugk.at[a, mine], s_kb.at[e - 1, 0], r_kb.at[e - 1, 0], dev(a, (b + e) % NB, y))
    for d in near:
        go(usv, ugv.at[a, mine], s_va.at[d - 1, 0], r_va.at[d - 1, 0], dev((a + d) % NA, b, y))
    for d in near:
        go(usk, ugk.at[a, mine], s_ka.at[d - 1, 0, 0], r_ka.at[d - 1, 0, 0], dev((a + d) % NA, b, y))
    for e in near:
        go(usv, ugv.at[a, mine], s_vb.at[e - 1, 0, 0], r_vb.at[e - 1, 0, 0], dev(a, (b + e) % NB, y))

    landed(rhalf, s_h.at[0], r_h.at[0])
    for k in range(NY):
        hs[k] = (lsum[k, core] + rhalf[k].astype(F32)).astype(BF16)
    go(hs.at[0], rh.at[0], s_h.at[1], r_h.at[1], far)
    go(hs.at[1], rh.at[1], s_h.at[2], r_h.at[2], across)
    go(hs.at[1], rh.at[2], s_h.at[3], r_h.at[3], corner)

    def k_over_a(slot, e, f):
        for d in near:
            go(slot, slot, s_ka.at[d - 1, e, f], r_ka.at[d - 1, e, f], dev((a + d) % NA, b, y))

    def v_over_b(slot, d, f):
        for e in near:
            go(slot, slot, s_vb.at[e - 1, d, f], r_vb.at[e - 1, d, f], dev(a, (b + e) % NB, y))

    other = b * NY + 1 - y
    landed(ugk.at[a, other], s_ky, r_ky)
    for e in near:
        go(ugk.at[a, other], ugk.at[a, other], s_kb.at[e - 1, 1], r_kb.at[e - 1, 1], dev(a, (b + e) % NB, y))
    landed(ugv.at[a, other], s_vy, r_vy)
    for d in near:
        go(ugv.at[a, other], ugv.at[a, other], s_va.at[d - 1, 1], r_va.at[d - 1, 1], dev((a + d) % NA, b, y))
    k_over_a(ugk.at[a, other], 0, 1)
    v_over_b(ugv.at[a, other], 0, 1)

    for j in range(NB):

        @pl.when(b != j)
        def _():
            landed(rq.at[j], s_dq.at[j], r_dq.at[j])

    dqf[...] = sum(rq[j].astype(F32) for j in range(NB)).astype(BF16)
    for d in near:
        go(dqf.at[(a + d) % NA], rdq.at[a], s_qf.at[d - 1], r_qf.at[d - 1], dev((a + d) % NA, b, y))
    rdq[a] = dqf[a]

    for f in range(NY):
        for e in near:
            slot = ugk.at[a, (b + NB - e) % NB * NY + (y + f) % NY]
            landed(slot, s_kb.at[e - 1, f], r_kb.at[e - 1, f])
            k_over_a(slot, e, f)
            slot = ugv.at[(a + NA - e) % NA, b * NY + (y + f) % NY]
            landed(slot, s_va.at[e - 1, f], r_va.at[e - 1, f])
            v_over_b(slot, e, f)

    for i in range(3):
        landed(rh.at[i], s_h.at[1 + i], r_h.at[1 + i])
    whole = hs[0].astype(F32) + rh[0].astype(F32) + rh[1].astype(F32) + rh[2].astype(F32)
    lfin[...] = whole
    go(lfin, rfin, s_h.at[4], r_h.at[4], twin)

    for d in near:
        landed(rdq.at[(a + NA - d) % NA], s_qf.at[d - 1], r_qf.at[d - 1])
    for h in range(NA):
        rope = jnp.concatenate([rdq[h, ROWS:, :64], rdq[h, ROWS:, 64:]], axis=0)
        qg_ref[:, h * 192 : (h + 1) * 192] = jnp.concatenate([rdq[h, :ROWS, :], rope], axis=1)

    landed(rfin, s_h.at[4], r_h.at[4])
    lg_ref[core] = lfin[...]
    lg_ref[1 - core] = rfin[...]

    for d in near:
        fa = (a + NA - d) % NA
        for e in range(NB):
            for f in range(NY):
                landed(
                    ugk.at[fa, (b + NB - e) % NB * NY + (y + f) % NY],
                    s_ka.at[d - 1, e, f], r_ka.at[d - 1, e, f],
                )
                landed(
                    ugv.at[(a + NA - e) % NA, (b + NB - d) % NB * NY + (y + f) % NY],
                    s_vb.at[d - 1, e, f], r_vb.at[d - 1, e, f],
                )
    for j in range(NB):

        @pl.when(b != j)
        def _():
            rcopy(dqs.at[j], dqs.at[j], s_dq.at[j], r_dq.at[j], across).wait_send()

    for c in done:
        c.wait_send()


def final_kernel(qg_in, lg_in, ugk, ugv, qg_ref, lg_ref, kug_ref, vug_ref, kf, vf, sem):
    outs = [
        pltpu.make_async_copy(qg_in, qg_ref, sem.at[0]),
        pltpu.make_async_copy(lg_in, lg_ref, sem.at[1]),
    ]
    for c in outs:
        c.start()
    quarter = D_LAT // 4
    for i in range(4):
        at = pl.ds(i * quarter, quarter)
        for n, (src, dst, out) in enumerate([(ugk, kf, kug_ref), (ugv, vf, vug_ref)]):
            for h in range(NA):
                dst[i * quarter : (i + 1) * quarter, h * 128 : (h + 1) * 128] = (
                    src[h, 2 * i : 2 * i + 2].reshape(quarter, 128).astype(F32)
                )
            c = pltpu.make_async_copy(dst.at[at], out.at[at], sem.at[2 + 2 * i + n])
            c.start()
            outs.append(c)
    for c in outs:
        c.wait()


def shards(queries, latents, key_up, value_up, out_grad, positions):
    half = NA * ROWS
    dma = pltpu.SemaphoreType.DMA
    scratch = [
        pltpu.VMEM((ROWS, 768), BF16),
        pltpu.VMEM((576, ROWS), BF16),
        pltpu.VMEM((D_LAT, 512), BF16),
        pltpu.VMEM((D_LAT, 512), BF16),
        pltpu.VMEM((ROWS, 512), BF16),
        pltpu.VMEM((NA, ROWS, QW), BF16),
        pltpu.VMEM((NA, ROWS, KW), BF16),
        pltpu.VMEM((NB, NA, ROWS, QW), BF16),
        pltpu.VMEM((NY, NA, ROWS, KW), BF16),
        pltpu.VMEM((NY, NA, D_LAT, ROWS), BF16),
        pltpu.VMEM((KTOK, TILE), F32),
        pltpu.VMEM((NB, KTOK, half), F32),
        pltpu.VMEM((NB, KTOK, half), F32),
        pltpu.VMEM((NB, 8, half), F32),
        pltpu.VMEM((NB, NB, 8, half), F32),
        pltpu.VMEM((NB, 8, half), F32),
        pltpu.VMEM((NB, KTOK, half), BF16),
        pltpu.VMEM((NB, NA, 192, 128), BF16),
        pltpu.VMEM((NB, NA, 192, 128), BF16),
        pltpu.VMEM((KTOK, 256), F32),
        pltpu.VMEM((KTOK, 128), F32),
        pltpu.VMEM((NA, ROWS, 384), BF16),
        pltpu.VMEM((NA, ROWS, 256), BF16),
        pltpu.VMEM((NA, ROWS, 384), BF16),
        pltpu.VMEM((NA, ROWS, 256), BF16),
        pltpu.VMEM((NA, 192, 128), BF16),
        pltpu.VMEM((NA, 192, 128), BF16),
        pltpu.VMEM((NB * NY, 64, 256), BF16),
        pltpu.VMEM((NB * NY, 64, 256), BF16),
        pltpu.VMEM((64, 128), BF16),
        pltpu.VMEM((64, 128), BF16),
        pltpu.VMEM((NY, 2, 288, ROWS), F32),
        pltpu.VMEM((NY, 288, ROWS), BF16),
        pltpu.VMEM((NY, 288, ROWS), BF16),
        pltpu.VMEM((NY, 288, ROWS), BF16),
        pltpu.VMEM((3, 288, ROWS), BF16),
        pltpu.VMEM((288, ROWS), F32),
        pltpu.VMEM((288, ROWS), F32),
    ]
    sems = [
        dma((5,)), dma((3,)), dma((3,)), dma((3,)), dma((3,)), dma((3,)), dma((3,)),
        dma((3, 4)), dma((4, 4)), dma((4,)), dma((4,)), dma((4,)), dma((4,)),
        dma((3, 4)), dma((4, 4)), dma((4,)), dma((4,)),
        dma((3,)), dma((3,)), dma((3,)), dma((3,)), dma((3,)), dma((3,)), dma((7,)), dma((7,)),
        dma, dma, dma((3, 2)), dma((3, 2)), dma((3, 4, 2)), dma((3, 4, 2)),
        dma, dma, dma((3, 2)), dma((3, 2)), dma((3, 4, 2)), dma((3, 4, 2)),
        dma((5,)), dma((5,)),
    ]
    hbm = pl.BlockSpec(memory_space=pltpu.HBM)
    qg, lg, ugk, ugv = pl.pallas_call(
        whole_kernel,
        out_shape=(
            shape((ROWS, 768)),
            shape((2, 288, ROWS), F32),
            shape((NA, NB * NY, 64, 128)),
            shape((NA, NB * NY, 64, 128)),
        ),
        in_specs=[SMEM] + [hbm] * 5,
        out_specs=(VMEM,) * 4,
        scratch_shapes=scratch + sems,
        compiler_params=pltpu.CompilerParams(
            collective_id=0, has_side_effects=True, vmem_limit_bytes=LIMIT * 1024 * 1024
        ),
    )(positions, queries, latents.T, key_up, value_up, out_grad)
    qg, lg, kug, vug = pl.pallas_call(
        final_kernel,
        out_shape=(
            shape((ROWS, 768)),
            shape((2, 288, ROWS), F32),
            shape((D_LAT, 512), F32),
            shape((D_LAT, 512), F32),
        ),
        in_specs=[VMEM] * 4,
        out_specs=(hbm,) * 4,
        scratch_shapes=[pltpu.VMEM((D_LAT, 512), F32), pltpu.VMEM((D_LAT, 512), F32), dma((10,))],
        compiler_params=pltpu.CompilerParams(vmem_limit_bytes=8 * 1024 * 1024),
    )(qg, lg, ugk, ugv)
    return (qg, lg.reshape(576, ROWS).T, kug, vug)


def solution(mesh):
    in_specs = (
        P("seq", "head"),
        P("seq", None),
        P(None, "head"),
        P(None, "head"),
        P("seq", "head"),
        P("seq"),
    )
    out_specs = (P("seq", "head"), P("seq", None), P(None, "head"), P(None, "head"))
    return jax.shard_map(shards, mesh=mesh, in_specs=in_specs, out_specs=out_specs, check_vma=False)
```

```python
import math

import jax
import jax.numpy as jnp
from jax import lax
from jax.experimental import pallas as pl
from jax.experimental.pallas import tpu as pltpu
from jax.sharding import PartitionSpec as P


D_LAT = 512
D_ROPE = 64
D_NOPE = 128
D_V = 128
ROWS = 128
NA = 4
NB = 4
NY = 2
BLOCK = 336
KTOK = NY * NA * ROWS
TILE = 256
NEG = -1e30
LIMIT = 60
FLOOR = -1e29
SCALE = 1.0 / math.sqrt(D_NOPE + D_ROPE)
LOG2E = math.log2(math.e)
MESH = pl.DeviceIdType.MESH
F32 = jnp.float32
BF16 = jnp.bfloat16
VMEM = pl.BlockSpec(memory_space=pltpu.VMEM)
SMEM = pl.BlockSpec(memory_space=pltpu.SMEM)
NT = (((1,), (1,)), ((), ()))
TN = (((0,), (0,)), ((), ()))


def coords():
    seq = lax.axis_index("seq")
    head = lax.axis_index("head")
    core = head % 2
    y = seq // 16
    z = (seq // 4) % 4
    x = seq % 4
    a = x + core * (z - x)
    b = z + core * (x - z)
    sa = 1 + 3 * core
    sb = 4 - 3 * core

    def dev(a2, b2, y2):
        return (y2 * 16 + a2 * sa + b2 * sb, head)

    return seq, head, y, a, b, dev


def rcopy(src, dst, send, recv, device):
    return pltpu.make_async_remote_copy(
        src_ref=src, dst_ref=dst, send_sem=send, recv_sem=recv, device_id=device, device_id_type=MESH
    )


def dot(u, v, dims=(((1,), (0,)), ((), ()))):
    return lax.dot_general(u, v, dims, preferred_element_type=F32)


def shape(dims, dtype=BF16):
    return jax.ShapeDtypeStruct(dims, dtype)


def whole_kernel(
    pos_ref, q_hbm, latt_hbm, ku_hbm, vu_hbm, g_hbm,
    qg_hbm, lg_hbm, ugk_hbm, ugv_hbm,
    q_ref, latt_ref, ku_ref, vu_ref, g_ref,
    pq, pk, qb, kb, qp, kp, kpt, cl, kpos, s_all, dp_all, stl, sb, rows, ds_all, dqs, rq, dka, dva, gs0, gs1, rg0, rg1,
    dqf, rdq, ups, rup, usk, usv, lsum, lhalf, rhalf, hs, rh, lfin, rfin, qg_ref, ugk, ugv,
    s_in, s_aq, r_aq, s_ak, r_ak, s_al, r_al, s_bq, r_bq, s_yk, r_yk, s_yl, r_yl, s_st, r_st, s_dq, r_dq,
    s_g0, r_g0, s_g1, r_g1, s_qf, r_qf, s_up, r_up,
    s_kb, r_kb, s_ka, r_ka, s_va, r_va, s_vb, r_vb, s_h, r_h, s_out,
):
    seq, head, y, a, b, dev = coords()
    core = head % 2
    twin = (seq, head + 1 - 2 * core)
    far = (seq, (head + 2) % 4)
    across = dev(a, b, 1 - y)
    corner = (across[0], (head + 2) % 4)
    near = (1, 3, 2)
    others = [(0, 1), (1, 0), (1, 1), (2, 0), (2, 1), (3, 0), (3, 1)]
    by_reach = (1, 5, 0, 3, 2, 6, 4)

    barrier = pltpu.get_barrier_semaphore()
    for p in (
        [dev((a + d) % NA, b, y) for d in near]
        + [dev(a, (b + e) % NB, (y + f) % NY) for e, f in others]
        + [dev((a + d) % NA, b, 1 - y) for d in near]
        + [twin, far, corner]
    ):
        pl.semaphore_signal(barrier, inc=1, device_id=p, device_id_type=MESH)

    done = []

    def go(src, dst, send, recv, device):
        c = rcopy(src, dst, send, recv, device)
        c.start()
        done.append(c)

    def landed(ref, send, recv):
        rcopy(ref, ref, send, recv, across).wait_recv()

    loads = [
        pltpu.make_async_copy(src, dst, s_in.at[i])
        for i, (src, dst) in enumerate(
            [(latt_hbm, latt_ref), (ku_hbm, ku_ref), (vu_hbm, vu_ref), (q_hbm, q_ref), (g_hbm, g_ref)]
        )
    ]
    for c in loads:
        c.start()
    for c in loads:
        c.wait()

    stripe = lax.shift_right_logical(pos_ref[0], 7).astype(F32)
    stripes = jnp.full((16, 128), stripe, F32).astype(BF16)
    comp = latt_ref[:D_LAT, :]
    kn = dot(comp, ku_ref[...], TN).astype(BF16)
    vv = dot(comp, vu_ref[...], TN).astype(BF16)
    eye = (
        lax.broadcasted_iota(jnp.int32, (64, 128), 0) == lax.broadcasted_iota(jnp.int32, (64, 128), 1)
    ).astype(F32).astype(BF16)
    k_rope = dot(latt_ref[D_LAT:, :], eye, TN).astype(BF16)
    k_rope = jnp.concatenate([k_rope[:64, :64], k_rope[64:, :64]], axis=1)
    for h in range(NA):
        pk[h, 0:128, :] = kn[:, h * 128 : (h + 1) * 128]
        pk[h, 128:256, :] = vv[:, h * 128 : (h + 1) * 128]
        pk[h, 256:320, :] = k_rope
        pk[h, 320:, :] = stripes
        q = q_ref[:, h * 192 : (h + 1) * 192]
        pq[h, 0:128, :] = q[:, :128]
        pq[h, 128:256, :] = g_ref[:, h * 128 : (h + 1) * 128]
        pq[h, 256:320, :] = jnp.concatenate([q[:64, 128:], q[64:, 128:]], axis=1)
        pq[h, 320:, :] = stripes

    pl.semaphore_wait(barrier, 6 + len(others) + 3)

    def on_a(d):
        return dev((a + d) % NA, b, y)

    def on_b(e):
        return dev(a, (b + e) % NB, y)

    for d in near:
        to = (a + d) % NA
        go(pk.at[to], kb.at[0, d], s_ak.at[d - 1], r_ak.at[d - 1], on_a(d))
        go(pq.at[to], qb.at[0, d], s_aq.at[d - 1], r_aq.at[d - 1], on_a(d))
    go(pk.at[a], kb.at[1, 0], s_yk.at[0], r_yk.at[0], across)
    for e in near:
        go(pq.at[a], qb.at[e, 0], s_bq.at[e - 1, 0], r_bq.at[e - 1, 0], on_b(e))
    qb[0, 0] = pq[a]
    kb[0, 0] = pk[a]
    cl[0, 0] = comp
    for d in near:
        landed(kb.at[0, d], s_ak.at[d - 1], r_ak.at[d - 1])
        go(kb.at[0, d], kb.at[1, d], s_yk.at[d], r_yk.at[d], across)
        landed(qb.at[0, d], s_aq.at[d - 1], r_aq.at[d - 1])
        for e in near:
            go(qb.at[0, d], qb.at[e, d], s_bq.at[e - 1, d], r_bq.at[e - 1, d], on_b(e))
    go(latt_ref.at[pl.ds(0, D_LAT)], cl.at[1, 0], s_yl, r_yl, across)

    half = NA * ROWS
    row = lax.broadcasted_iota(jnp.int32, (ROWS, TILE), 0).astype(F32)
    col = lax.broadcasted_iota(jnp.int32, (1, ROWS), 1).astype(F32)
    blank = jnp.zeros((ROWS, 64), BF16)
    pairs = ((0, 1), (3, 2))

    def wide(block):
        rope = jnp.concatenate([block[256:320, :64], block[256:320, 64:]], axis=0)
        return jnp.concatenate([block[:128, :], rope, blank], axis=1)

    def open_keys(k):
        for d in range(NA):
            at = slice(d * ROWS, (d + 1) * ROWS)
            block = kb[k, d]
            kp[k, at, :] = wide(block)
            stripe = block[320:321, :].astype(F32) * 128.0
            kpos[k, at, :] = jnp.concatenate([stripe, stripe], axis=1) + row

    def open_queries(e, t):
        for i, d in enumerate(pairs[t]):
            at = slice(t * TILE + i * ROWS, t * TILE + (i + 1) * ROWS)
            qp[e, at, :] = wide(qb[e, d])

    def wait_q(e, t):
        for d in pairs[t]:
            landed(qb.at[e, d], s_bq.at[e - 1, d], r_bq.at[e - 1, d])

    def grads_of(e, t):
        d0, d1 = pairs[t]
        return jnp.concatenate([qb[e, d0, 128:256, :], qb[e, d1, 128:256, :]], axis=0)

    def unit(k, e, t, first):
        at = slice(t * TILE, (t + 1) * TILE)
        if first:
            open_queries(e, t)
        qpos = jnp.concatenate([qb[e, d, 320:321, :].astype(F32) * 128.0 + col for d in pairs[t]], axis=1)
        raw = dot(kp[k], qp[e, at, :], NT)
        s = jnp.where(kpos[k] <= qpos, raw * (SCALE * LOG2E), NEG)
        s_all[k, e, :, at] = s
        dp = dot(kb[k, :, 128:256, :].reshape(half, 128), grads_of(e, t), NT)
        dp_all[k, e, :, at] = dp
        top = jnp.max(s, axis=0, keepdims=True)
        if not first:
            old = stl[e, 0:1, at]
            top = jnp.maximum(top, old)
        w = jnp.exp2(s - jnp.maximum(top, FLOOR))
        total = jnp.sum(w, axis=0, keepdims=True)
        weighted = jnp.sum(w * dp, axis=0, keepdims=True)
        if not first:
            fade = jnp.exp2(old - top)
            total = total + fade * stl[e, 1:2, at]
            weighted = weighted + fade * stl[e, 2:3, at]
        stl[e, 0:1, at] = top
        stl[e, 1:2, at] = total
        stl[e, 2:3, at] = weighted

    def tell(e):
        for g in near:
            go(stl.at[e], sb.at[(e + g) % NB, g], s_st.at[e, g - 1], r_st.at[(e + g) % NB, g - 1], on_b(g))

    stl[...] = jnp.zeros_like(stl)
    open_keys(0)
    unit(0, 0, 0, True)
    unit(0, 0, 1, True)
    for e in near:
        wait_q(e, 0)
        unit(0, e, 0, True)
    for d in (0, 1, 3, 2):
        landed(kb.at[1, d], s_yk.at[d], r_yk.at[d])
    open_keys(1)
    unit(1, 0, 0, False)
    unit(1, 0, 1, False)
    tell(0)
    for e in near:
        unit(1, e, 0, False)
    for e in near:
        wait_q(e, 1)
        if e == 2:
            landed(cl.at[1, 0], s_yl, r_yl)
            for d in near:
                go(latt_ref.at[pl.ds(0, D_LAT)], cl.at[0, d], s_al.at[0, d - 1], r_al.at[0, d - 1], on_a(d))
                go(cl.at[1, 0], cl.at[1, d], s_al.at[1, d - 1], r_al.at[1, d - 1], on_a(d))
        unit(0, e, 1, True)
        unit(1, e, 1, False)
        tell(e)
    kpt[...] = kp[...].reshape(KTOK, 256).T

    for k in (1, 0):
        ks = slice(k * half, (k + 1) * half)
        for n, e in enumerate((0, 1, 3, 2)):
            if k == 1:
                for g in near:
                    landed(sb.at[e, g], s_st.at[e, g - 1], r_st.at[e, g - 1])
                got = [stl[e]] + [sb[e, g] for g in near]
                tops = [r[0:1, :] for r in got]
                top = jnp.maximum(jnp.maximum(tops[0], tops[1]), jnp.maximum(tops[2], tops[3]))
                fades = [jnp.exp2(t - top) for t in tops]
                total = sum(f * r[1:2, :] for f, r in zip(fades, got))
                rows[e, 1:2, :] = sum(f * r[2:3, :] for f, r in zip(fades, got)) / total
                rows[e, 0:1, :] = top + jnp.log(total) * LOG2E
            grads = jnp.concatenate([grads_of(e, 0), grads_of(e, 1)], axis=0)
            p = jnp.exp2(s_all[k, e] - rows[e, 0:1, :])
            ds = (p * (dp_all[k, e] - rows[e, 1:2, :]) * SCALE).astype(BF16)
            ds_all[e, ks, :] = ds
            dv = dot(p.astype(BF16), grads)
            dk = dot(ds, qp[e])
            if n == 0:
                dva[ks, :] = dv
                dka[ks, :] = dk
            else:
                dva[ks, :] += dv
                dka[ks, :] += dk
        if k == 1:
            for d in range(NA):
                at = slice(half + d * ROWS, half + (d + 1) * ROWS)
                gs1[d, :, :128] = dka[at, :128].astype(BF16)
                gs1[d, :, 128:] = dva[at, :].astype(BF16)
            for d in near:
                go(gs1.at[d], rg1.at[a], s_g1.at[d - 1], r_g1.at[d - 1], on_a(NA - d))
        else:
            for d in range(NA):
                at = slice(d * ROWS, (d + 1) * ROWS)
                at1 = slice(half + d * ROWS, half + (d + 1) * ROWS)
                gs0[d, :, :128] = dka[at, :128].astype(BF16)
                gs0[d, :, 128:256] = dva[at, :].astype(BF16)
                gs0[d, :, 256:] = jnp.concatenate([dka[at, 128:192], dka[at1, 128:192]], axis=1).astype(BF16)
            for d in near:
                go(gs0.at[d], rg0.at[a], s_g0.at[d - 1], r_g0.at[d - 1], on_a(NA - d))

    for d in near:
        for k in range(NY):
            landed(cl.at[k, d], s_al.at[k, d - 1], r_al.at[k, d - 1])
    g = jnp.concatenate([dka[:, :128], dva[...]], axis=1).astype(BF16)
    comps = jnp.concatenate([cl[k, i] for k in range(NY) for i in range(NA)], axis=1)
    up = dot(comps, g)
    for i in range(NB * NY):
        ups[i] = up[i * 64 : (i + 1) * 64, :].astype(BF16)
    mine = b * NY + y
    for i, (e, f) in enumerate(others):
        tb, ty = (b + e) % NB, (y + f) % NY
        go(ups.at[tb * NY + ty], rup.at[mine], s_up.at[i], r_up.at[i], dev(a, tb, ty))
    rup[mine] = ups[mine]

    for e in (2, 1, 3, 0):
        dq = dot(kpt[:192, :], ds_all[e]).astype(BF16)
        for t, (d0, d1) in enumerate(pairs):
            dqs[e, d0] = dq[:, t * TILE : t * TILE + ROWS]
            dqs[e, d1] = dq[:, t * TILE + ROWS : (t + 1) * TILE]
        if e:
            go(dqs.at[e], rq.at[e], s_dq.at[e], r_dq.at[e], on_b(NB - e))
    rg0[a] = gs0[0]
    rg1[a] = gs1[0]

    for d in near:
        landed(rg1.at[(a + d) % NA], s_g1.at[d - 1], r_g1.at[d - 1])
        landed(rg0.at[(a + d) % NA], s_g0.at[d - 1], r_g0.at[d - 1])
    dk_all = jnp.concatenate(
        [jnp.concatenate([r[h, :, :128] for h in range(NA)], axis=1) for r in (rg0, rg1)], axis=0
    )
    dv_all = jnp.concatenate(
        [jnp.concatenate([r[h, :, 128:256] for h in range(NA)], axis=1) for r in (rg0, rg1)], axis=0
    )
    lp = dot(ku_ref[...], dk_all, NT) + dot(vu_ref[...], dv_all, NT)
    rope = sum(rg0[h, :, 256:].astype(F32) for h in range(NA)).T
    for k in range(NY):
        whole = jnp.concatenate([lp[:, k * 128 : (k + 1) * 128], rope[k * 64 : (k + 1) * 64, :]], axis=0)
        lsum[k] = whole.reshape(2, 288, ROWS)
    for k in range(NY):
        lhalf[k] = lsum[k, 1 - core].astype(BF16)
    go(lhalf, rhalf, s_h.at[0], r_h.at[0], twin)

    for i, (e, f) in enumerate(others):
        fb, fy = (b + NB - e) % NB, (y + f) % NY
        landed(rup.at[fb * NY + fy], s_up.at[i], r_up.at[i])
    us = sum(rup[i].astype(F32) for i in range(NB * NY)).astype(BF16)
    usk[...] = us[:, :128]
    usv[...] = us[:, 128:]
    ugk[a, mine] = us[:, :128]
    ugv[a, mine] = us[:, 128:]
    for i, (e, f) in enumerate(others):
        fy = (y + f) % NY
        go(usk, ugk.at[a, mine], s_kb.at[i], r_kb.at[i], dev(a, (b + e) % NB, fy))
        go(usv, ugv.at[a, mine], s_va.at[i], r_va.at[i], dev((a + e) % NA, b, fy))

    def k_over_a(slot, i):
        for d in near:
            go(slot, slot, s_ka.at[d - 1, i], r_ka.at[d - 1, i], dev((a + d) % NA, b, y))

    def v_over_b(slot, i):
        for d in near:
            go(slot, slot, s_vb.at[d - 1, i], r_vb.at[d - 1, i], dev(a, (b + d) % NB, y))

    k_over_a(ugk.at[a, mine], 7)
    v_over_b(ugv.at[a, mine], 7)

    landed(rhalf, s_h.at[0], r_h.at[0])
    for k in range(NY):
        hs[k] = (lsum[k, core] + rhalf[k].astype(F32)).astype(BF16)
    go(hs.at[0], rh.at[0], s_h.at[1], r_h.at[1], far)
    go(hs.at[1], rh.at[1], s_h.at[2], r_h.at[2], across)
    go(hs.at[1], rh.at[2], s_h.at[3], r_h.at[3], corner)

    for e in near:
        landed(rq.at[e], s_dq.at[e], r_dq.at[e])
    dqf[...] = (dqs[0].astype(F32) + sum(rq[e].astype(F32) for e in near)).astype(BF16)
    for d in near:
        go(dqf.at[d], rdq.at[a], s_qf.at[d - 1], r_qf.at[d - 1], on_a(NA - d))
    rdq[a] = dqf[0]

    def piece(i, axis):
        e, f = others[i]
        if axis == "b":
            return (b + NB - e) % NB * NY + (y + f) % NY
        return (a + NA - e) % NA, (y + f) % NY

    for i in by_reach:
        slot = ugk.at[a, piece(i, "b")]
        landed(slot, s_kb.at[i], r_kb.at[i])
        k_over_a(slot, i)
        fa, fy = piece(i, "a")
        slot = ugv.at[fa, b * NY + fy]
        landed(slot, s_va.at[i], r_va.at[i])
        v_over_b(slot, i)

    for i in range(3):
        landed(rh.at[i], s_h.at[1 + i], r_h.at[1 + i])
    whole = hs[0].astype(F32) + rh[0].astype(F32) + rh[1].astype(F32) + rh[2].astype(F32)
    lfin[...] = whole
    go(lfin, rfin, s_h.at[4], r_h.at[4], twin)

    for d in near:
        landed(rdq.at[(a + d) % NA], s_qf.at[d - 1], r_qf.at[d - 1])
    for h in range(NA):
        qg_ref[:, h * 192 : (h + 1) * 192] = rdq[h].T

    outs = []

    def write(src, dst):
        c = pltpu.make_async_copy(src, dst, s_out.at[len(outs)])
        c.start()
        outs.append(c)

    write(qg_ref, qg_hbm)
    landed(rfin, s_h.at[4], r_h.at[4])
    write(lfin, lg_hbm.at[core])
    write(rfin, lg_hbm.at[1 - core])
    write(ugk.at[a], ugk_hbm.at[a])
    own_b = pl.ds(b * NY, NY)
    write(ugv.at[:, own_b], ugv_hbm.at[:, own_b])

    for d in near:
        fa, fb = (a + NA - d) % NA, (b + NB - d) % NB
        for i in range(8):
            p = mine if i == 7 else piece(i, "b")
            landed(ugk.at[fa, p], s_ka.at[d - 1, i], r_ka.at[d - 1, i])
            pa, py = (a, y) if i == 7 else piece(i, "a")
            landed(ugv.at[pa, fb * NY + py], s_vb.at[d - 1, i], r_vb.at[d - 1, i])
        write(ugk.at[fa], ugk_hbm.at[fa])
        from_b = pl.ds(fb * NY, NY)
        write(ugv.at[:, from_b], ugv_hbm.at[:, from_b])
    for c in outs:
        c.wait()
    for c in done:
        c.wait_send()


def final_kernel(
    qg_hbm, lg_hbm, ugk_hbm, ugv_hbm, qg_ref, lg_ref, kug_ref, vug_ref, qv, lv, kv, vv, kf, vf, s_in, s_out
):
    quarter = D_LAT // 4
    loads, outs = [], []

    def start(pile, src, dst, sem):
        c = pltpu.make_async_copy(src, dst, sem)
        c.start()
        pile.append(c)

    for i in range(4):
        at = pl.ds(2 * i, 2)
        start(loads, ugk_hbm.at[:, at], kv.at[:, at], s_in.at[2 * i])
        start(loads, ugv_hbm.at[:, at], vv.at[:, at], s_in.at[2 * i + 1])
    start(loads, qg_hbm, qv, s_in.at[8])
    start(loads, lg_hbm, lv, s_in.at[9])
    for i in range(4):
        at = pl.ds(i * quarter, quarter)
        for n, (src, dst, out) in enumerate([(kv, kf, kug_ref), (vv, vf, vug_ref)]):
            loads[2 * i + n].wait()
            for h in range(NA):
                dst[i * quarter : (i + 1) * quarter, h * 128 : (h + 1) * 128] = (
                    src[h, 2 * i : 2 * i + 2].reshape(quarter, 128).astype(F32)
                )
            start(outs, dst.at[at], out.at[at], s_out.at[2 * i + n])
    loads[8].wait()
    start(outs, qv, qg_ref, s_out.at[8])
    loads[9].wait()
    start(outs, lv, lg_ref, s_out.at[9])
    for c in outs:
        c.wait()


def shards(queries, latents, key_up, value_up, out_grad, positions):
    half = NA * ROWS
    dma = pltpu.SemaphoreType.DMA
    scratch = [
        pltpu.VMEM((ROWS, 768), BF16),
        pltpu.VMEM((576, ROWS), BF16),
        pltpu.VMEM((D_LAT, 512), BF16),
        pltpu.VMEM((D_LAT, 512), BF16),
        pltpu.VMEM((ROWS, 512), BF16),
        pltpu.VMEM((NA, BLOCK, 128), BF16),
        pltpu.VMEM((NA, BLOCK, 128), BF16),
        pltpu.VMEM((NB, NA, BLOCK, 128), BF16),
        pltpu.VMEM((NY, NA, BLOCK, 128), BF16),
        pltpu.VMEM((NB, half, 256), BF16),
        pltpu.VMEM((NY, half, 256), BF16),
        pltpu.VMEM((256, KTOK), BF16),
        pltpu.VMEM((NY, NA, D_LAT, ROWS), BF16),
        pltpu.VMEM((NY, half, TILE), F32),
        pltpu.VMEM((NY, NB, half, half), F32),
        pltpu.VMEM((NY, NB, half, half), F32),
        pltpu.VMEM((NB, 8, half), F32),
        pltpu.VMEM((NB, NB, 8, half), F32),
        pltpu.VMEM((NB, 8, half), F32),
        pltpu.VMEM((NB, KTOK, half), BF16),
        pltpu.VMEM((NB, NA, 192, 128), BF16),
        pltpu.VMEM((NB, NA, 192, 128), BF16),
        pltpu.VMEM((KTOK, 256), F32),
        pltpu.VMEM((KTOK, 128), F32),
        pltpu.VMEM((NA, ROWS, 384), BF16),
        pltpu.VMEM((NA, ROWS, 256), BF16),
        pltpu.VMEM((NA, ROWS, 384), BF16),
        pltpu.VMEM((NA, ROWS, 256), BF16),
        pltpu.VMEM((NA, 192, 128), BF16),
        pltpu.VMEM((NA, 192, 128), BF16),
        pltpu.VMEM((NB * NY, 64, 256), BF16),
        pltpu.VMEM((NB * NY, 64, 256), BF16),
        pltpu.VMEM((64, 128), BF16),
        pltpu.VMEM((64, 128), BF16),
        pltpu.VMEM((NY, 2, 288, ROWS), F32),
        pltpu.VMEM((NY, 288, ROWS), BF16),
        pltpu.VMEM((NY, 288, ROWS), BF16),
        pltpu.VMEM((NY, 288, ROWS), BF16),
        pltpu.VMEM((3, 288, ROWS), BF16),
        pltpu.VMEM((288, ROWS), F32),
        pltpu.VMEM((288, ROWS), F32),
        pltpu.VMEM((ROWS, 768), BF16),
        pltpu.VMEM((NA, NB * NY, 64, 128), BF16),
        pltpu.VMEM((NA, NB * NY, 64, 128), BF16),
    ]
    sems = [
        dma((5,)), dma((3,)), dma((3,)), dma((3,)), dma((3,)), dma((2, 3)), dma((2, 3)),
        dma((3, 4)), dma((3, 4)), dma((4,)), dma((4,)), dma, dma,
        dma((4, 3)), dma((4, 3)), dma((4,)), dma((4,)),
        dma((3,)), dma((3,)), dma((3,)), dma((3,)), dma((3,)), dma((3,)), dma((7,)), dma((7,)),
        dma((7,)), dma((7,)), dma((3, 8)), dma((3, 8)), dma((7,)), dma((7,)), dma((3, 8)), dma((3, 8)),
        dma((5,)), dma((5,)), dma((11,)),
    ]
    hbm = pl.BlockSpec(memory_space=pltpu.HBM)
    qg, lg, ugk, ugv = pl.pallas_call(
        whole_kernel,
        out_shape=(
            shape((ROWS, 768)),
            shape((2, 288, ROWS), F32),
            shape((NA, NB * NY, 64, 128)),
            shape((NA, NB * NY, 64, 128)),
        ),
        in_specs=[SMEM] + [hbm] * 5,
        out_specs=(hbm,) * 4,
        scratch_shapes=scratch + sems,
        compiler_params=pltpu.CompilerParams(
            collective_id=0, has_side_effects=True, vmem_limit_bytes=LIMIT * 1024 * 1024
        ),
    )(positions, queries, latents.T, key_up, value_up, out_grad)
    qg, lg, kug, vug = pl.pallas_call(
        final_kernel,
        out_shape=(
            shape((ROWS, 768)),
            shape((2, 288, ROWS), F32),
            shape((D_LAT, 512), F32),
            shape((D_LAT, 512), F32),
        ),
        in_specs=[hbm] * 4,
        out_specs=(hbm,) * 4,
        scratch_shapes=[
            pltpu.VMEM((ROWS, 768), BF16),
            pltpu.VMEM((2, 288, ROWS), F32),
            pltpu.VMEM((NA, NB * NY, 64, 128), BF16),
            pltpu.VMEM((NA, NB * NY, 64, 128), BF16),
            pltpu.VMEM((D_LAT, 512), F32),
            pltpu.VMEM((D_LAT, 512), F32),
            dma((10,)),
            dma((10,)),
        ],
        compiler_params=pltpu.CompilerParams(vmem_limit_bytes=LIMIT * 1024 * 1024),
    )(qg, lg, ugk, ugv)
    return (qg, lg.reshape(576, ROWS).T, kug, vug)


def solution(mesh):
    in_specs = (
        P("seq", "head"),
        P("seq", None),
        P(None, "head"),
        P(None, "head"),
        P("seq", "head"),
        P("seq"),
    )
    out_specs = (P("seq", "head"), P("seq", None), P(None, "head"), P(None, "head"))
    return jax.shard_map(shards, mesh=mesh, in_specs=in_specs, out_specs=out_specs, check_vma=False)
```

```python
import math

import jax
import jax.numpy as jnp
from jax import lax
from jax.experimental import pallas as pl
from jax.experimental.pallas import tpu as pltpu
from jax.sharding import PartitionSpec as P


D_LAT = 512
D_ROPE = 64
D_NOPE = 128
D_V = 128
ROWS = 128
NA = 4
NB = 4
NY = 2
BLOCK = 336
KTOK = NY * NA * ROWS
TILE = 256
NEG = -1e30
LIMIT = 60
FLOOR = -1e29
SCALE = 1.0 / math.sqrt(D_NOPE + D_ROPE)
LOG2E = math.log2(math.e)
MESH = pl.DeviceIdType.MESH
F32 = jnp.float32
BF16 = jnp.bfloat16
VMEM = pl.BlockSpec(memory_space=pltpu.VMEM)
SMEM = pl.BlockSpec(memory_space=pltpu.SMEM)
NT = (((1,), (1,)), ((), ()))
TN = (((0,), (0,)), ((), ()))


def coords():
    seq = lax.axis_index("seq")
    head = lax.axis_index("head")
    core = head % 2
    y = seq // 16
    z = (seq // 4) % 4
    x = seq % 4
    a = x + core * (z - x)
    b = z + core * (x - z)
    sa = 1 + 3 * core
    sb = 4 - 3 * core

    def dev(a2, b2, y2):
        return (y2 * 16 + a2 * sa + b2 * sb, head)

    return seq, head, y, a, b, dev


def rcopy(src, dst, send, recv, device):
    return pltpu.make_async_remote_copy(
        src_ref=src, dst_ref=dst, send_sem=send, recv_sem=recv, device_id=device, device_id_type=MESH
    )


def dot(u, v, dims=(((1,), (0,)), ((), ()))):
    return lax.dot_general(u, v, dims, preferred_element_type=F32)


def shape(dims, dtype=BF16):
    return jax.ShapeDtypeStruct(dims, dtype)


def whole_kernel(
    pos_ref, q_hbm, latt_hbm, ku_hbm, vu_hbm, g_hbm,
    qg_hbm, lg_hbm, ugk_hbm, ugv_hbm,
    q_ref, latt_ref, ku_ref, vu_ref, g_ref,
    pq, pk, qb, kb, qp, kp, kpt, cl, kpos, s_all, dp_all, stl, sb, rows, ds_all, dqs, rq, dka, dva, gs0, gs1, rg0, rg1,
    dqf, rdq, ups, rup, usk, usv, lsum, lhalf, rhalf, hs, rh, lfin, rfin, qg_ref, ugk, ugv,
    s_in, s_aq, r_aq, s_ak, r_ak, s_al, r_al, s_bq, r_bq, s_yk, r_yk, s_yl, r_yl, s_st, r_st, s_dq, r_dq,
    s_g0, r_g0, s_g1, r_g1, s_qf, r_qf, s_up, r_up,
    s_kb, r_kb, s_ka, r_ka, s_va, r_va, s_vb, r_vb, s_h, r_h, s_out,
):
    seq, head, y, a, b, dev = coords()
    core = head % 2
    twin = (seq, head + 1 - 2 * core)
    far = (seq, (head + 2) % 4)
    across = dev(a, b, 1 - y)
    corner = (across[0], (head + 2) % 4)
    near = (1, 3, 2)
    others = [(0, 1), (1, 0), (1, 1), (2, 0), (2, 1), (3, 0), (3, 1)]
    by_reach = (1, 5, 0, 3, 2, 6, 4)

    barrier = pltpu.get_barrier_semaphore()
    for p in (
        [dev((a + d) % NA, b, y) for d in near]
        + [dev(a, (b + e) % NB, (y + f) % NY) for e, f in others]
        + [dev((a + d) % NA, b, 1 - y) for d in near]
        + [twin, far, corner]
    ):
        pl.semaphore_signal(barrier, inc=1, device_id=p, device_id_type=MESH)

    def go(src, dst, send, recv, device):
        rcopy(src, dst, send, recv, device).start()

    def landed(ref, recv):
        rcopy(ref, ref, recv, recv, across).wait_recv()

    def left(ref, send):
        rcopy(ref, ref, send, send, across).wait_send()

    loads = [
        pltpu.make_async_copy(src, dst, s_in.at[i])
        for i, (src, dst) in enumerate(
            [(q_hbm, q_ref), (g_hbm, g_ref), (latt_hbm, latt_ref), (ku_hbm, ku_ref), (vu_hbm, vu_ref)]
        )
    ]
    for c in loads:
        c.start()
    loads[0].wait()
    loads[1].wait()

    stripe = lax.shift_right_logical(pos_ref[0], 7).astype(F32)
    stripes = jnp.full((16, 128), stripe, F32).astype(BF16)
    for h in range(NA):
        q = q_ref[:, h * 192 : (h + 1) * 192]
        pq[h, 0:128, :] = q[:, :128]
        pq[h, 128:256, :] = g_ref[:, h * 128 : (h + 1) * 128]
        pq[h, 256:320, :] = jnp.concatenate([q[:64, 128:], q[64:, 128:]], axis=1)
        pq[h, 320:, :] = stripes
    qb[0, 0] = pq[a]
    for c in loads[2:]:
        c.wait()
    comp = latt_ref[:D_LAT, :]
    kn = dot(comp, ku_ref[...], TN).astype(BF16)
    vv = dot(comp, vu_ref[...], TN).astype(BF16)
    eye = (
        lax.broadcasted_iota(jnp.int32, (64, 128), 0) == lax.broadcasted_iota(jnp.int32, (64, 128), 1)
    ).astype(F32).astype(BF16)
    k_rope = dot(latt_ref[D_LAT:, :], eye, TN).astype(BF16)
    k_rope = jnp.concatenate([k_rope[:64, :64], k_rope[64:, :64]], axis=1)
    for h in range(NA):
        pk[h, 0:128, :] = kn[:, h * 128 : (h + 1) * 128]
        pk[h, 128:256, :] = vv[:, h * 128 : (h + 1) * 128]
        pk[h, 256:320, :] = k_rope
        pk[h, 320:, :] = stripes
    kb[0, 0] = pk[a]
    cl[0, 0] = comp

    pl.semaphore_wait(barrier, 6 + len(others) + 3)

    def on_a(d):
        return dev((a + d) % NA, b, y)

    def on_b(e):
        return dev(a, (b + e) % NB, y)

    def tile_of(d):
        return 0 if d < 2 else 1

    for d in near:
        go(pk.at[(a + d) % NA], kb.at[0, d], s_ak, r_ak.at[d - 1], on_a(d))
    go(pk.at[a], kb.at[1, 0], s_yk, r_yk, across)
    for d in near:
        go(pq.at[(a + d) % NA], qb.at[0, d], s_aq, r_aq.at[d - 1], on_a(d))
    for e in near:
        go(pq.at[a], qb.at[e, 0], s_bq, r_bq.at[e - 1, 0], on_b(e))
    def pass_q(d):
        landed(qb.at[0, d], r_aq.at[d - 1])
        for e in near:
            go(qb.at[0, d], qb.at[e, d], s_bq, r_bq.at[e - 1, tile_of(d)], on_b(e))

    def pass_k(d):
        landed(kb.at[0, d], r_ak.at[d - 1])
        go(kb.at[0, d], kb.at[1, d], s_yk, r_yk, across)

    pass_k(1)
    pass_k(3)
    pass_k(2)
    pass_q(1)
    pass_q(3)
    pass_q(2)
    go(latt_ref.at[pl.ds(0, D_LAT)], cl.at[1, 0], s_yl, r_yl, across)

    half = NA * ROWS
    row = lax.broadcasted_iota(jnp.int32, (ROWS, TILE), 0).astype(F32)
    col = lax.broadcasted_iota(jnp.int32, (1, ROWS), 1).astype(F32)
    blank = jnp.zeros((ROWS, 64), BF16)
    pairs = ((0, 1), (3, 2))

    def wide(block):
        rope = jnp.concatenate([block[256:320, :64], block[256:320, 64:]], axis=0)
        return jnp.concatenate([block[:128, :], rope, blank], axis=1)

    def open_keys(k):
        for d in range(NA):
            at = slice(d * ROWS, (d + 1) * ROWS)
            block = kb[k, d]
            kp[k, at, :] = wide(block)
            stripe = block[320:321, :].astype(F32) * 128.0
            kpos[k, at, :] = jnp.concatenate([stripe, stripe], axis=1) + row

    def open_queries(e, t):
        for i, d in enumerate(pairs[t]):
            at = slice(t * TILE + i * ROWS, t * TILE + (i + 1) * ROWS)
            qp[e, at, :] = wide(qb[e, d])

    def wait_q(e, t):
        landed(qb.at[e, pl.ds(2 * t, 2)], r_bq.at[e - 1, t])

    def grads_of(e, t):
        d0, d1 = pairs[t]
        return jnp.concatenate([qb[e, d0, 128:256, :], qb[e, d1, 128:256, :]], axis=0)

    def unit(k, e, t, first):
        at = slice(t * TILE, (t + 1) * TILE)
        if first:
            open_queries(e, t)
        qpos = jnp.concatenate([qb[e, d, 320:321, :].astype(F32) * 128.0 + col for d in pairs[t]], axis=1)
        raw = dot(kp[k], qp[e, at, :], NT)
        s = jnp.where(kpos[k] <= qpos, raw * (SCALE * LOG2E), NEG)
        s_all[k, e, :, at] = s
        dp = dot(kb[k, :, 128:256, :].reshape(half, 128), grads_of(e, t), NT)
        dp_all[k, e, :, at] = dp
        top = jnp.max(s, axis=0, keepdims=True)
        if not first:
            old = stl[t, e, 0:1, :]
            top = jnp.maximum(top, old)
        w = jnp.exp2(s - jnp.maximum(top, FLOOR))
        total = jnp.sum(w, axis=0, keepdims=True)
        weighted = jnp.sum(w * dp, axis=0, keepdims=True)
        if not first:
            fade = jnp.exp2(old - top)
            total = total + fade * stl[t, e, 1:2, :]
            weighted = weighted + fade * stl[t, e, 2:3, :]
        stl[t, e, 0:1, :] = top
        stl[t, e, 1:2, :] = total
        stl[t, e, 2:3, :] = weighted

    def tell(t, e):
        for g in near:
            to = (e + g) % NB
            go(stl.at[t, e], sb.at[t, to, g], s_st, r_st.at[t, to], on_b(g))

    stl[...] = jnp.zeros_like(stl)
    open_keys(0)
    unit(0, 0, 0, True)
    unit(0, 0, 1, True)
    for e in near:
        wait_q(e, 0)
        unit(0, e, 0, True)
    landed(kb.at[1], r_yk)
    for d in near:
        go(latt_ref.at[pl.ds(0, D_LAT)], cl.at[0, d], s_al, r_al, on_a(d))
    open_keys(1)
    unit(1, 0, 0, False)
    tell(0, 0)
    for e in near:
        unit(1, e, 0, False)
        tell(0, e)
    unit(1, 0, 1, False)
    tell(1, 0)
    for e in near:
        wait_q(e, 1)
        if e == 1:
            landed(cl.at[1, 0], r_yl)
            for d in near:
                go(cl.at[1, 0], cl.at[1, d], s_al, r_al, on_a(d))
        unit(0, e, 1, True)
        unit(1, e, 1, False)
        tell(1, e)
    kpt[...] = kp[...].reshape(KTOK, 256).T

    def backward(k, t):
        ks = slice(k * half, (k + 1) * half)
        at = slice(t * TILE, (t + 1) * TILE)
        for n, e in enumerate((0, 1, 3, 2)):
            if k == 1:
                landed(sb.at[t, e, pl.ds(1, 3)], r_st.at[t, e])
                got = [stl[t, e]] + [sb[t, e, g] for g in near]
                tops = [r[0:1, :] for r in got]
                top = jnp.maximum(jnp.maximum(tops[0], tops[1]), jnp.maximum(tops[2], tops[3]))
                fades = [jnp.exp2(u - top) for u in tops]
                total = sum(f * r[1:2, :] for f, r in zip(fades, got))
                rows[e, 1:2, at] = sum(f * r[2:3, :] for f, r in zip(fades, got)) / total
                rows[e, 0:1, at] = top + jnp.log(total) * LOG2E
            p = jnp.exp2(s_all[k, e, :, at] - rows[e, 0:1, at])
            ds = (p * (dp_all[k, e, :, at] - rows[e, 1:2, at]) * SCALE).astype(BF16)
            ds_all[e, ks, at] = ds
            dv = dot(p.astype(BF16), grads_of(e, t))
            dk = dot(ds, qp[e, at, :])
            if n == 0 and t == 0:
                dva[ks, :] = dv
                dka[ks, :] = dk
            else:
                dva[ks, :] += dv
                dka[ks, :] += dk

    def query_sums(t):
        at = slice(t * TILE, (t + 1) * TILE)
        for e in (2, 1, 3, 0):
            dq = dot(kpt[:192, :], ds_all[e, :, at]).astype(BF16)
            dqs[t, e, 0] = dq[:, :ROWS]
            dqs[t, e, 1] = dq[:, ROWS:]
            if e:
                go(dqs.at[t, e], rq.at[t, e], s_dq, r_dq, on_b(NB - e))

    backward(1, 0)
    backward(0, 0)
    query_sums(0)
    backward(1, 1)
    for d in range(NA):
        at = slice(half + d * ROWS, half + (d + 1) * ROWS)
        gs1[d, :, :128] = dka[at, :128].astype(BF16)
        gs1[d, :, 128:] = dva[at, :].astype(BF16)
    for d in near:
        go(gs1.at[d], rg1.at[a], s_g1, r_g1, on_a(NA - d))
    backward(0, 1)
    for d in range(NA):
        at = slice(d * ROWS, (d + 1) * ROWS)
        at1 = slice(half + d * ROWS, half + (d + 1) * ROWS)
        gs0[d, :, :128] = dka[at, :128].astype(BF16)
        gs0[d, :, 128:256] = dva[at, :].astype(BF16)
        gs0[d, :, 256:] = jnp.concatenate([dka[at, 128:192], dka[at1, 128:192]], axis=1).astype(BF16)
    for d in near:
        go(gs0.at[d], rg0.at[a], s_g0, r_g0, on_a(NA - d))

    landed(cl.at[:, pl.ds(1, 3)], r_al)
    g = jnp.concatenate([dka[:, :128], dva[...]], axis=1).astype(BF16)
    comps = jnp.concatenate([cl[k, i] for k in range(NY) for i in range(NA)], axis=1)
    up = dot(comps, g)
    for i in range(NB * NY):
        ups[i] = up[i * 64 : (i + 1) * 64, :].astype(BF16)
    mine = b * NY + y
    for i, (e, f) in enumerate(others):
        tb, ty = (b + e) % NB, (y + f) % NY
        go(ups.at[tb * NY + ty], rup.at[mine], s_up, r_up, dev(a, tb, ty))
    rup[mine] = ups[mine]

    query_sums(1)
    rg0[a] = gs0[0]
    rg1[a] = gs1[0]

    landed(rg1.at[pl.ds(0, 3)], r_g1)
    landed(rg0.at[pl.ds(0, 3)], r_g0)
    dk_all = jnp.concatenate(
        [jnp.concatenate([r[h, :, :128] for h in range(NA)], axis=1) for r in (rg0, rg1)], axis=0
    )
    dv_all = jnp.concatenate(
        [jnp.concatenate([r[h, :, 128:256] for h in range(NA)], axis=1) for r in (rg0, rg1)], axis=0
    )
    lp = dot(ku_ref[...], dk_all, NT) + dot(vu_ref[...], dv_all, NT)
    rope = sum(rg0[h, :, 256:].astype(F32) for h in range(NA)).T
    for k in range(NY):
        whole = jnp.concatenate([lp[:, k * 128 : (k + 1) * 128], rope[k * 64 : (k + 1) * 64, :]], axis=0)
        lsum[k] = whole.reshape(2, 288, ROWS)
    for k in range(NY):
        lhalf[k] = lsum[k, 1 - core].astype(BF16)
    go(lhalf, rhalf, s_h.at[0], r_h.at[0], twin)

    landed(rup.at[pl.ds(0, 7)], r_up)
    us = sum(rup[i].astype(F32) for i in range(NB * NY)).astype(BF16)
    usk[...] = us[:, :128]
    usv[...] = us[:, 128:]
    ugk[a, mine] = us[:, :128]
    ugv[a, mine] = us[:, 128:]
    for i, (e, f) in enumerate(others):
        fy = (y + f) % NY
        go(usk, ugk.at[a, mine], s_kb, r_kb.at[i], dev(a, (b + e) % NB, fy))
        go(usv, ugv.at[a, mine], s_va, r_va.at[i], dev((a + e) % NA, b, fy))

    def k_over_a(slot):
        for d in near:
            go(slot, slot, s_ka, r_ka.at[d - 1], on_a(d))

    def v_over_b(slot):
        for e in near:
            go(slot, slot, s_vb, r_vb.at[e - 1], on_b(e))

    k_over_a(ugk.at[a, mine])
    v_over_b(ugv.at[a, mine])

    landed(rhalf, r_h.at[0])
    for k in range(NY):
        hs[k] = (lsum[k, core] + rhalf[k].astype(F32)).astype(BF16)
    go(hs.at[0], rh.at[0], s_h.at[1], r_h.at[1], far)
    go(hs.at[1], rh.at[1], s_h.at[1], r_h.at[1], across)
    go(hs.at[1], rh.at[2], s_h.at[1], r_h.at[1], corner)

    landed(rq.at[:, pl.ds(1, 3)], r_dq)
    for t in range(2):
        for i, d in enumerate(pairs[t]):
            dqf[d] = (dqs[t, 0, i].astype(F32) + sum(rq[t, e, i].astype(F32) for e in near)).astype(BF16)
    for d in near:
        go(dqf.at[d], rdq.at[a], s_qf, r_qf, on_a(NA - d))
    rdq[a] = dqf[0]

    def piece(i, axis):
        e, f = others[i]
        if axis == "b":
            return (b + NB - e) % NB * NY + (y + f) % NY
        return (a + NA - e) % NA, (y + f) % NY

    for i in by_reach:
        slot = ugk.at[a, piece(i, "b")]
        landed(slot, r_kb.at[i])
        k_over_a(slot)
        fa, fy = piece(i, "a")
        slot = ugv.at[fa, b * NY + fy]
        landed(slot, r_va.at[i])
        v_over_b(slot)

    landed(rh, r_h.at[1])
    whole = hs[0].astype(F32) + rh[0].astype(F32) + rh[1].astype(F32) + rh[2].astype(F32)
    lfin[...] = whole
    go(lfin, rfin, s_h.at[2], r_h.at[2], twin)

    landed(rdq.at[pl.ds(0, 3)], r_qf)
    for h in range(NA):
        qg_ref[:, h * 192 : (h + 1) * 192] = rdq[h].T

    def write(src, dst, sem):
        pltpu.make_async_copy(src, dst, s_out.at[sem]).start()

    write(qg_ref, qg_hbm, 0)
    landed(rfin, r_h.at[2])
    write(lfin, lg_hbm.at[core], 1)
    write(rfin, lg_hbm.at[1 - core], 1)
    write(ugk.at[a], ugk_hbm.at[a], 2)
    own_b = pl.ds(b * NY, NY)
    write(ugv.at[:, own_b], ugv_hbm.at[:, own_b], 3)

    for d in near:
        fa, from_b = (a + NA - d) % NA, pl.ds((b + NB - d) % NB * NY, NY)
        landed(ugk.at[fa], r_ka.at[d - 1])
        write(ugk.at[fa], ugk_hbm.at[fa], 2)
        landed(ugv.at[:, from_b], r_vb.at[d - 1])
        write(ugv.at[:, from_b], ugv_hbm.at[:, from_b], 3)
    left(pq.at[pl.ds(0, 3)], s_aq)
    left(pk.at[pl.ds(0, 3)], s_ak)
    left(qb.at[pl.ds(0, 3)], s_bq)
    left(kb.at[0], s_yk)
    left(cl.at[1, 0], s_yl)
    left(cl.at[:, pl.ds(1, 3)], s_al)
    left(sb.at[:, pl.ds(0, 3)], s_st)
    left(rq.at[:, pl.ds(1, 3)], s_dq)
    left(rg0.at[pl.ds(0, 3)], s_g0)
    left(rg1.at[pl.ds(0, 3)], s_g1)
    left(rdq.at[pl.ds(0, 3)], s_qf)
    left(rup.at[pl.ds(0, 7)], s_up)
    left(ugk.at[0, pl.ds(0, 7)], s_kb)
    left(ugk.at[0, pl.ds(0, 7)], s_va)
    left(ugk.at[pl.ds(0, 3)], s_ka)
    left(ugv.at[pl.ds(0, 3)], s_vb)
    left(lhalf, s_h.at[0])
    left(rh, s_h.at[1])
    left(lfin, s_h.at[2])
    pltpu.make_async_copy(qg_ref, qg_hbm, s_out.at[0]).wait()
    pltpu.make_async_copy(lsum.at[0], lg_hbm, s_out.at[1]).wait()
    pltpu.make_async_copy(ugk, ugk_hbm, s_out.at[2]).wait()
    pltpu.make_async_copy(ugv, ugv_hbm, s_out.at[3]).wait()


def final_kernel(
    qg_hbm, lg_hbm, ugk_hbm, ugv_hbm, qg_ref, lg_ref, kug_ref, vug_ref, qv, lv, kv, vv, kf, vf, s_in, s_out
):
    quarter = D_LAT // 4
    loads, outs = [], []

    def start(pile, src, dst, sem):
        c = pltpu.make_async_copy(src, dst, sem)
        c.start()
        pile.append(c)

    for i in range(4):
        at = pl.ds(2 * i, 2)
        start(loads, ugk_hbm.at[:, at], kv.at[:, at], s_in.at[2 * i])
        start(loads, ugv_hbm.at[:, at], vv.at[:, at], s_in.at[2 * i + 1])
    start(loads, qg_hbm, qv, s_in.at[8])
    start(loads, lg_hbm, lv, s_in.at[9])
    for i in range(4):
        at = pl.ds(i * quarter, quarter)
        for n, (src, dst, out) in enumerate([(kv, kf, kug_ref), (vv, vf, vug_ref)]):
            loads[2 * i + n].wait()
            for h in range(NA):
                dst[i * quarter : (i + 1) * quarter, h * 128 : (h + 1) * 128] = (
                    src[h, 2 * i : 2 * i + 2].reshape(quarter, 128).astype(F32)
                )
            start(outs, dst.at[at], out.at[at], s_out.at[2 * i + n])
    loads[8].wait()
    start(outs, qv, qg_ref, s_out.at[8])
    loads[9].wait()
    start(outs, lv, lg_ref, s_out.at[9])
    for c in outs:
        c.wait()


def shards(queries, latents, key_up, value_up, out_grad, positions):
    half = NA * ROWS
    dma = pltpu.SemaphoreType.DMA
    scratch = [
        pltpu.VMEM((ROWS, 768), BF16),
        pltpu.VMEM((576, ROWS), BF16),
        pltpu.VMEM((D_LAT, 512), BF16),
        pltpu.VMEM((D_LAT, 512), BF16),
        pltpu.VMEM((ROWS, 512), BF16),
        pltpu.VMEM((NA, BLOCK, 128), BF16),
        pltpu.VMEM((NA, BLOCK, 128), BF16),
        pltpu.VMEM((NB, NA, BLOCK, 128), BF16),
        pltpu.VMEM((NY, NA, BLOCK, 128), BF16),
        pltpu.VMEM((NB, half, 256), BF16),
        pltpu.VMEM((NY, half, 256), BF16),
        pltpu.VMEM((256, KTOK), BF16),
        pltpu.VMEM((NY, NA, D_LAT, ROWS), BF16),
        pltpu.VMEM((NY, half, TILE), F32),
        pltpu.VMEM((NY, NB, half, half), F32),
        pltpu.VMEM((NY, NB, half, half), F32),
        pltpu.VMEM((2, NB, 8, TILE), F32),
        pltpu.VMEM((2, NB, NB, 8, TILE), F32),
        pltpu.VMEM((NB, 8, half), F32),
        pltpu.VMEM((NB, KTOK, half), BF16),
        pltpu.VMEM((2, NB, 2, 192, 128), BF16),
        pltpu.VMEM((2, NB, 2, 192, 128), BF16),
        pltpu.VMEM((KTOK, 256), F32),
        pltpu.VMEM((KTOK, 128), F32),
        pltpu.VMEM((NA, ROWS, 384), BF16),
        pltpu.VMEM((NA, ROWS, 256), BF16),
        pltpu.VMEM((NA, ROWS, 384), BF16),
        pltpu.VMEM((NA, ROWS, 256), BF16),
        pltpu.VMEM((NA, 192, 128), BF16),
        pltpu.VMEM((NA, 192, 128), BF16),
        pltpu.VMEM((NB * NY, 64, 256), BF16),
        pltpu.VMEM((NB * NY, 64, 256), BF16),
        pltpu.VMEM((64, 128), BF16),
        pltpu.VMEM((64, 128), BF16),
        pltpu.VMEM((NY, 2, 288, ROWS), F32),
        pltpu.VMEM((NY, 288, ROWS), BF16),
        pltpu.VMEM((NY, 288, ROWS), BF16),
        pltpu.VMEM((NY, 288, ROWS), BF16),
        pltpu.VMEM((3, 288, ROWS), BF16),
        pltpu.VMEM((288, ROWS), F32),
        pltpu.VMEM((288, ROWS), F32),
        pltpu.VMEM((ROWS, 768), BF16),
        pltpu.VMEM((NA, NB * NY, 64, 128), BF16),
        pltpu.VMEM((NA, NB * NY, 64, 128), BF16),
    ]
    sems = [
        dma((5,)), dma, dma((3,)), dma, dma((3,)), dma, dma,
        dma, dma((3, 2)), dma, dma, dma, dma,
        dma, dma((2, 4)), dma, dma,
        dma, dma, dma, dma, dma, dma, dma, dma,
        dma, dma((7,)), dma, dma((3,)), dma, dma((7,)), dma, dma((3,)),
        dma((3,)), dma((3,)), dma((4,)),
    ]
    hbm = pl.BlockSpec(memory_space=pltpu.HBM)
    qg, lg, ugk, ugv = pl.pallas_call(
        whole_kernel,
        out_shape=(
            shape((ROWS, 768)),
            shape((2, 288, ROWS), F32),
            shape((NA, NB * NY, 64, 128)),
            shape((NA, NB * NY, 64, 128)),
        ),
        in_specs=[SMEM] + [hbm] * 5,
        out_specs=(hbm,) * 4,
        scratch_shapes=scratch + sems,
        compiler_params=pltpu.CompilerParams(
            collective_id=0, has_side_effects=True, vmem_limit_bytes=LIMIT * 1024 * 1024
        ),
    )(positions, queries, latents.T, key_up, value_up, out_grad)
    qg, lg, kug, vug = pl.pallas_call(
        final_kernel,
        out_shape=(
            shape((ROWS, 768)),
            shape((2, 288, ROWS), F32),
            shape((D_LAT, 512), F32),
            shape((D_LAT, 512), F32),
        ),
        in_specs=[hbm] * 4,
        out_specs=(hbm,) * 4,
        scratch_shapes=[
            pltpu.VMEM((ROWS, 768), BF16),
            pltpu.VMEM((2, 288, ROWS), F32),
            pltpu.VMEM((NA, NB * NY, 64, 128), BF16),
            pltpu.VMEM((NA, NB * NY, 64, 128), BF16),
            pltpu.VMEM((D_LAT, 512), F32),
            pltpu.VMEM((D_LAT, 512), F32),
            dma((10,)),
            dma((10,)),
        ],
        compiler_params=pltpu.CompilerParams(vmem_limit_bytes=LIMIT * 1024 * 1024),
    )(qg, lg, ugk, ugv)
    return (qg, lg.reshape(576, ROWS).T, kug, vug)


def solution(mesh):
    in_specs = (
        P("seq", "head"),
        P("seq", None),
        P(None, "head"),
        P(None, "head"),
        P("seq", "head"),
        P("seq"),
    )
    out_specs = (P("seq", "head"), P("seq", None), P(None, "head"), P(None, "head"))
    return jax.shard_map(shards, mesh=mesh, in_specs=in_specs, out_specs=out_specs, check_vma=False)
```

```python
import math

import jax
import jax.numpy as jnp
from jax import lax
from jax.experimental import pallas as pl
from jax.experimental.pallas import tpu as pltpu
from jax.sharding import PartitionSpec as P


D_LAT = 512
D_ROPE = 64
D_NOPE = 128
D_V = 128
ROWS = 128
NA = 4
NB = 4
NY = 2
BLOCK = 336
KTOK = NY * NA * ROWS
TILE = 256
NEG = -1e30
LIMIT = 60
FLOOR = -1e29
SCALE = 1.0 / math.sqrt(D_NOPE + D_ROPE)
LOG2E = math.log2(math.e)
MESH = pl.DeviceIdType.MESH
F32 = jnp.float32
BF16 = jnp.bfloat16
VMEM = pl.BlockSpec(memory_space=pltpu.VMEM)
SMEM = pl.BlockSpec(memory_space=pltpu.SMEM)
NT = (((1,), (1,)), ((), ()))
TN = (((0,), (0,)), ((), ()))


def coords():
    seq = lax.axis_index("seq")
    head = lax.axis_index("head")
    core = head % 2
    y = seq // 16
    z = (seq // 4) % 4
    x = seq % 4
    a = x + core * (z - x)
    b = z + core * (x - z)
    sa = 1 + 3 * core
    sb = 4 - 3 * core

    def dev(a2, b2, y2):
        return (y2 * 16 + a2 * sa + b2 * sb, head)

    return seq, head, y, a, b, dev


def rcopy(src, dst, send, recv, device):
    return pltpu.make_async_remote_copy(
        src_ref=src, dst_ref=dst, send_sem=send, recv_sem=recv, device_id=device, device_id_type=MESH
    )


def dot(u, v, dims=(((1,), (0,)), ((), ()))):
    return lax.dot_general(u, v, dims, preferred_element_type=F32)


def shape(dims, dtype=BF16):
    return jax.ShapeDtypeStruct(dims, dtype)


def whole_kernel(
    pos_ref, q_hbm, latt_hbm, ku_hbm, vu_hbm, g_hbm,
    qg_hbm, lg_hbm, ugk_hbm, ugv_hbm,
    q_ref, latt_ref, ku_ref, vu_ref, g_ref,
    pq, pk, qb, kb, qp, kp, kpt, cl, kpos, s_all, dp_all, stl, sb, rows, ds_all, dqs, rq, dka, dva, gs0, gs1, rg0, rg1,
    dqf, rdq, ups, rup, usk, usv, lsum, lhalf, rhalf, hs, rh, lfin, rfin, qg_ref, ugk, ugv,
    s_in, s_aq, r_aq, s_ak, r_ak, s_al, r_al, s_bq, r_bq, s_yk, r_yk, s_yl, r_yl, s_st, r_st, s_dq, r_dq,
    s_g0, r_g0, s_g1, r_g1, s_qf, r_qf, s_up, r_up,
    s_kb, r_kb, s_ka, r_ka, s_va, r_va, s_vb, r_vb, s_h, r_h, s_out,
):
    seq, head, y, a, b, dev = coords()
    core = head % 2
    twin = (seq, head + 1 - 2 * core)
    far = (seq, (head + 2) % 4)
    across = dev(a, b, 1 - y)
    corner = (across[0], (head + 2) % 4)
    near = (1, 3, 2)
    others = [(0, 1), (1, 0), (1, 1), (2, 0), (2, 1), (3, 0), (3, 1)]
    by_reach = (1, 5, 0, 3, 2, 6, 4)
    far_first = by_reach[::-1]

    barrier = pltpu.get_barrier_semaphore()
    for p in (
        [dev((a + d) % NA, b, y) for d in near]
        + [dev(a, (b + e) % NB, (y + f) % NY) for e, f in others]
        + [dev((a + d) % NA, b, 1 - y) for d in near]
        + [twin, far, corner]
    ):
        pl.semaphore_signal(barrier, inc=1, device_id=p, device_id_type=MESH)

    def go(src, dst, send, recv, device):
        rcopy(src, dst, send, recv, device).start()

    def landed(ref, recv):
        rcopy(ref, ref, recv, recv, across).wait_recv()

    def left(ref, send):
        rcopy(ref, ref, send, send, across).wait_send()

    loads = [
        pltpu.make_async_copy(src, dst, s_in.at[i])
        for i, (src, dst) in enumerate(
            [(q_hbm, q_ref), (g_hbm, g_ref), (latt_hbm, latt_ref), (ku_hbm, ku_ref), (vu_hbm, vu_ref)]
        )
    ]
    for c in loads:
        c.start()
    loads[0].wait()
    loads[1].wait()

    stripe = lax.shift_right_logical(pos_ref[0], 7).astype(F32)
    stripes = jnp.full((16, 128), stripe, F32).astype(BF16)
    for h in range(NA):
        q = q_ref[:, h * 192 : (h + 1) * 192]
        pq[h, 0:128, :] = q[:, :128]
        pq[h, 128:256, :] = g_ref[:, h * 128 : (h + 1) * 128]
        pq[h, 256:320, :] = jnp.concatenate([q[:64, 128:], q[64:, 128:]], axis=1)
        pq[h, 320:, :] = stripes
    qb[0, 0] = pq[a]
    for c in loads[2:]:
        c.wait()
    comp = latt_ref[:D_LAT, :]
    kn = dot(comp, ku_ref[...], TN).astype(BF16)
    vv = dot(comp, vu_ref[...], TN).astype(BF16)
    eye = (
        lax.broadcasted_iota(jnp.int32, (64, 128), 0) == lax.broadcasted_iota(jnp.int32, (64, 128), 1)
    ).astype(F32).astype(BF16)
    k_rope = dot(latt_ref[D_LAT:, :], eye, TN).astype(BF16)
    k_rope = jnp.concatenate([k_rope[:64, :64], k_rope[64:, :64]], axis=1)
    for h in range(NA):
        pk[h, 0:128, :] = kn[:, h * 128 : (h + 1) * 128]
        pk[h, 128:256, :] = vv[:, h * 128 : (h + 1) * 128]
        pk[h, 256:320, :] = k_rope
        pk[h, 320:, :] = stripes
    kb[0, 0] = pk[a]
    cl[0, 0] = comp

    pl.semaphore_wait(barrier, 6 + len(others) + 3)

    def on_a(d):
        return dev((a + d) % NA, b, y)

    def on_b(e):
        return dev(a, (b + e) % NB, y)

    def tile_of(d):
        return 0 if d < 2 else 1

    for d in near:
        go(pk.at[(a + d) % NA], kb.at[0, d], s_ak, r_ak.at[d - 1], on_a(d))
    go(pk.at[a], kb.at[1, 0], s_yk, r_yk, across)
    for d in near:
        go(pq.at[(a + d) % NA], qb.at[0, d], s_aq, r_aq.at[d - 1], on_a(d))
    for e in near:
        go(pq.at[a], qb.at[e, 0], s_bq, r_bq.at[e - 1, 0], on_b(e))
    def pass_q(d):
        landed(qb.at[0, d], r_aq.at[d - 1])
        for e in near:
            go(qb.at[0, d], qb.at[e, d], s_bq, r_bq.at[e - 1, tile_of(d)], on_b(e))

    def pass_k(d):
        landed(kb.at[0, d], r_ak.at[d - 1])
        go(kb.at[0, d], kb.at[1, d], s_yk, r_yk, across)

    pass_k(1)
    pass_k(3)
    pass_k(2)
    pass_q(1)
    pass_q(3)
    pass_q(2)
    go(latt_ref.at[pl.ds(0, D_LAT)], cl.at[1, 0], s_yl, r_yl, across)

    half = NA * ROWS
    row = lax.broadcasted_iota(jnp.int32, (ROWS, TILE), 0).astype(F32)
    col = lax.broadcasted_iota(jnp.int32, (1, ROWS), 1).astype(F32)
    blank = jnp.zeros((ROWS, 64), BF16)
    pairs = ((0, 1), (3, 2))

    def wide(block):
        rope = jnp.concatenate([block[256:320, :64], block[256:320, 64:]], axis=0)
        return jnp.concatenate([block[:128, :], rope, blank], axis=1)

    def open_keys(k):
        for d in range(NA):
            at = slice(d * ROWS, (d + 1) * ROWS)
            block = kb[k, d]
            kp[k, at, :] = wide(block)
            stripe = block[320:321, :].astype(F32) * 128.0
            kpos[k, at, :] = jnp.concatenate([stripe, stripe], axis=1) + row

    def open_queries(e, t):
        for i, d in enumerate(pairs[t]):
            at = slice(t * TILE + i * ROWS, t * TILE + (i + 1) * ROWS)
            qp[e, at, :] = wide(qb[e, d])

    def wait_q(e, t):
        landed(qb.at[e, pl.ds(2 * t, 2)], r_bq.at[e - 1, t])

    def grads_of(e, t):
        d0, d1 = pairs[t]
        return jnp.concatenate([qb[e, d0, 128:256, :], qb[e, d1, 128:256, :]], axis=0)

    def unit(k, e, t, first):
        at = slice(t * TILE, (t + 1) * TILE)
        if first:
            open_queries(e, t)
        qpos = jnp.concatenate([qb[e, d, 320:321, :].astype(F32) * 128.0 + col for d in pairs[t]], axis=1)
        raw = dot(kp[k], qp[e, at, :], NT)
        s = jnp.where(kpos[k] <= qpos, raw * (SCALE * LOG2E), NEG)
        s_all[k, e, :, at] = s
        dp = dot(kb[k, :, 128:256, :].reshape(half, 128), grads_of(e, t), NT)
        dp_all[k, e, :, at] = dp
        top = jnp.max(s, axis=0, keepdims=True)
        if not first:
            old = stl[t, e, 0:1, :]
            top = jnp.maximum(top, old)
        w = jnp.exp2(s - jnp.maximum(top, FLOOR))
        total = jnp.sum(w, axis=0, keepdims=True)
        weighted = jnp.sum(w * dp, axis=0, keepdims=True)
        if not first:
            fade = jnp.exp2(old - top)
            total = total + fade * stl[t, e, 1:2, :]
            weighted = weighted + fade * stl[t, e, 2:3, :]
        stl[t, e, 0:1, :] = top
        stl[t, e, 1:2, :] = total
        stl[t, e, 2:3, :] = weighted

    def tell(t, e):
        for g in near:
            to = (e + g) % NB
            go(stl.at[t, e], sb.at[t, to, g], s_st, r_st.at[t, to], on_b(g))

    stl[...] = jnp.zeros_like(stl)
    open_keys(0)
    unit(0, 0, 0, True)
    unit(0, 0, 1, True)
    for e in near:
        wait_q(e, 0)
        unit(0, e, 0, True)
    landed(kb.at[1], r_yk)
    for d in near:
        go(latt_ref.at[pl.ds(0, D_LAT)], cl.at[0, d], s_al, r_al, on_a(d))
    open_keys(1)
    unit(1, 0, 0, False)
    tell(0, 0)
    for e in near:
        unit(1, e, 0, False)
        tell(0, e)
    unit(1, 0, 1, False)
    tell(1, 0)
    for e in near:
        wait_q(e, 1)
        if e == 1:
            landed(cl.at[1, 0], r_yl)
            for d in near:
                go(cl.at[1, 0], cl.at[1, d], s_al, r_al, on_a(d))
        unit(0, e, 1, True)
        unit(1, e, 1, False)
        tell(1, e)
    kpt[...] = kp[...].reshape(KTOK, 256).T

    def backward(k, t):
        ks = slice(k * half, (k + 1) * half)
        at = slice(t * TILE, (t + 1) * TILE)
        for n, e in enumerate((0, 1, 3, 2)):
            if k == 1:
                landed(sb.at[t, e, pl.ds(1, 3)], r_st.at[t, e])
                got = [stl[t, e]] + [sb[t, e, g] for g in near]
                tops = [r[0:1, :] for r in got]
                top = jnp.maximum(jnp.maximum(tops[0], tops[1]), jnp.maximum(tops[2], tops[3]))
                fades = [jnp.exp2(u - top) for u in tops]
                total = sum(f * r[1:2, :] for f, r in zip(fades, got))
                rows[e, 1:2, at] = sum(f * r[2:3, :] for f, r in zip(fades, got)) / total
                rows[e, 0:1, at] = top + jnp.log(total) * LOG2E
            p = jnp.exp2(s_all[k, e, :, at] - rows[e, 0:1, at])
            ds = (p * (dp_all[k, e, :, at] - rows[e, 1:2, at]) * SCALE).astype(BF16)
            ds_all[e, ks, at] = ds
            dv = dot(p.astype(BF16), grads_of(e, t))
            dk = dot(ds, qp[e, at, :])
            if n == 0 and t == 0:
                dva[ks, :] = dv
                dka[ks, :] = dk
            else:
                dva[ks, :] += dv
                dka[ks, :] += dk

    def query_sums(t):
        at = slice(t * TILE, (t + 1) * TILE)
        for e in (2, 1, 3, 0):
            dq = dot(kpt[:192, :], ds_all[e, :, at]).astype(BF16)
            dqs[t, e, 0] = dq[:, :ROWS]
            dqs[t, e, 1] = dq[:, ROWS:]
            if e:
                go(dqs.at[t, e], rq.at[t, e], s_dq, r_dq, on_b(NB - e))

    backward(1, 0)
    backward(0, 0)
    query_sums(0)
    backward(1, 1)
    for d in range(NA):
        at = slice(half + d * ROWS, half + (d + 1) * ROWS)
        gs1[d, :, :128] = dka[at, :128].astype(BF16)
        gs1[d, :, 128:] = dva[at, :].astype(BF16)
    for d in near:
        go(gs1.at[d], rg1.at[a], s_g1, r_g1, on_a(NA - d))
    backward(0, 1)
    for d in range(NA):
        at = slice(d * ROWS, (d + 1) * ROWS)
        at1 = slice(half + d * ROWS, half + (d + 1) * ROWS)
        gs0[d, :, :128] = dka[at, :128].astype(BF16)
        gs0[d, :, 128:256] = dva[at, :].astype(BF16)
        gs0[d, :, 256:] = jnp.concatenate([dka[at, 128:192], dka[at1, 128:192]], axis=1).astype(BF16)
    for d in near:
        go(gs0.at[d], rg0.at[a], s_g0, r_g0, on_a(NA - d))

    landed(cl.at[:, pl.ds(1, 3)], r_al)
    g = jnp.concatenate([dka[:, :128], dva[...]], axis=1).astype(BF16)
    comps = jnp.concatenate([cl[k, i] for k in range(NY) for i in range(NA)], axis=1)
    up = dot(comps, g)
    for i in range(NB * NY):
        ups[i] = up[i * 64 : (i + 1) * 64, :].astype(BF16)
    mine = b * NY + y
    for i in far_first:
        e, f = others[i]
        tb, ty = (b + e) % NB, (y + f) % NY
        go(ups.at[tb * NY + ty], rup.at[mine], s_up, r_up, dev(a, tb, ty))
    rup[mine] = ups[mine]

    query_sums(1)
    rg0[a] = gs0[0]
    rg1[a] = gs1[0]

    landed(rup.at[pl.ds(0, 7)], r_up)
    us = sum(rup[i].astype(F32) for i in range(NB * NY)).astype(BF16)
    usk[...] = us[:, :128]
    usv[...] = us[:, 128:]
    ugk[a, mine] = us[:, :128]
    ugv[a, mine] = us[:, 128:]
    for i in far_first:
        e, f = others[i]
        fy = (y + f) % NY
        go(usk, ugk.at[a, mine], s_kb, r_kb.at[i], dev(a, (b + e) % NB, fy))
        go(usv, ugv.at[a, mine], s_va, r_va.at[i], dev((a + e) % NA, b, fy))

    def k_over_a(slot):
        for d in near:
            go(slot, slot, s_ka, r_ka.at[d - 1], on_a(d))

    def v_over_b(slot):
        for e in near:
            go(slot, slot, s_vb, r_vb.at[e - 1], on_b(e))

    k_over_a(ugk.at[a, mine])
    v_over_b(ugv.at[a, mine])

    landed(rg1.at[pl.ds(0, 3)], r_g1)
    landed(rg0.at[pl.ds(0, 3)], r_g0)
    dk_all = jnp.concatenate(
        [jnp.concatenate([r[h, :, :128] for h in range(NA)], axis=1) for r in (rg0, rg1)], axis=0
    )
    dv_all = jnp.concatenate(
        [jnp.concatenate([r[h, :, 128:256] for h in range(NA)], axis=1) for r in (rg0, rg1)], axis=0
    )
    lp = dot(ku_ref[...], dk_all, NT) + dot(vu_ref[...], dv_all, NT)
    rope = sum(rg0[h, :, 256:].astype(F32) for h in range(NA)).T
    for k in range(NY):
        whole = jnp.concatenate([lp[:, k * 128 : (k + 1) * 128], rope[k * 64 : (k + 1) * 64, :]], axis=0)
        lsum[k] = whole.reshape(2, 288, ROWS)
    for k in range(NY):
        lhalf[k] = lsum[k, 1 - core].astype(BF16)
    go(lhalf, rhalf, s_h.at[0], r_h.at[0], twin)

    def piece(i, axis):
        e, f = others[i]
        if axis == "b":
            return (b + NB - e) % NB * NY + (y + f) % NY
        return (a + NA - e) % NA, (y + f) % NY

    def pass_on(i):
        slot = ugk.at[a, piece(i, "b")]
        landed(slot, r_kb.at[i])
        k_over_a(slot)
        fa, fy = piece(i, "a")
        slot = ugv.at[fa, b * NY + fy]
        landed(slot, r_va.at[i])
        v_over_b(slot)

    for i in by_reach[:4]:
        pass_on(i)
    landed(rhalf, r_h.at[0])
    for k in range(NY):
        hs[k] = (lsum[k, core] + rhalf[k].astype(F32)).astype(BF16)
    go(hs.at[0], rh.at[0], s_h.at[1], r_h.at[1], far)
    go(hs.at[1], rh.at[1], s_h.at[1], r_h.at[1], across)
    go(hs.at[1], rh.at[2], s_h.at[1], r_h.at[1], corner)

    for i in by_reach[4:]:
        pass_on(i)
    landed(rq.at[:, pl.ds(1, 3)], r_dq)
    for t in range(2):
        for i, d in enumerate(pairs[t]):
            dqf[d] = (dqs[t, 0, i].astype(F32) + sum(rq[t, e, i].astype(F32) for e in near)).astype(BF16)
    for d in near:
        go(dqf.at[d], rdq.at[a], s_qf, r_qf, on_a(NA - d))
    rdq[a] = dqf[0]

    landed(rh, r_h.at[1])
    whole = hs[0].astype(F32) + rh[0].astype(F32) + rh[1].astype(F32) + rh[2].astype(F32)
    lfin[...] = whole
    go(lfin, rfin, s_h.at[2], r_h.at[2], twin)

    landed(rdq.at[pl.ds(0, 3)], r_qf)
    for h in range(NA):
        qg_ref[:, h * 192 : (h + 1) * 192] = rdq[h].T

    def write(src, dst, sem):
        pltpu.make_async_copy(src, dst, s_out.at[sem]).start()

    write(qg_ref, qg_hbm, 0)
    write(ugk.at[a], ugk_hbm.at[a], 2)
    own_b = pl.ds(b * NY, NY)
    write(ugv.at[:, own_b], ugv_hbm.at[:, own_b], 3)

    for d in near:
        fa, from_b = (a + NA - d) % NA, pl.ds((b + NB - d) % NB * NY, NY)
        landed(ugk.at[fa], r_ka.at[d - 1])
        write(ugk.at[fa], ugk_hbm.at[fa], 2)
        landed(ugv.at[:, from_b], r_vb.at[d - 1])
        write(ugv.at[:, from_b], ugv_hbm.at[:, from_b], 3)
    landed(rfin, r_h.at[2])
    write(lfin, lg_hbm.at[core], 1)
    write(rfin, lg_hbm.at[1 - core], 1)
    left(pq.at[pl.ds(0, 3)], s_aq)
    left(pk.at[pl.ds(0, 3)], s_ak)
    left(qb.at[pl.ds(0, 3)], s_bq)
    left(kb.at[0], s_yk)
    left(cl.at[1, 0], s_yl)
    left(cl.at[:, pl.ds(1, 3)], s_al)
    left(sb.at[:, pl.ds(0, 3)], s_st)
    left(rq.at[:, pl.ds(1, 3)], s_dq)
    left(rg0.at[pl.ds(0, 3)], s_g0)
    left(rg1.at[pl.ds(0, 3)], s_g1)
    left(rdq.at[pl.ds(0, 3)], s_qf)
    left(rup.at[pl.ds(0, 7)], s_up)
    left(ugk.at[0, pl.ds(0, 7)], s_kb)
    left(ugk.at[0, pl.ds(0, 7)], s_va)
    left(ugk.at[pl.ds(0, 3)], s_ka)
    left(ugv.at[pl.ds(0, 3)], s_vb)
    left(lhalf, s_h.at[0])
    left(rh, s_h.at[1])
    left(lfin, s_h.at[2])
    pltpu.make_async_copy(qg_ref, qg_hbm, s_out.at[0]).wait()
    pltpu.make_async_copy(lsum.at[0], lg_hbm, s_out.at[1]).wait()
    pltpu.make_async_copy(ugk, ugk_hbm, s_out.at[2]).wait()
    pltpu.make_async_copy(ugv, ugv_hbm, s_out.at[3]).wait()


def final_kernel(
    qg_hbm, lg_hbm, ugk_hbm, ugv_hbm, qg_ref, lg_ref, kug_ref, vug_ref, qv, lv, kv, vv, kf, vf, s_in, s_out
):
    quarter = D_LAT // 4
    loads, outs = [], []

    def start(pile, src, dst, sem):
        c = pltpu.make_async_copy(src, dst, sem)
        c.start()
        pile.append(c)

    for i in range(4):
        at = pl.ds(2 * i, 2)
        start(loads, ugk_hbm.at[:, at], kv.at[:, at], s_in.at[2 * i])
        start(loads, ugv_hbm.at[:, at], vv.at[:, at], s_in.at[2 * i + 1])
    start(loads, qg_hbm, qv, s_in.at[8])
    start(loads, lg_hbm, lv, s_in.at[9])
    for i in range(4):
        at = pl.ds(i * quarter, quarter)
        for n, (src, dst, out) in enumerate([(kv, kf, kug_ref), (vv, vf, vug_ref)]):
            loads[2 * i + n].wait()
            for h in range(NA):
                dst[i * quarter : (i + 1) * quarter, h * 128 : (h + 1) * 128] = (
                    src[h, 2 * i : 2 * i + 2].reshape(quarter, 128).astype(F32)
                )
            start(outs, dst.at[at], out.at[at], s_out.at[2 * i + n])
    loads[8].wait()
    start(outs, qv, qg_ref, s_out.at[8])
    loads[9].wait()
    start(outs, lv, lg_ref, s_out.at[9])
    for c in outs:
        c.wait()


def shards(queries, latents, key_up, value_up, out_grad, positions):
    half = NA * ROWS
    dma = pltpu.SemaphoreType.DMA
    scratch = [
        pltpu.VMEM((ROWS, 768), BF16),
        pltpu.VMEM((576, ROWS), BF16),
        pltpu.VMEM((D_LAT, 512), BF16),
        pltpu.VMEM((D_LAT, 512), BF16),
        pltpu.VMEM((ROWS, 512), BF16),
        pltpu.VMEM((NA, BLOCK, 128), BF16),
        pltpu.VMEM((NA, BLOCK, 128), BF16),
        pltpu.VMEM((NB, NA, BLOCK, 128), BF16),
        pltpu.VMEM((NY, NA, BLOCK, 128), BF16),
        pltpu.VMEM((NB, half, 256), BF16),
        pltpu.VMEM((NY, half, 256), BF16),
        pltpu.VMEM((256, KTOK), BF16),
        pltpu.VMEM((NY, NA, D_LAT, ROWS), BF16),
        pltpu.VMEM((NY, half, TILE), F32),
        pltpu.VMEM((NY, NB, half, half), F32),
        pltpu.VMEM((NY, NB, half, half), F32),
        pltpu.VMEM((2, NB, 8, TILE), F32),
        pltpu.VMEM((2, NB, NB, 8, TILE), F32),
        pltpu.VMEM((NB, 8, half), F32),
        pltpu.VMEM((NB, KTOK, half), BF16),
        pltpu.VMEM((2, NB, 2, 192, 128), BF16),
        pltpu.VMEM((2, NB, 2, 192, 128), BF16),
        pltpu.VMEM((KTOK, 256), F32),
        pltpu.VMEM((KTOK, 128), F32),
        pltpu.VMEM((NA, ROWS, 384), BF16),
        pltpu.VMEM((NA, ROWS, 256), BF16),
        pltpu.VMEM((NA, ROWS, 384), BF16),
        pltpu.VMEM((NA, ROWS, 256), BF16),
        pltpu.VMEM((NA, 192, 128), BF16),
        pltpu.VMEM((NA, 192, 128), BF16),
        pltpu.VMEM((NB * NY, 64, 256), BF16),
        pltpu.VMEM((NB * NY, 64, 256), BF16),
        pltpu.VMEM((64, 128), BF16),
        pltpu.VMEM((64, 128), BF16),
        pltpu.VMEM((NY, 2, 288, ROWS), F32),
        pltpu.VMEM((NY, 288, ROWS), BF16),
        pltpu.VMEM((NY, 288, ROWS), BF16),
        pltpu.VMEM((NY, 288, ROWS), BF16),
        pltpu.VMEM((3, 288, ROWS), BF16),
        pltpu.VMEM((288, ROWS), F32),
        pltpu.VMEM((288, ROWS), F32),
        pltpu.VMEM((ROWS, 768), BF16),
        pltpu.VMEM((NA, NB * NY, 64, 128), BF16),
        pltpu.VMEM((NA, NB * NY, 64, 128), BF16),
    ]
    sems = [
        dma((5,)), dma, dma((3,)), dma, dma((3,)), dma, dma,
        dma, dma((3, 2)), dma, dma, dma, dma,
        dma, dma((2, 4)), dma, dma,
        dma, dma, dma, dma, dma, dma, dma, dma,
        dma, dma((7,)), dma, dma((3,)), dma, dma((7,)), dma, dma((3,)),
        dma((3,)), dma((3,)), dma((4,)),
    ]
    hbm = pl.BlockSpec(memory_space=pltpu.HBM)
    qg, lg, ugk, ugv = pl.pallas_call(
        whole_kernel,
        out_shape=(
            shape((ROWS, 768)),
            shape((2, 288, ROWS), F32),
            shape((NA, NB * NY, 64, 128)),
            shape((NA, NB * NY, 64, 128)),
        ),
        in_specs=[SMEM] + [hbm] * 5,
        out_specs=(hbm,) * 4,
        scratch_shapes=scratch + sems,
        compiler_params=pltpu.CompilerParams(
            collective_id=0, has_side_effects=True, vmem_limit_bytes=LIMIT * 1024 * 1024
        ),
    )(positions, queries, latents.T, key_up, value_up, out_grad)
    qg, lg, kug, vug = pl.pallas_call(
        final_kernel,
        out_shape=(
            shape((ROWS, 768)),
            shape((2, 288, ROWS), F32),
            shape((D_LAT, 512), F32),
            shape((D_LAT, 512), F32),
        ),
        in_specs=[hbm] * 4,
        out_specs=(hbm,) * 4,
        scratch_shapes=[
            pltpu.VMEM((ROWS, 768), BF16),
            pltpu.VMEM((2, 288, ROWS), F32),
            pltpu.VMEM((NA, NB * NY, 64, 128), BF16),
            pltpu.VMEM((NA, NB * NY, 64, 128), BF16),
            pltpu.VMEM((D_LAT, 512), F32),
            pltpu.VMEM((D_LAT, 512), F32),
            dma((10,)),
            dma((10,)),
        ],
        compiler_params=pltpu.CompilerParams(vmem_limit_bytes=LIMIT * 1024 * 1024),
    )(qg, lg, ugk, ugv)
    return (qg, lg.reshape(576, ROWS).T, kug, vug)


def solution(mesh):
    in_specs = (
        P("seq", "head"),
        P("seq", None),
        P(None, "head"),
        P(None, "head"),
        P("seq", "head"),
        P("seq"),
    )
    out_specs = (P("seq", "head"), P("seq", None), P(None, "head"), P(None, "head"))
    return jax.shard_map(shards, mesh=mesh, in_specs=in_specs, out_specs=out_specs, check_vma=False)
```

```python
import math

import jax
import jax.numpy as jnp
from jax import lax
from jax.experimental import pallas as pl
from jax.experimental.pallas import tpu as pltpu
from jax.sharding import PartitionSpec as P


D_LAT = 512
D_ROPE = 64
D_NOPE = 128
D_V = 128
ROWS = 128
NA = 4
NB = 4
NY = 2
BLOCK = 336
KTOK = NY * NA * ROWS
TILE = 256
NEG = -1e30
LIMIT = 60
FLOOR = -1e29
SCALE = 1.0 / math.sqrt(D_NOPE + D_ROPE)
LOG2E = math.log2(math.e)
MESH = pl.DeviceIdType.MESH
F32 = jnp.float32
BF16 = jnp.bfloat16
VMEM = pl.BlockSpec(memory_space=pltpu.VMEM)
NT = (((1,), (1,)), ((), ()))
TN = (((0,), (0,)), ((), ()))


def coords():
    seq = lax.axis_index("seq")
    head = lax.axis_index("head")
    core = head % 2
    y = seq // 16
    z = (seq // 4) % 4
    x = seq % 4
    a = x + core * (z - x)
    b = z + core * (x - z)
    sa = 1 + 3 * core
    sb = 4 - 3 * core

    def dev(a2, b2, y2):
        return (y2 * 16 + a2 * sa + b2 * sb, head)

    return seq, head, y, a, b, dev


def rcopy(src, dst, send, recv, device):
    return pltpu.make_async_remote_copy(
        src_ref=src, dst_ref=dst, send_sem=send, recv_sem=recv, device_id=device, device_id_type=MESH
    )


def dot(u, v, dims=(((1,), (0,)), ((), ()))):
    return lax.dot_general(u, v, dims, preferred_element_type=F32)


def shape(dims, dtype=BF16):
    return jax.ShapeDtypeStruct(dims, dtype)


def whole_kernel(
    pos_hbm, q_hbm, latt_hbm, ku_hbm, vu_hbm, g_hbm,
    qg_hbm, lg_hbm, ugk_hbm, ugv_hbm,
    pos_ref, q_ref, latt_ref, ku_ref, vu_ref, g_ref,
    pq, pk, qb, kb, qp, kp, kpt, cl, kpos, s_all, dp_all, stl, sb, rows, ds_all, dqs, rq, dka, dva, gs0, gs1, rg0, rg1,
    dqf, rdq, ups, rup, usk, usv, lsum, lhalf, rhalf, hs, rh, lfin, rfin, qg_ref, ugk, ugv,
    s_in, s_aq, r_aq, s_ak, r_ak, s_al, r_al, s_bq, r_bq, s_yk, r_yk, s_yl, r_yl, s_st, r_st, s_dq, r_dq,
    s_g0, r_g0, s_g1, r_g1, s_qf, r_qf, s_up, r_up,
    s_kb, r_kb, s_ka, r_ka, s_va, r_va, s_vb, r_vb, s_h, r_h, s_out,
):
    seq, head, y, a, b, dev = coords()
    core = head % 2
    twin = (seq, head + 1 - 2 * core)
    far = (seq, (head + 2) % 4)
    across = dev(a, b, 1 - y)
    corner = (across[0], (head + 2) % 4)
    near = (1, 3, 2)
    others = [(0, 1), (1, 0), (1, 1), (2, 0), (2, 1), (3, 0), (3, 1)]
    by_reach = (1, 5, 0, 3, 2, 6, 4)
    far_first = by_reach[::-1]

    barrier = pltpu.get_barrier_semaphore()
    for p in (
        [dev((a + d) % NA, b, y) for d in near]
        + [dev(a, (b + e) % NB, (y + f) % NY) for e, f in others]
        + [dev((a + d) % NA, b, 1 - y) for d in near]
        + [twin, far, corner]
    ):
        pl.semaphore_signal(barrier, inc=1, device_id=p, device_id_type=MESH)

    def go(src, dst, send, recv, device):
        rcopy(src, dst, send, recv, device).start()

    def landed(ref, recv):
        rcopy(ref, ref, recv, recv, across).wait_recv()

    def left(ref, send):
        rcopy(ref, ref, send, send, across).wait_send()

    loads = [
        pltpu.make_async_copy(src, dst, s_in.at[i])
        for i, (src, dst) in enumerate(
            [(pos_hbm, pos_ref), (q_hbm, q_ref), (g_hbm, g_ref), (latt_hbm, latt_ref), (ku_hbm, ku_ref), (vu_hbm, vu_ref)]
        )
    ]
    for c in loads:
        c.start()
    for c in loads[:3]:
        c.wait()

    stripe = lax.shift_right_logical(pos_ref[0], 7).astype(F32)
    stripes = jnp.full((16, 128), stripe, F32).astype(BF16)
    for h in range(NA):
        q = q_ref[:, h * 192 : (h + 1) * 192]
        pq[h, 0:128, :] = q[:, :128]
        pq[h, 128:256, :] = g_ref[:, h * 128 : (h + 1) * 128]
        pq[h, 256:320, :] = jnp.concatenate([q[:64, 128:], q[64:, 128:]], axis=1)
        pq[h, 320:, :] = stripes
    qb[0, 0] = pq[a]
    for c in loads[3:]:
        c.wait()
    comp = latt_ref[:D_LAT, :]
    kn = dot(comp, ku_ref[...], TN).astype(BF16)
    vv = dot(comp, vu_ref[...], TN).astype(BF16)
    eye = (
        lax.broadcasted_iota(jnp.int32, (64, 128), 0) == lax.broadcasted_iota(jnp.int32, (64, 128), 1)
    ).astype(F32).astype(BF16)
    k_rope = dot(latt_ref[D_LAT:, :], eye, TN).astype(BF16)
    k_rope = jnp.concatenate([k_rope[:64, :64], k_rope[64:, :64]], axis=1)
    for h in range(NA):
        pk[h, 0:128, :] = kn[:, h * 128 : (h + 1) * 128]
        pk[h, 128:256, :] = vv[:, h * 128 : (h + 1) * 128]
        pk[h, 256:320, :] = k_rope
        pk[h, 320:, :] = stripes
    kb[0, 0] = pk[a]
    cl[0, 0] = comp

    pl.semaphore_wait(barrier, 6 + len(others) + 3)

    def on_a(d):
        return dev((a + d) % NA, b, y)

    def on_b(e):
        return dev(a, (b + e) % NB, y)

    def tile_of(d):
        return 0 if d < 2 else 1

    for d in near:
        go(pk.at[(a + d) % NA], kb.at[0, d], s_ak, r_ak.at[d - 1], on_a(d))
    go(pk.at[a], kb.at[1, 0], s_yk, r_yk, across)
    for d in near:
        go(pq.at[(a + d) % NA], qb.at[0, d], s_aq, r_aq.at[d - 1], on_a(d))
    for e in near:
        go(pq.at[a], qb.at[e, 0], s_bq, r_bq.at[e - 1, 0], on_b(e))
    def pass_q(d):
        landed(qb.at[0, d], r_aq.at[d - 1])
        for e in near:
            go(qb.at[0, d], qb.at[e, d], s_bq, r_bq.at[e - 1, tile_of(d)], on_b(e))

    def pass_k(d):
        landed(kb.at[0, d], r_ak.at[d - 1])
        go(kb.at[0, d], kb.at[1, d], s_yk, r_yk, across)

    pass_k(1)
    pass_k(3)
    pass_k(2)
    pass_q(1)
    pass_q(3)
    pass_q(2)
    go(latt_ref.at[pl.ds(0, D_LAT)], cl.at[1, 0], s_yl, r_yl, across)

    half = NA * ROWS
    row = lax.broadcasted_iota(jnp.int32, (ROWS, TILE), 0).astype(F32)
    col = lax.broadcasted_iota(jnp.int32, (1, ROWS), 1).astype(F32)
    blank = jnp.zeros((ROWS, 64), BF16)
    pairs = ((0, 1), (3, 2))

    def wide(block):
        rope = jnp.concatenate([block[256:320, :64], block[256:320, 64:]], axis=0)
        return jnp.concatenate([block[:128, :], rope, blank], axis=1)

    def open_keys(k):
        for d in range(NA):
            at = slice(d * ROWS, (d + 1) * ROWS)
            block = kb[k, d]
            kp[k, at, :] = wide(block)
            stripe = block[320:321, :].astype(F32) * 128.0
            kpos[k, at, :] = jnp.concatenate([stripe, stripe], axis=1) + row

    def open_queries(e, t):
        for i, d in enumerate(pairs[t]):
            at = slice(t * TILE + i * ROWS, t * TILE + (i + 1) * ROWS)
            qp[e, at, :] = wide(qb[e, d])

    def wait_q(e, t):
        landed(qb.at[e, pl.ds(2 * t, 2)], r_bq.at[e - 1, t])

    def grads_of(e, t):
        d0, d1 = pairs[t]
        return jnp.concatenate([qb[e, d0, 128:256, :], qb[e, d1, 128:256, :]], axis=0)

    def unit(k, e, t, first):
        at = slice(t * TILE, (t + 1) * TILE)
        if first:
            open_queries(e, t)
        qpos = jnp.concatenate([qb[e, d, 320:321, :].astype(F32) * 128.0 + col for d in pairs[t]], axis=1)
        raw = dot(kp[k], qp[e, at, :], NT)
        s = jnp.where(kpos[k] <= qpos, raw * (SCALE * LOG2E), NEG)
        s_all[k, e, :, at] = s
        dp = dot(kb[k, :, 128:256, :].reshape(half, 128), grads_of(e, t), NT)
        dp_all[k, e, :, at] = dp
        top = jnp.max(s, axis=0, keepdims=True)
        if not first:
            old = stl[t, e, 0:1, :]
            top = jnp.maximum(top, old)
        w = jnp.exp2(s - jnp.maximum(top, FLOOR))
        total = jnp.sum(w, axis=0, keepdims=True)
        weighted = jnp.sum(w * dp, axis=0, keepdims=True)
        if not first:
            fade = jnp.exp2(old - top)
            total = total + fade * stl[t, e, 1:2, :]
            weighted = weighted + fade * stl[t, e, 2:3, :]
        stl[t, e, 0:1, :] = top
        stl[t, e, 1:2, :] = total
        stl[t, e, 2:3, :] = weighted

    def tell(t, e):
        for g in near:
            to = (e + g) % NB
            go(stl.at[t, e], sb.at[t, to, g], s_st, r_st.at[t, to], on_b(g))

    stl[...] = jnp.zeros_like(stl)
    open_keys(0)
    unit(0, 0, 0, True)
    unit(0, 0, 1, True)
    for e in near:
        wait_q(e, 0)
        unit(0, e, 0, True)
    landed(kb.at[1], r_yk)
    for d in near:
        go(latt_ref.at[pl.ds(0, D_LAT)], cl.at[0, d], s_al, r_al, on_a(d))
    open_keys(1)
    unit(1, 0, 0, False)
    tell(0, 0)
    for e in near:
        unit(1, e, 0, False)
        tell(0, e)
    unit(1, 0, 1, False)
    tell(1, 0)
    for e in near:
        wait_q(e, 1)
        if e == 1:
            landed(cl.at[1, 0], r_yl)
            for d in near:
                go(cl.at[1, 0], cl.at[1, d], s_al, r_al, on_a(d))
        unit(0, e, 1, True)
        unit(1, e, 1, False)
        tell(1, e)
    kpt[...] = kp[...].reshape(KTOK, 256).T

    def backward(k, t):
        ks = slice(k * half, (k + 1) * half)
        at = slice(t * TILE, (t + 1) * TILE)
        for n, e in enumerate((0, 1, 3, 2)):
            if k == 1:
                landed(sb.at[t, e, pl.ds(1, 3)], r_st.at[t, e])
                got = [stl[t, e]] + [sb[t, e, g] for g in near]
                tops = [r[0:1, :] for r in got]
                top = jnp.maximum(jnp.maximum(tops[0], tops[1]), jnp.maximum(tops[2], tops[3]))
                fades = [jnp.exp2(u - top) for u in tops]
                total = sum(f * r[1:2, :] for f, r in zip(fades, got))
                rows[e, 1:2, at] = sum(f * r[2:3, :] for f, r in zip(fades, got)) / total
                rows[e, 0:1, at] = top + jnp.log(total) * LOG2E
            p = jnp.exp2(s_all[k, e, :, at] - rows[e, 0:1, at])
            ds = (p * (dp_all[k, e, :, at] - rows[e, 1:2, at]) * SCALE).astype(BF16)
            ds_all[e, ks, at] = ds
            dv = dot(p.astype(BF16), grads_of(e, t))
            dk = dot(ds, qp[e, at, :])
            if n == 0 and t == 0:
                dva[ks, :] = dv
                dka[ks, :] = dk
            else:
                dva[ks, :] += dv
                dka[ks, :] += dk

    def query_sums(t):
        at = slice(t * TILE, (t + 1) * TILE)
        for e in (2, 1, 3, 0):
            dq = dot(kpt[:192, :], ds_all[e, :, at]).astype(BF16)
            dqs[t, e, 0] = dq[:, :ROWS]
            dqs[t, e, 1] = dq[:, ROWS:]
            if e:
                go(dqs.at[t, e], rq.at[t, e], s_dq, r_dq, on_b(NB - e))

    backward(1, 0)
    backward(0, 0)
    query_sums(0)
    backward(1, 1)
    for d in range(NA):
        at = slice(half + d * ROWS, half + (d + 1) * ROWS)
        gs1[d, :, :128] = dka[at, :128].astype(BF16)
        gs1[d, :, 128:] = dva[at, :].astype(BF16)
    for d in near:
        go(gs1.at[d], rg1.at[a], s_g1, r_g1, on_a(NA - d))
    backward(0, 1)
    for d in range(NA):
        at = slice(d * ROWS, (d + 1) * ROWS)
        at1 = slice(half + d * ROWS, half + (d + 1) * ROWS)
        gs0[d, :, :128] = dka[at, :128].astype(BF16)
        gs0[d, :, 128:256] = dva[at, :].astype(BF16)
        gs0[d, :, 256:] = jnp.concatenate([dka[at, 128:192], dka[at1, 128:192]], axis=1).astype(BF16)
    for d in near:
        go(gs0.at[d], rg0.at[a], s_g0, r_g0, on_a(NA - d))

    landed(cl.at[:, pl.ds(1, 3)], r_al)
    g = jnp.concatenate([dka[:, :128], dva[...]], axis=1).astype(BF16)
    comps = jnp.concatenate([cl[k, i] for k in range(NY) for i in range(NA)], axis=1)
    up = dot(comps, g)
    for i in range(NB * NY):
        ups[i] = up[i * 64 : (i + 1) * 64, :].astype(BF16)
    mine = b * NY + y
    for i in far_first:
        e, f = others[i]
        tb, ty = (b + e) % NB, (y + f) % NY
        go(ups.at[tb * NY + ty], rup.at[mine], s_up, r_up, dev(a, tb, ty))
    rup[mine] = ups[mine]

    query_sums(1)
    rg0[a] = gs0[0]
    rg1[a] = gs1[0]

    landed(rup.at[pl.ds(0, 7)], r_up)
    us = sum(rup[i].astype(F32) for i in range(NB * NY)).astype(BF16)
    usk[...] = us[:, :128]
    usv[...] = us[:, 128:]
    ugk[a, mine] = us[:, :128]
    ugv[a, mine] = us[:, 128:]
    for i in far_first:
        e, f = others[i]
        fy = (y + f) % NY
        go(usk, ugk.at[a, mine], s_kb, r_kb.at[i], dev(a, (b + e) % NB, fy))
        go(usv, ugv.at[a, mine], s_va, r_va.at[i], dev((a + e) % NA, b, fy))

    def k_over_a(slot):
        for d in near:
            go(slot, slot, s_ka, r_ka.at[d - 1], on_a(d))

    def v_over_b(slot):
        for e in near:
            go(slot, slot, s_vb, r_vb.at[e - 1], on_b(e))

    k_over_a(ugk.at[a, mine])
    v_over_b(ugv.at[a, mine])

    landed(rg1.at[pl.ds(0, 3)], r_g1)
    landed(rg0.at[pl.ds(0, 3)], r_g0)
    dk_all = jnp.concatenate(
        [jnp.concatenate([r[h, :, :128] for h in range(NA)], axis=1) for r in (rg0, rg1)], axis=0
    )
    dv_all = jnp.concatenate(
        [jnp.concatenate([r[h, :, 128:256] for h in range(NA)], axis=1) for r in (rg0, rg1)], axis=0
    )
    lp = dot(ku_ref[...], dk_all, NT) + dot(vu_ref[...], dv_all, NT)
    rope = sum(rg0[h, :, 256:].astype(F32) for h in range(NA)).T
    for k in range(NY):
        whole = jnp.concatenate([lp[:, k * 128 : (k + 1) * 128], rope[k * 64 : (k + 1) * 64, :]], axis=0)
        lsum[k] = whole.reshape(2, 288, ROWS)
    for k in range(NY):
        lhalf[k] = lsum[k, 1 - core].astype(BF16)
    go(lhalf, rhalf, s_h.at[0], r_h.at[0], twin)

    def piece(i, axis):
        e, f = others[i]
        if axis == "b":
            return (b + NB - e) % NB * NY + (y + f) % NY
        return (a + NA - e) % NA, (y + f) % NY

    def pass_on(i):
        slot = ugk.at[a, piece(i, "b")]
        landed(slot, r_kb.at[i])
        k_over_a(slot)
        fa, fy = piece(i, "a")
        slot = ugv.at[fa, b * NY + fy]
        landed(slot, r_va.at[i])
        v_over_b(slot)

    for i in by_reach[:4]:
        pass_on(i)
    landed(rhalf, r_h.at[0])
    for k in range(NY):
        hs[k] = (lsum[k, core] + rhalf[k].astype(F32)).astype(BF16)
    go(hs.at[0], rh.at[0], s_h.at[1], r_h.at[1], far)
    go(hs.at[1], rh.at[1], s_h.at[1], r_h.at[1], across)
    go(hs.at[1], rh.at[2], s_h.at[1], r_h.at[1], corner)

    for i in by_reach[4:]:
        pass_on(i)
    landed(rq.at[:, pl.ds(1, 3)], r_dq)
    for t in range(2):
        for i, d in enumerate(pairs[t]):
            dqf[d] = (dqs[t, 0, i].astype(F32) + sum(rq[t, e, i].astype(F32) for e in near)).astype(BF16)
    for d in near:
        go(dqf.at[d], rdq.at[a], s_qf, r_qf, on_a(NA - d))
    rdq[a] = dqf[0]

    landed(rh, r_h.at[1])
    whole = hs[0].astype(F32) + rh[0].astype(F32) + rh[1].astype(F32) + rh[2].astype(F32)
    lfin[...] = whole
    go(lfin, rfin, s_h.at[2], r_h.at[2], twin)

    landed(rdq.at[pl.ds(0, 3)], r_qf)
    for h in range(NA):
        qg_ref[:, h * 192 : (h + 1) * 192] = rdq[h].T

    def write(src, dst, sem):
        pltpu.make_async_copy(src, dst, s_out.at[sem]).start()

    write(qg_ref, qg_hbm, 0)
    write(ugk.at[a], ugk_hbm.at[a], 2)
    own_b = pl.ds(b * NY, NY)
    write(ugv.at[:, own_b], ugv_hbm.at[:, own_b], 3)

    for d in near:
        fa, from_b = (a + NA - d) % NA, pl.ds((b + NB - d) % NB * NY, NY)
        landed(ugk.at[fa], r_ka.at[d - 1])
        write(ugk.at[fa], ugk_hbm.at[fa], 2)
        landed(ugv.at[:, from_b], r_vb.at[d - 1])
        write(ugv.at[:, from_b], ugv_hbm.at[:, from_b], 3)
    landed(rfin, r_h.at[2])
    write(lfin, lg_hbm.at[core], 1)
    write(rfin, lg_hbm.at[1 - core], 1)
    left(pq.at[pl.ds(0, 3)], s_aq)
    left(pk.at[pl.ds(0, 3)], s_ak)
    left(qb.at[pl.ds(0, 3)], s_bq)
    left(kb.at[0], s_yk)
    left(cl.at[1, 0], s_yl)
    left(cl.at[:, pl.ds(1, 3)], s_al)
    left(sb.at[:, pl.ds(0, 3)], s_st)
    left(rq.at[:, pl.ds(1, 3)], s_dq)
    left(rg0.at[pl.ds(0, 3)], s_g0)
    left(rg1.at[pl.ds(0, 3)], s_g1)
    left(rdq.at[pl.ds(0, 3)], s_qf)
    left(rup.at[pl.ds(0, 7)], s_up)
    left(ugk.at[0, pl.ds(0, 7)], s_kb)
    left(ugk.at[0, pl.ds(0, 7)], s_va)
    left(ugk.at[pl.ds(0, 3)], s_ka)
    left(ugv.at[pl.ds(0, 3)], s_vb)
    left(lhalf, s_h.at[0])
    left(rh, s_h.at[1])
    left(lfin, s_h.at[2])
    pltpu.make_async_copy(qg_ref, qg_hbm, s_out.at[0]).wait()
    pltpu.make_async_copy(lsum.at[0], lg_hbm, s_out.at[1]).wait()
    pltpu.make_async_copy(ugk, ugk_hbm, s_out.at[2]).wait()
    pltpu.make_async_copy(ugv, ugv_hbm, s_out.at[3]).wait()


def final_kernel(
    qg_hbm, lg_hbm, ugk_hbm, ugv_hbm, qg_ref, lg_ref, kug_ref, vug_ref, qv, lv, kv, vv, kf, vf, s_in, s_out
):
    quarter = D_LAT // 4
    loads, outs = [], []

    def start(pile, src, dst, sem):
        c = pltpu.make_async_copy(src, dst, sem)
        c.start()
        pile.append(c)

    for i in range(4):
        at = pl.ds(2 * i, 2)
        start(loads, ugk_hbm.at[:, at], kv.at[:, at], s_in.at[2 * i])
        start(loads, ugv_hbm.at[:, at], vv.at[:, at], s_in.at[2 * i + 1])
    start(loads, qg_hbm, qv, s_in.at[8])
    start(loads, lg_hbm, lv, s_in.at[9])
    for i in range(4):
        at = pl.ds(i * quarter, quarter)
        for n, (src, dst, out) in enumerate([(kv, kf, kug_ref), (vv, vf, vug_ref)]):
            loads[2 * i + n].wait()
            for h in range(NA):
                dst[i * quarter : (i + 1) * quarter, h * 128 : (h + 1) * 128] = (
                    src[h, 2 * i : 2 * i + 2].reshape(quarter, 128).astype(F32)
                )
            start(outs, dst.at[at], out.at[at], s_out.at[2 * i + n])
    loads[8].wait()
    start(outs, qv, qg_ref, s_out.at[8])
    loads[9].wait()
    start(outs, lv, lg_ref, s_out.at[9])
    for c in outs:
        c.wait()


def shards(queries, latents, key_up, value_up, out_grad, positions):
    half = NA * ROWS
    dma = pltpu.SemaphoreType.DMA
    scratch = [
        pltpu.SMEM((ROWS,), jnp.int32),
        pltpu.VMEM((ROWS, 768), BF16),
        pltpu.VMEM((576, ROWS), BF16),
        pltpu.VMEM((D_LAT, 512), BF16),
        pltpu.VMEM((D_LAT, 512), BF16),
        pltpu.VMEM((ROWS, 512), BF16),
        pltpu.VMEM((NA, BLOCK, 128), BF16),
        pltpu.VMEM((NA, BLOCK, 128), BF16),
        pltpu.VMEM((NB, NA, BLOCK, 128), BF16),
        pltpu.VMEM((NY, NA, BLOCK, 128), BF16),
        pltpu.VMEM((NB, half, 256), BF16),
        pltpu.VMEM((NY, half, 256), BF16),
        pltpu.VMEM((256, KTOK), BF16),
        pltpu.VMEM((NY, NA, D_LAT, ROWS), BF16),
        pltpu.VMEM((NY, half, TILE), F32),
        pltpu.VMEM((NY, NB, half, half), F32),
        pltpu.VMEM((NY, NB, half, half), F32),
        pltpu.VMEM((2, NB, 8, TILE), F32),
        pltpu.VMEM((2, NB, NB, 8, TILE), F32),
        pltpu.VMEM((NB, 8, half), F32),
        pltpu.VMEM((NB, KTOK, half), BF16),
        pltpu.VMEM((2, NB, 2, 192, 128), BF16),
        pltpu.VMEM((2, NB, 2, 192, 128), BF16),
        pltpu.VMEM((KTOK, 256), F32),
        pltpu.VMEM((KTOK, 128), F32),
        pltpu.VMEM((NA, ROWS, 384), BF16),
        pltpu.VMEM((NA, ROWS, 256), BF16),
        pltpu.VMEM((NA, ROWS, 384), BF16),
        pltpu.VMEM((NA, ROWS, 256), BF16),
        pltpu.VMEM((NA, 192, 128), BF16),
        pltpu.VMEM((NA, 192, 128), BF16),
        pltpu.VMEM((NB * NY, 64, 256), BF16),
        pltpu.VMEM((NB * NY, 64, 256), BF16),
        pltpu.VMEM((64, 128), BF16),
        pltpu.VMEM((64, 128), BF16),
        pltpu.VMEM((NY, 2, 288, ROWS), F32),
        pltpu.VMEM((NY, 288, ROWS), BF16),
        pltpu.VMEM((NY, 288, ROWS), BF16),
        pltpu.VMEM((NY, 288, ROWS), BF16),
        pltpu.VMEM((3, 288, ROWS), BF16),
        pltpu.VMEM((288, ROWS), F32),
        pltpu.VMEM((288, ROWS), F32),
        pltpu.VMEM((ROWS, 768), BF16),
        pltpu.VMEM((NA, NB * NY, 64, 128), BF16),
        pltpu.VMEM((NA, NB * NY, 64, 128), BF16),
    ]
    sems = [
        dma((6,)), dma, dma((3,)), dma, dma((3,)), dma, dma,
        dma, dma((3, 2)), dma, dma, dma, dma,
        dma, dma((2, 4)), dma, dma,
        dma, dma, dma, dma, dma, dma, dma, dma,
        dma, dma((7,)), dma, dma((3,)), dma, dma((7,)), dma, dma((3,)),
        dma((3,)), dma((3,)), dma((4,)),
    ]
    hbm = pl.BlockSpec(memory_space=pltpu.HBM)
    qg, lg, ugk, ugv = pl.pallas_call(
        whole_kernel,
        out_shape=(
            shape((ROWS, 768)),
            shape((2, 288, ROWS), F32),
            shape((NA, NB * NY, 64, 128)),
            shape((NA, NB * NY, 64, 128)),
        ),
        in_specs=[hbm] * 6,
        out_specs=(hbm,) * 4,
        scratch_shapes=scratch + sems,
        compiler_params=pltpu.CompilerParams(
            collective_id=0, has_side_effects=True, vmem_limit_bytes=LIMIT * 1024 * 1024
        ),
    )(positions, queries, latents.T, key_up, value_up, out_grad)
    qg, lg, kug, vug = pl.pallas_call(
        final_kernel,
        out_shape=(
            shape((ROWS, 768)),
            shape((2, 288, ROWS), F32),
            shape((D_LAT, 512), F32),
            shape((D_LAT, 512), F32),
        ),
        in_specs=[hbm] * 4,
        out_specs=(hbm,) * 4,
        scratch_shapes=[
            pltpu.VMEM((ROWS, 768), BF16),
            pltpu.VMEM((2, 288, ROWS), F32),
            pltpu.VMEM((NA, NB * NY, 64, 128), BF16),
            pltpu.VMEM((NA, NB * NY, 64, 128), BF16),
            pltpu.VMEM((D_LAT, 512), F32),
            pltpu.VMEM((D_LAT, 512), F32),
            dma((10,)),
            dma((10,)),
        ],
        compiler_params=pltpu.CompilerParams(vmem_limit_bytes=LIMIT * 1024 * 1024),
    )(qg, lg, ugk, ugv)
    return (qg, lg.reshape(576, ROWS).T, kug, vug)


def solution(mesh):
    in_specs = (
        P("seq", "head"),
        P("seq", None),
        P(None, "head"),
        P(None, "head"),
        P("seq", "head"),
        P("seq"),
    )
    out_specs = (P("seq", "head"), P("seq", None), P(None, "head"), P(None, "head"))
    return jax.shard_map(shards, mesh=mesh, in_specs=in_specs, out_specs=out_specs, check_vma=False)
```

```python
import math

import jax
import jax.numpy as jnp
from jax import lax
from jax.experimental import pallas as pl
from jax.experimental.pallas import tpu as pltpu
from jax.sharding import PartitionSpec as P


D_LAT = 512
D_ROPE = 64
D_NOPE = 128
D_V = 128
ROWS = 128
NA = 4
NB = 4
NY = 2
BLOCK = 336
KTOK = NY * NA * ROWS
TILE = 256
NEG = -1e30
LIMIT = 60
FLOOR = -1e29
SCALE = 1.0 / math.sqrt(D_NOPE + D_ROPE)
LOG2E = math.log2(math.e)
MESH = pl.DeviceIdType.MESH
F32 = jnp.float32
BF16 = jnp.bfloat16
VMEM = pl.BlockSpec(memory_space=pltpu.VMEM)
NT = (((1,), (1,)), ((), ()))
TN = (((0,), (0,)), ((), ()))


def coords():
    seq = lax.axis_index("seq")
    head = lax.axis_index("head")
    core = head % 2
    y = seq // 16
    z = (seq // 4) % 4
    x = seq % 4
    a = x + core * (z - x)
    b = z + core * (x - z)
    sa = 1 + 3 * core
    sb = 4 - 3 * core

    def dev(a2, b2, y2):
        return (y2 * 16 + a2 * sa + b2 * sb, head)

    return seq, head, y, a, b, dev


def rcopy(src, dst, send, recv, device):
    return pltpu.make_async_remote_copy(
        src_ref=src, dst_ref=dst, send_sem=send, recv_sem=recv, device_id=device, device_id_type=MESH
    )


def dot(u, v, dims=(((1,), (0,)), ((), ()))):
    return lax.dot_general(u, v, dims, preferred_element_type=F32)


def shape(dims, dtype=BF16):
    return jax.ShapeDtypeStruct(dims, dtype)


def whole_kernel(
    pos_hbm, q_hbm, latt_hbm, ku_hbm, vu_hbm, g_hbm,
    qg_hbm, lg_hbm, ugk_hbm, ugv_hbm,
    pos_ref, q_ref, latt_ref, ku_ref, vu_ref, g_ref,
    pq, pk, qb, kb, qp, kp, kpt, cl, kpos, s_all, dp_all, stl, sb, rows, ds_all, dqs, rq, dka, dva, gs0, gs1, rg0, rg1,
    dqf, rdq, ups, rup, usk, usv, lsum, lhalf, rhalf, hs, rh, lfin, rfin, qg_ref, ugk, ugv,
    s_in, s_aq, r_aq, s_ak, r_ak, s_al, r_al, s_bq, r_bq, s_yk, r_yk, s_yl, r_yl, s_st, r_st, s_dq, r_dq,
    s_g0, r_g0, s_g1, r_g1, s_qf, r_qf, s_up, r_up,
    s_kb, r_kb, s_ka, r_ka, s_va, r_va, s_vb, r_vb, s_h, r_h, s_out,
):
    seq, head, y, a, b, dev = coords()
    core = head % 2
    twin = (seq, head + 1 - 2 * core)
    far = (seq, (head + 2) % 4)
    across = dev(a, b, 1 - y)
    corner = (across[0], (head + 2) % 4)
    near = (1, 3, 2)
    others = [(0, 1), (1, 0), (1, 1), (2, 0), (2, 1), (3, 0), (3, 1)]
    by_reach = (1, 5, 0, 3, 2, 6, 4)
    far_first = by_reach[::-1]

    barrier = pltpu.get_barrier_semaphore()
    for p in (
        [dev((a + d) % NA, b, y) for d in near]
        + [dev(a, (b + e) % NB, (y + f) % NY) for e, f in others]
        + [dev((a + d) % NA, b, 1 - y) for d in near]
        + [twin, far, corner]
    ):
        pl.semaphore_signal(barrier, inc=1, device_id=p, device_id_type=MESH)

    def go(src, dst, send, recv, device):
        rcopy(src, dst, send, recv, device).start()

    def landed(ref, recv):
        rcopy(ref, ref, recv, recv, across).wait_recv()

    def left(ref, send):
        rcopy(ref, ref, send, send, across).wait_send()

    loads = [
        pltpu.make_async_copy(src, dst, s_in.at[i])
        for i, (src, dst) in enumerate(
            [(pos_hbm, pos_ref), (q_hbm, q_ref), (g_hbm, g_ref), (latt_hbm, latt_ref), (ku_hbm, ku_ref), (vu_hbm, vu_ref)]
        )
    ]
    for c in loads:
        c.start()
    for c in loads[:3]:
        c.wait()

    stripe = lax.shift_right_logical(pos_ref[0], 7).astype(F32)
    stripes = jnp.full((16, 128), stripe, F32).astype(BF16)
    for h in range(NA):
        q = q_ref[:, h * 192 : (h + 1) * 192]
        pq[h, 0:128, :] = q[:, :128]
        pq[h, 128:256, :] = g_ref[:, h * 128 : (h + 1) * 128]
        pq[h, 256:320, :] = jnp.concatenate([q[:64, 128:], q[64:, 128:]], axis=1)
        pq[h, 320:, :] = stripes
    qb[0, 0] = pq[a]
    for c in loads[3:]:
        c.wait()
    comp = latt_ref[:D_LAT, :]
    kn = dot(comp, ku_ref[...], TN).astype(BF16)
    vv = dot(comp, vu_ref[...], TN).astype(BF16)
    eye = (
        lax.broadcasted_iota(jnp.int32, (64, 128), 0) == lax.broadcasted_iota(jnp.int32, (64, 128), 1)
    ).astype(F32).astype(BF16)
    k_rope = dot(latt_ref[D_LAT:, :], eye, TN).astype(BF16)
    k_rope = jnp.concatenate([k_rope[:64, :64], k_rope[64:, :64]], axis=1)
    for h in range(NA):
        pk[h, 0:128, :] = kn[:, h * 128 : (h + 1) * 128]
        pk[h, 128:256, :] = vv[:, h * 128 : (h + 1) * 128]
        pk[h, 256:320, :] = k_rope
        pk[h, 320:, :] = stripes
    kb[0, 0] = pk[a]
    cl[0, 0] = comp

    pl.semaphore_wait(barrier, 6 + len(others) + 3)

    def on_a(d):
        return dev((a + d) % NA, b, y)

    def on_b(e):
        return dev(a, (b + e) % NB, y)

    def tile_of(d):
        return 0 if d < 2 else 1

    for d in near:
        go(pk.at[(a + d) % NA], kb.at[0, d], s_ak, r_ak.at[d - 1], on_a(d))
    go(pk.at[a], kb.at[1, 0], s_yk, r_yk, across)
    for d in near:
        go(pq.at[(a + d) % NA], qb.at[0, d], s_aq, r_aq.at[d - 1], on_a(d))
    for e in near:
        go(pq.at[a], qb.at[e, 0], s_bq, r_bq.at[e - 1, 0], on_b(e))
    def pass_q(d):
        landed(qb.at[0, d], r_aq.at[d - 1])
        for e in near:
            go(qb.at[0, d], qb.at[e, d], s_bq, r_bq.at[e - 1, tile_of(d)], on_b(e))

    def pass_k(d):
        landed(kb.at[0, d], r_ak.at[d - 1])
        go(kb.at[0, d], kb.at[1, d], s_yk, r_yk, across)

    pass_k(1)
    pass_k(3)
    pass_q(1)
    pass_q(3)
    pass_k(2)
    pass_q(2)
    go(latt_ref.at[pl.ds(0, D_LAT)], cl.at[1, 0], s_yl, r_yl, across)

    half = NA * ROWS
    row = lax.broadcasted_iota(jnp.int32, (ROWS, TILE), 0).astype(F32)
    col = lax.broadcasted_iota(jnp.int32, (1, ROWS), 1).astype(F32)
    blank = jnp.zeros((ROWS, 64), BF16)
    pairs = ((0, 1), (3, 2))

    def wide(block):
        rope = jnp.concatenate([block[256:320, :64], block[256:320, 64:]], axis=0)
        return jnp.concatenate([block[:128, :], rope, blank], axis=1)

    def open_keys(k):
        for d in range(NA):
            at = slice(d * ROWS, (d + 1) * ROWS)
            block = kb[k, d]
            kp[k, at, :] = wide(block)
            stripe = block[320:321, :].astype(F32) * 128.0
            kpos[k, at, :] = jnp.concatenate([stripe, stripe], axis=1) + row

    def open_queries(e, t):
        for i, d in enumerate(pairs[t]):
            at = slice(t * TILE + i * ROWS, t * TILE + (i + 1) * ROWS)
            qp[e, at, :] = wide(qb[e, d])

    def wait_q(e, t):
        landed(qb.at[e, pl.ds(2 * t, 2)], r_bq.at[e - 1, t])

    def grads_of(e, t):
        d0, d1 = pairs[t]
        return jnp.concatenate([qb[e, d0, 128:256, :], qb[e, d1, 128:256, :]], axis=0)

    def unit(k, e, t, first):
        at = slice(t * TILE, (t + 1) * TILE)
        if first:
            open_queries(e, t)
        qpos = jnp.concatenate([qb[e, d, 320:321, :].astype(F32) * 128.0 + col for d in pairs[t]], axis=1)
        raw = dot(kp[k], qp[e, at, :], NT)
        s = jnp.where(kpos[k] <= qpos, raw * (SCALE * LOG2E), NEG)
        s_all[k, e, :, at] = s
        dp = dot(kb[k, :, 128:256, :].reshape(half, 128), grads_of(e, t), NT)
        dp_all[k, e, :, at] = dp
        top = jnp.max(s, axis=0, keepdims=True)
        if not first:
            old = stl[t, e, 0:1, :]
            top = jnp.maximum(top, old)
        w = jnp.exp2(s - jnp.maximum(top, FLOOR))
        total = jnp.sum(w, axis=0, keepdims=True)
        weighted = jnp.sum(w * dp, axis=0, keepdims=True)
        if not first:
            fade = jnp.exp2(old - top)
            total = total + fade * stl[t, e, 1:2, :]
            weighted = weighted + fade * stl[t, e, 2:3, :]
        stl[t, e, 0:1, :] = top
        stl[t, e, 1:2, :] = total
        stl[t, e, 2:3, :] = weighted

    def tell(t, e):
        for g in near:
            to = (e + g) % NB
            go(stl.at[t, e], sb.at[t, to, g], s_st, r_st.at[t, to], on_b(g))

    stl[...] = jnp.zeros_like(stl)
    open_keys(0)
    unit(0, 0, 0, True)
    unit(0, 0, 1, True)
    for e in near:
        wait_q(e, 0)
        unit(0, e, 0, True)
    landed(kb.at[1], r_yk)
    for d in near:
        go(latt_ref.at[pl.ds(0, D_LAT)], cl.at[0, d], s_al, r_al, on_a(d))
    open_keys(1)
    unit(1, 0, 0, False)
    tell(0, 0)
    for e in near:
        unit(1, e, 0, False)
        tell(0, e)
    unit(1, 0, 1, False)
    tell(1, 0)
    for e in near:
        wait_q(e, 1)
        if e == 1:
            landed(cl.at[1, 0], r_yl)
            for d in near:
                go(cl.at[1, 0], cl.at[1, d], s_al, r_al, on_a(d))
        unit(0, e, 1, True)
        unit(1, e, 1, False)
        tell(1, e)
    kpt[...] = kp[...].reshape(KTOK, 256).T

    def backward(k, t):
        ks = slice(k * half, (k + 1) * half)
        at = slice(t * TILE, (t + 1) * TILE)
        for n, e in enumerate((0, 1, 3, 2)):
            if k == 1:
                landed(sb.at[t, e, pl.ds(1, 3)], r_st.at[t, e])
                got = [stl[t, e]] + [sb[t, e, g] for g in near]
                tops = [r[0:1, :] for r in got]
                top = jnp.maximum(jnp.maximum(tops[0], tops[1]), jnp.maximum(tops[2], tops[3]))
                fades = [jnp.exp2(u - top) for u in tops]
                total = sum(f * r[1:2, :] for f, r in zip(fades, got))
                rows[e, 1:2, at] = sum(f * r[2:3, :] for f, r in zip(fades, got)) / total
                rows[e, 0:1, at] = top + jnp.log(total) * LOG2E
            p = jnp.exp2(s_all[k, e, :, at] - rows[e, 0:1, at])
            ds = (p * (dp_all[k, e, :, at] - rows[e, 1:2, at]) * SCALE).astype(BF16)
            ds_all[e, ks, at] = ds
            dv = dot(p.astype(BF16), grads_of(e, t))
            dk = dot(ds, qp[e, at, :])
            if n == 0 and t == 0:
                dva[ks, :] = dv
                dka[ks, :] = dk
            else:
                dva[ks, :] += dv
                dka[ks, :] += dk

    def query_sums(t):
        at = slice(t * TILE, (t + 1) * TILE)
        for e in (2, 1, 3, 0):
            dq = dot(kpt[:192, :], ds_all[e, :, at]).astype(BF16)
            dqs[t, e, 0] = dq[:, :ROWS]
            dqs[t, e, 1] = dq[:, ROWS:]
            if e:
                go(dqs.at[t, e], rq.at[t, e], s_dq, r_dq, on_b(NB - e))

    backward(1, 0)
    backward(0, 0)
    query_sums(0)
    backward(1, 1)
    for d in range(NA):
        at = slice(half + d * ROWS, half + (d + 1) * ROWS)
        gs1[d, :, :128] = dka[at, :128].astype(BF16)
        gs1[d, :, 128:] = dva[at, :].astype(BF16)
    for d in near:
        go(gs1.at[d], rg1.at[a], s_g1, r_g1, on_a(NA - d))
    backward(0, 1)
    for d in range(NA):
        at = slice(d * ROWS, (d + 1) * ROWS)
        at1 = slice(half + d * ROWS, half + (d + 1) * ROWS)
        gs0[d, :, :128] = dka[at, :128].astype(BF16)
        gs0[d, :, 128:256] = dva[at, :].astype(BF16)
        gs0[d, :, 256:] = jnp.concatenate([dka[at, 128:192], dka[at1, 128:192]], axis=1).astype(BF16)
    for d in near:
        go(gs0.at[d], rg0.at[a], s_g0, r_g0, on_a(NA - d))

    landed(cl.at[:, pl.ds(1, 3)], r_al)
    g = jnp.concatenate([dka[:, :128], dva[...]], axis=1).astype(BF16)
    comps = jnp.concatenate([cl[k, i] for k in range(NY) for i in range(NA)], axis=1)
    up = dot(comps, g)
    for i in range(NB * NY):
        ups[i] = up[i * 64 : (i + 1) * 64, :].astype(BF16)
    mine = b * NY + y
    for i in far_first:
        e, f = others[i]
        tb, ty = (b + e) % NB, (y + f) % NY
        go(ups.at[tb * NY + ty], rup.at[mine], s_up, r_up, dev(a, tb, ty))
    rup[mine] = ups[mine]

    query_sums(1)
    rg0[a] = gs0[0]
    rg1[a] = gs1[0]

    landed(rup.at[pl.ds(0, 7)], r_up)
    us = sum(rup[i].astype(F32) for i in range(NB * NY)).astype(BF16)
    usk[...] = us[:, :128]
    usv[...] = us[:, 128:]
    ugk[a, mine] = us[:, :128]
    ugv[a, mine] = us[:, 128:]
    for i in far_first:
        e, f = others[i]
        fy = (y + f) % NY
        go(usk, ugk.at[a, mine], s_kb, r_kb.at[i], dev(a, (b + e) % NB, fy))
        go(usv, ugv.at[a, mine], s_va, r_va.at[i], dev((a + e) % NA, b, fy))

    def k_over_a(slot):
        for d in near:
            go(slot, slot, s_ka, r_ka.at[d - 1], on_a(d))

    def v_over_b(slot):
        for e in near:
            go(slot, slot, s_vb, r_vb.at[e - 1], on_b(e))

    k_over_a(ugk.at[a, mine])
    v_over_b(ugv.at[a, mine])

    landed(rg1.at[pl.ds(0, 3)], r_g1)
    landed(rg0.at[pl.ds(0, 3)], r_g0)
    dk_all = jnp.concatenate(
        [jnp.concatenate([r[h, :, :128] for h in range(NA)], axis=1) for r in (rg0, rg1)], axis=0
    )
    dv_all = jnp.concatenate(
        [jnp.concatenate([r[h, :, 128:256] for h in range(NA)], axis=1) for r in (rg0, rg1)], axis=0
    )
    lp = dot(ku_ref[...], dk_all, NT) + dot(vu_ref[...], dv_all, NT)
    rope = sum(rg0[h, :, 256:].astype(F32) for h in range(NA)).T
    for k in range(NY):
        whole = jnp.concatenate([lp[:, k * 128 : (k + 1) * 128], rope[k * 64 : (k + 1) * 64, :]], axis=0)
        lsum[k] = whole.reshape(2, 288, ROWS)
    for k in range(NY):
        lhalf[k] = lsum[k, 1 - core].astype(BF16)
    go(lhalf, rhalf, s_h.at[0], r_h.at[0], twin)

    landed(rq.at[:, pl.ds(1, 3)], r_dq)
    for t in range(2):
        for i, d in enumerate(pairs[t]):
            dqf[d] = (dqs[t, 0, i].astype(F32) + sum(rq[t, e, i].astype(F32) for e in near)).astype(BF16)
    for d in near:
        go(dqf.at[d], rdq.at[a], s_qf, r_qf, on_a(NA - d))
    rdq[a] = dqf[0]

    def piece(i, axis):
        e, f = others[i]
        if axis == "b":
            return (b + NB - e) % NB * NY + (y + f) % NY
        return (a + NA - e) % NA, (y + f) % NY

    def pass_on(i):
        slot = ugk.at[a, piece(i, "b")]
        landed(slot, r_kb.at[i])
        k_over_a(slot)
        fa, fy = piece(i, "a")
        slot = ugv.at[fa, b * NY + fy]
        landed(slot, r_va.at[i])
        v_over_b(slot)

    for i in by_reach[:4]:
        pass_on(i)
    landed(rhalf, r_h.at[0])
    for k in range(NY):
        hs[k] = (lsum[k, core] + rhalf[k].astype(F32)).astype(BF16)
    go(hs.at[0], rh.at[0], s_h.at[1], r_h.at[1], far)
    go(hs.at[1], rh.at[1], s_h.at[1], r_h.at[1], across)
    go(hs.at[1], rh.at[2], s_h.at[1], r_h.at[1], corner)

    for i in by_reach[4:]:
        pass_on(i)
    landed(rh, r_h.at[1])
    whole = hs[0].astype(F32) + rh[0].astype(F32) + rh[1].astype(F32) + rh[2].astype(F32)
    lfin[...] = whole
    go(lfin, rfin, s_h.at[2], r_h.at[2], twin)

    landed(rdq.at[pl.ds(0, 3)], r_qf)
    for h in range(NA):
        qg_ref[:, h * 192 : (h + 1) * 192] = rdq[h].T

    def write(src, dst, sem):
        pltpu.make_async_copy(src, dst, s_out.at[sem]).start()

    write(qg_ref, qg_hbm, 0)
    write(ugk.at[a], ugk_hbm.at[a], 2)
    own_b = pl.ds(b * NY, NY)
    write(ugv.at[:, own_b], ugv_hbm.at[:, own_b], 3)

    for d in near:
        fa, from_b = (a + NA - d) % NA, pl.ds((b + NB - d) % NB * NY, NY)
        landed(ugk.at[fa], r_ka.at[d - 1])
        write(ugk.at[fa], ugk_hbm.at[fa], 2)
        landed(ugv.at[:, from_b], r_vb.at[d - 1])
        write(ugv.at[:, from_b], ugv_hbm.at[:, from_b], 3)
    landed(rfin, r_h.at[2])
    write(lfin, lg_hbm.at[core], 1)
    write(rfin, lg_hbm.at[1 - core], 1)
    left(pq.at[pl.ds(0, 3)], s_aq)
    left(pk.at[pl.ds(0, 3)], s_ak)
    left(qb.at[pl.ds(0, 3)], s_bq)
    left(kb.at[0], s_yk)
    left(cl.at[1, 0], s_yl)
    left(cl.at[:, pl.ds(1, 3)], s_al)
    left(sb.at[:, pl.ds(0, 3)], s_st)
    left(rq.at[:, pl.ds(1, 3)], s_dq)
    left(rg0.at[pl.ds(0, 3)], s_g0)
    left(rg1.at[pl.ds(0, 3)], s_g1)
    left(rdq.at[pl.ds(0, 3)], s_qf)
    left(rup.at[pl.ds(0, 7)], s_up)
    left(ugk.at[0, pl.ds(0, 7)], s_kb)
    left(ugk.at[0, pl.ds(0, 7)], s_va)
    left(ugk.at[pl.ds(0, 3)], s_ka)
    left(ugv.at[pl.ds(0, 3)], s_vb)
    left(lhalf, s_h.at[0])
    left(rh, s_h.at[1])
    left(lfin, s_h.at[2])
    pltpu.make_async_copy(qg_ref, qg_hbm, s_out.at[0]).wait()
    pltpu.make_async_copy(lsum.at[0], lg_hbm, s_out.at[1]).wait()
    pltpu.make_async_copy(ugk, ugk_hbm, s_out.at[2]).wait()
    pltpu.make_async_copy(ugv, ugv_hbm, s_out.at[3]).wait()


def final_kernel(
    qg_hbm, lg_hbm, ugk_hbm, ugv_hbm, qg_ref, lg_ref, kug_ref, vug_ref, qv, lv, kv, vv, kf, vf, s_in, s_out
):
    quarter = D_LAT // 4
    loads, outs = [], []

    def start(pile, src, dst, sem):
        c = pltpu.make_async_copy(src, dst, sem)
        c.start()
        pile.append(c)

    for i in range(4):
        at = pl.ds(2 * i, 2)
        start(loads, ugk_hbm.at[:, at], kv.at[:, at], s_in.at[2 * i])
        start(loads, ugv_hbm.at[:, at], vv.at[:, at], s_in.at[2 * i + 1])
    start(loads, qg_hbm, qv, s_in.at[8])
    start(loads, lg_hbm, lv, s_in.at[9])
    for i in range(4):
        at = pl.ds(i * quarter, quarter)
        for n, (src, dst, out) in enumerate([(kv, kf, kug_ref), (vv, vf, vug_ref)]):
            loads[2 * i + n].wait()
            for h in range(NA):
                dst[i * quarter : (i + 1) * quarter, h * 128 : (h + 1) * 128] = (
                    src[h, 2 * i : 2 * i + 2].reshape(quarter, 128).astype(F32)
                )
            start(outs, dst.at[at], out.at[at], s_out.at[2 * i + n])
    loads[8].wait()
    start(outs, qv, qg_ref, s_out.at[8])
    loads[9].wait()
    start(outs, lv, lg_ref, s_out.at[9])
    for c in outs:
        c.wait()


def shards(queries, latents, key_up, value_up, out_grad, positions):
    half = NA * ROWS
    dma = pltpu.SemaphoreType.DMA
    scratch = [
        pltpu.SMEM((ROWS,), jnp.int32),
        pltpu.VMEM((ROWS, 768), BF16),
        pltpu.VMEM((576, ROWS), BF16),
        pltpu.VMEM((D_LAT, 512), BF16),
        pltpu.VMEM((D_LAT, 512), BF16),
        pltpu.VMEM((ROWS, 512), BF16),
        pltpu.VMEM((NA, BLOCK, 128), BF16),
        pltpu.VMEM((NA, BLOCK, 128), BF16),
        pltpu.VMEM((NB, NA, BLOCK, 128), BF16),
        pltpu.VMEM((NY, NA, BLOCK, 128), BF16),
        pltpu.VMEM((NB, half, 256), BF16),
        pltpu.VMEM((NY, half, 256), BF16),
        pltpu.VMEM((256, KTOK), BF16),
        pltpu.VMEM((NY, NA, D_LAT, ROWS), BF16),
        pltpu.VMEM((NY, half, TILE), F32),
        pltpu.VMEM((NY, NB, half, half), F32),
        pltpu.VMEM((NY, NB, half, half), F32),
        pltpu.VMEM((2, NB, 8, TILE), F32),
        pltpu.VMEM((2, NB, NB, 8, TILE), F32),
        pltpu.VMEM((NB, 8, half), F32),
        pltpu.VMEM((NB, KTOK, half), BF16),
        pltpu.VMEM((2, NB, 2, 192, 128), BF16),
        pltpu.VMEM((2, NB, 2, 192, 128), BF16),
        pltpu.VMEM((KTOK, 256), F32),
        pltpu.VMEM((KTOK, 128), F32),
        pltpu.VMEM((NA, ROWS, 384), BF16),
        pltpu.VMEM((NA, ROWS, 256), BF16),
        pltpu.VMEM((NA, ROWS, 384), BF16),
        pltpu.VMEM((NA, ROWS, 256), BF16),
        pltpu.VMEM((NA, 192, 128), BF16),
        pltpu.VMEM((NA, 192, 128), BF16),
        pltpu.VMEM((NB * NY, 64, 256), BF16),
        pltpu.VMEM((NB * NY, 64, 256), BF16),
        pltpu.VMEM((64, 128), BF16),
        pltpu.VMEM((64, 128), BF16),
        pltpu.VMEM((NY, 2, 288, ROWS), F32),
        pltpu.VMEM((NY, 288, ROWS), BF16),
        pltpu.VMEM((NY, 288, ROWS), BF16),
        pltpu.VMEM((NY, 288, ROWS), BF16),
        pltpu.VMEM((3, 288, ROWS), BF16),
        pltpu.VMEM((288, ROWS), F32),
        pltpu.VMEM((288, ROWS), F32),
        pltpu.VMEM((ROWS, 768), BF16),
        pltpu.VMEM((NA, NB * NY, 64, 128), BF16),
        pltpu.VMEM((NA, NB * NY, 64, 128), BF16),
    ]
    sems = [
        dma((6,)), dma, dma((3,)), dma, dma((3,)), dma, dma,
        dma, dma((3, 2)), dma, dma, dma, dma,
        dma, dma((2, 4)), dma, dma,
        dma, dma, dma, dma, dma, dma, dma, dma,
        dma, dma((7,)), dma, dma((3,)), dma, dma((7,)), dma, dma((3,)),
        dma((3,)), dma((3,)), dma((4,)),
    ]
    hbm = pl.BlockSpec(memory_space=pltpu.HBM)
    qg, lg, ugk, ugv = pl.pallas_call(
        whole_kernel,
        out_shape=(
            shape((ROWS, 768)),
            shape((2, 288, ROWS), F32),
            shape((NA, NB * NY, 64, 128)),
            shape((NA, NB * NY, 64, 128)),
        ),
        in_specs=[hbm] * 6,
        out_specs=(hbm,) * 4,
        scratch_shapes=scratch + sems,
        compiler_params=pltpu.CompilerParams(
            collective_id=0, has_side_effects=True, vmem_limit_bytes=LIMIT * 1024 * 1024
        ),
    )(positions, queries, latents.T, key_up, value_up, out_grad)
    qg, lg, kug, vug = pl.pallas_call(
        final_kernel,
        out_shape=(
            shape((ROWS, 768)),
            shape((2, 288, ROWS), F32),
            shape((D_LAT, 512), F32),
            shape((D_LAT, 512), F32),
        ),
        in_specs=[hbm] * 4,
        out_specs=(hbm,) * 4,
        scratch_shapes=[
            pltpu.VMEM((ROWS, 768), BF16),
            pltpu.VMEM((2, 288, ROWS), F32),
            pltpu.VMEM((NA, NB * NY, 64, 128), BF16),
            pltpu.VMEM((NA, NB * NY, 64, 128), BF16),
            pltpu.VMEM((D_LAT, 512), F32),
            pltpu.VMEM((D_LAT, 512), F32),
            dma((10,)),
            dma((10,)),
        ],
        compiler_params=pltpu.CompilerParams(vmem_limit_bytes=LIMIT * 1024 * 1024),
    )(qg, lg, ugk, ugv)
    return (qg, lg.reshape(576, ROWS).T, kug, vug)


def solution(mesh):
    in_specs = (
        P("seq", "head"),
        P("seq", None),
        P(None, "head"),
        P(None, "head"),
        P("seq", "head"),
        P("seq"),
    )
    out_specs = (P("seq", "head"), P("seq", None), P(None, "head"), P(None, "head"))
    return jax.shard_map(shards, mesh=mesh, in_specs=in_specs, out_specs=out_specs, check_vma=False)
```
